256 devices in a mesh: section: 4 (over y_lo, core), lon: 32 (over z, x), lat: 2 (over y_hi).
Axes of the slice: x: 4, y: 4 (y_hi: 2, y_lo: 2; y = y_hi * 2 + y_lo), z: 8, core: 2. Of those that a mesh axis runs over, the one named last changes fastest.
Arguments:
- inputs: bfloat16 [4, 8, 12, 384, 192], P('section', None, 'lat', 'lon'), may hold values from -6 to 6
- grad_output: bfloat16 [4, 8, 12, 384, 192], P('section', None, 'lat', 'lon'), may hold values from -6 to 6
- norm_gains: float32 [4, 2, 2, 192], P('section'), may hold values from 0.25 to 1.75
- input_weight: bfloat16 [4, 2, 192, 576], P('section'), may hold values from -0.4375 to 0.4375
- output_weight: bfloat16 [4, 2, 192, 192], P('section'), may hold values from -0.4375 to 0.4375
- expand_weight: bfloat16 [4, 2, 192, 768], P('section'), may hold values from -0.4375 to 0.4375
- reduce_weight: bfloat16 [4, 2, 768, 192], P('section'), may hold values from -0.21875 to 0.21875
- bias_table: float32 [4, 2, 4, 2, 6, 3312], P('section'), may hold values from -4 to 400
Outputs:
- upstream: bfloat16 [4, 8, 12, 384, 192], P('section', None, 'lat', 'lon')
- input_weight_grad: float32 [4, 2, 192, 576], P('section')
- output_weight_grad: float32 [4, 2, 192, 192], P('section')
- expand_weight_grad: float32 [4, 2, 192, 768], P('section')
- reduce_weight_grad: float32 [4, 2, 768, 192], P('section')
- norm_gain_grad: float32 [4, 2, 2, 192], P('section')
- bias_table_grad: float32 [4, 2, 4, 2, 6, 3312], P('section')
The draws below stay inside these ranges and needn't reach their ends.
All inputs are finite; a program needn't handle non-finite values.
Results may differ from the reference program's by a relative error of at most 0.04.
Values may be sent and summed in bfloat16 or wider, within the bound.
No kernel may reach another device: no remote copies, remote signals or barrier semaphores. Data moves between devices by JAX's collectives and lax.ppermute only.
A program may use at most 128 MiB of HBM per device.

```python
import jax
import jax.numpy as jnp
from jax import lax

MODEL_WIDTH = 192
HEADS = 6
MLP_WIDTH = 768
HEAD_SIZE = 32
LEVELS = 8
WIN_LEVELS = 2
WIN_LAT = 6
WIN_LON = 12
BLOCKS = 2
WIN_TOKENS = 144
BIAS_SLOTS = 3312
SECTIONS = 4
LAT_ROWS = 12
LON_COLS = 384
LEVEL_WINDOWS = 4
LAT_WINDOWS = 2
N_LON = 32


def draw_bias_table(key, part):
    shape = (SECTIONS, BLOCKS, LEVEL_WINDOWS, LAT_WINDOWS, HEADS, BIAS_SLOTS)
    base_key = jax.random.fold_in(key, 11)
    return jnp.clip(jax.random.normal(base_key, shape, jnp.float32), -3.0, 3.0)


def shard_levels(rng, shape, cuts, smallest, largest):
    level = 1.0
    for axis_at, blocks in cuts:
        draws = jax.random.uniform(jax.random.fold_in(jax.random.fold_in(rng, 6), axis_at), (blocks,), jnp.float32, smallest / len(cuts), largest / len(cuts))
        level = level * jnp.repeat(jnp.exp(draws), shape[axis_at] // blocks).reshape((-1,) + (1,) * (len(shape) - 1 - axis_at))
    return level


def noise(key, shape, width, bound, cuts=(), kind=jnp.bfloat16):
    gain = shard_levels(key, shape, cuts, -0.22, 0.18) if cuts else 1.0
    entries = jax.random.normal(key, shape, jnp.float32) * width * gain
    return jnp.minimum(jnp.maximum(entries, -bound), bound).astype(kind)


def setup_inputs(seed: int = 0) -> dict:
    streams_of = jax.random.split(jax.random.key(seed), 9)
    return {
        "inputs": noise(streams_of[0], (SECTIONS, LEVELS, LAT_ROWS, LON_COLS, MODEL_WIDTH), 1.0, 6.0, ((0, 4), (2, 2), (3, 32))),
        "grad_output": noise(streams_of[1], (SECTIONS, LEVELS, LAT_ROWS, LON_COLS, MODEL_WIDTH), 1.0, 6.0, ((0, 4), (2, 2), (3, 32))),
        "norm_gains": jnp.clip(1.0 + 0.15 * jax.random.normal(streams_of[2], (SECTIONS, BLOCKS, 2, MODEL_WIDTH), jnp.float32), 0.25, 1.75),
        "input_weight": noise(streams_of[3], (SECTIONS, BLOCKS, MODEL_WIDTH, 3 * MODEL_WIDTH), MODEL_WIDTH ** -0.5, 0.4375, ((0, 4),)),
        "output_weight": noise(streams_of[4], (SECTIONS, BLOCKS, MODEL_WIDTH, MODEL_WIDTH), MODEL_WIDTH ** -0.5, 0.4375, ((0, 4),)),
        "expand_weight": noise(streams_of[5], (SECTIONS, BLOCKS, MODEL_WIDTH, MLP_WIDTH), MODEL_WIDTH ** -0.5, 0.4375, ((0, 4),)),
        "reduce_weight": noise(streams_of[6], (SECTIONS, BLOCKS, MLP_WIDTH, MODEL_WIDTH), MLP_WIDTH ** -0.5, 0.21875, ((0, 4),)),
        "bias_table": draw_bias_table(jax.random.fold_in(streams_of[8], 71), 0),
    }


NORM_EPS = 1e-05
MASK_FILL = -10000.0

def layer_norm(activity, gain_vec):
    centred = activity - lax.optimization_barrier(jnp.mean(activity, axis=-1, keepdims=True))
    spread = lax.optimization_barrier(jnp.mean(centred * centred, axis=-1, keepdims=True))
    return centred * lax.rsqrt(spread + NORM_EPS) * gain_vec

def gelu_tanh(activity):
    return jax.nn.gelu(activity, approximate=True)

def to_windows(tokens_in):
    levels_n, rows_n, cols_n, chans = tokens_in.shape
    shaped = tokens_in.reshape(levels_n // WIN_LEVELS, WIN_LEVELS, rows_n // WIN_LAT, WIN_LAT, cols_n // WIN_LON, WIN_LON, chans)
    shaped = shaped.transpose(0, 2, 4, 1, 3, 5, 6)
    return shaped.reshape(levels_n // WIN_LEVELS, rows_n // WIN_LAT, cols_n // WIN_LON, WIN_TOKENS, chans)

def from_windows(blocks_in):
    level_w, lat_w, lon_w, _, chans = blocks_in.shape
    shaped = blocks_in.reshape(level_w, lat_w, lon_w, WIN_LEVELS, WIN_LAT, WIN_LON, chans)
    shaped = shaped.transpose(0, 3, 1, 4, 2, 5, 6)
    return shaped.reshape(level_w * WIN_LEVELS, lat_w * WIN_LAT, lon_w * WIN_LON, chans)

def slot_index():
    positions = jnp.arange(WIN_TOKENS, dtype=jnp.int32)
    level_of = positions // (WIN_LAT * WIN_LON)
    row_of = positions // WIN_LON % WIN_LAT
    col_of = positions % WIN_LON
    level_pair = level_of[:, None] * WIN_LEVELS + level_of[None, :]
    row_pair = row_of[:, None] * WIN_LAT + row_of[None, :]
    offset = col_of[:, None] - col_of[None, :] + WIN_LON - 1
    return ((level_pair * WIN_LAT * WIN_LAT + row_pair) * (2 * WIN_LON - 1) + offset).astype(jnp.int32)

def region(position, extent, window_len):
    return jnp.where(position < extent - window_len, 0, jnp.where(position < extent - window_len // 2, 1, 2)).astype(jnp.int32)

def dense_bias(table_rows, first_row, lat_total, shifted):
    slot_ids = slot_index().reshape(-1)
    bias_dense = jnp.take(table_rows, slot_ids, axis=-1)
    bias_dense = bias_dense.reshape(table_rows.shape[:-1] + (WIN_TOKENS, WIN_TOKENS))
    if shifted:
        local_rows = table_rows.shape[1] * WIN_LAT
        level_ids = region(jnp.arange(LEVELS, dtype=jnp.int32), LEVELS, WIN_LEVELS)
        row_ids = region(first_row + jnp.arange(local_rows, dtype=jnp.int32), lat_total, WIN_LAT)
        region_ids = level_ids[:, None] * 3 + row_ids[None, :]
        region_grid = jnp.broadcast_to(region_ids[:, :, None, None], (LEVELS, local_rows, WIN_LON, 1))
        token_ids = to_windows(region_grid)[:, :, 0, :, 0]
        matched = token_ids[..., :, None] == token_ids[..., None, :]
        bias_dense = bias_dense + jnp.where(matched, 0.0, MASK_FILL).astype(jnp.float32)[:, :, None]
    return bias_dense[:, :, None]

def mix_tokens(tokens_in, weight):
    token_rows = tokens_in.reshape(-1, tokens_in.shape[-1])
    result = jnp.dot(token_rows, weight, preferred_element_type=jnp.float32)
    return result.reshape(tokens_in.shape[:-1] + (weight.shape[1],))

def mix_back(tokens_in, weight):
    token_rows = tokens_in.reshape(-1, tokens_in.shape[-1])
    result = lax.dot_general(token_rows, weight, (((1,), (1,)), ((), ())), preferred_element_type=jnp.float32)
    return result.reshape(tokens_in.shape[:-1] + (weight.shape[0],))

def grad_weight(tokens_in, grad_in):
    token_rows = tokens_in.reshape(-1, tokens_in.shape[-1])
    grad_rows = grad_in.reshape(-1, grad_in.shape[-1])
    return lax.dot_general(token_rows, grad_rows, (((0,), (0,)), ((), ())), preferred_element_type=jnp.float32)

def attend_parts(windows, bias_dense, input_weight):
    leading = windows.shape[:-2]
    token_rows = windows.reshape(-1, MODEL_WIDTH)
    projected = jnp.dot(token_rows, input_weight, preferred_element_type=jnp.float32)
    head_shape = leading + (WIN_TOKENS, HEADS, HEAD_SIZE)
    queries = (projected[:, :MODEL_WIDTH] * HEAD_SIZE ** (-0.5)).astype(jnp.bfloat16).reshape(head_shape)
    key_part = projected[:, MODEL_WIDTH:2 * MODEL_WIDTH].astype(jnp.bfloat16).reshape(head_shape)
    values = projected[:, 2 * MODEL_WIDTH:].astype(jnp.bfloat16).reshape(head_shape)
    scores = jnp.einsum('...qhe,...khe->...hqk', queries.astype(jnp.float32), key_part.astype(jnp.float32)) + bias_dense
    attention = jax.nn.softmax(scores, axis=-1)
    weights = attention.astype(jnp.bfloat16)
    mixture = jnp.einsum('...hqk,...khe->...qhe', weights.astype(jnp.float32), values.astype(jnp.float32)).astype(jnp.bfloat16)
    return (token_rows, queries, key_part, values, attention, weights, mixture)

def attend(windows, bias_dense, input_weight, output_weight):
    parts = attend_parts(windows, bias_dense, input_weight)
    mixture = parts[6]
    result = jnp.dot(mixture.reshape(-1, MODEL_WIDTH), output_weight, preferred_element_type=jnp.float32)
    return result.reshape(windows.shape)

def attend_grad(windows, bias_dense, input_weight, output_weight, grad_windows_in):
    token_rows, queries, key_part, values, attention, weights, mixture = attend_parts(windows, bias_dense, input_weight)
    leading = windows.shape[:-2]
    grad_rows = grad_windows_in.reshape(-1, MODEL_WIDTH)
    output_grad = grad_weight(mixture.reshape(-1, MODEL_WIDTH), grad_rows)
    grad_mixture = mix_back(grad_rows, output_weight).astype(jnp.bfloat16).reshape(leading + (WIN_TOKENS, HEADS, HEAD_SIZE))
    grad_values = jnp.einsum('...hqk,...qhe->...khe', weights.astype(jnp.float32), grad_mixture.astype(jnp.float32))
    grad_weights = jnp.einsum('...qhe,...khe->...hqk', grad_mixture.astype(jnp.float32), values.astype(jnp.float32))
    grad_scores = attention * (grad_weights - lax.optimization_barrier(jnp.sum(attention * grad_weights, axis=-1, keepdims=True)))
    score_part = grad_scores.astype(jnp.bfloat16).astype(jnp.float32)
    grad_queries = jnp.einsum('...hqk,...khe->...qhe', score_part, key_part.astype(jnp.float32)) * HEAD_SIZE ** (-0.5)
    grad_keys = jnp.einsum('...hqk,...qhe->...khe', score_part, queries.astype(jnp.float32))
    grad_projected = jnp.concatenate([piece_grad.reshape(-1, MODEL_WIDTH) for piece_grad in (grad_queries, grad_keys, grad_values)], axis=1).astype(jnp.bfloat16)
    input_grad = grad_weight(token_rows, grad_projected)
    grad_windows = mix_back(grad_projected, input_weight).reshape(windows.shape)
    return (grad_windows, input_grad, output_grad, grad_scores)

def table_grad(grad_scores):
    summed = lax.optimization_barrier(jnp.sum(grad_scores, axis=2))
    flat_rows = summed.reshape(-1, WIN_TOKENS * WIN_TOKENS)
    slot_ids = slot_index().reshape(-1)
    result = jax.ops.segment_sum(flat_rows.T, slot_ids, num_segments=BIAS_SLOTS)
    return result.T.reshape(summed.shape[:3] + (BIAS_SLOTS,))

def grouped(windows):
    level_w, lat_w, lon_w = windows.shape[:3]
    shaped = windows.reshape((level_w, lat_w, N_LON, lon_w // N_LON) + windows.shape[3:])
    return jnp.moveaxis(shaped, 2, 0)

def ungrouped(groups, like_shape):
    return jnp.moveaxis(groups, 0, 2).reshape(like_shape)

def attention_forward(framed, bias_dense, input_weight, output_weight):
    windows = to_windows(framed)
    results = lax.map(lambda group_in: attend(group_in, bias_dense, input_weight, output_weight), grouped(windows))
    return from_windows(ungrouped(results, windows.shape))

def attention_backward(framed, bias_dense, input_weight, output_weight, grad_attended):
    windows = to_windows(framed)
    grad_windows = to_windows(grad_attended)

    def accumulate(totals, pieces):
        grad_piece, input_grad, output_grad, grad_scores = attend_grad(pieces[0], bias_dense, input_weight, output_weight, pieces[1])
        return ((totals[0] + input_grad, totals[1] + output_grad, totals[2] + table_grad(grad_scores)), grad_piece)
    initial = (jnp.zeros((MODEL_WIDTH, 3 * MODEL_WIDTH), jnp.float32), jnp.zeros((MODEL_WIDTH, MODEL_WIDTH), jnp.float32), jnp.zeros(bias_dense.shape[:2] + (HEADS, BIAS_SLOTS), jnp.float32))
    totals, grad_groups = lax.scan(accumulate, initial, (grouped(windows), grouped(grad_windows)))
    return (from_windows(ungrouped(grad_groups, windows.shape)), totals[0], totals[1], totals[2])

def roll_fore(tokens_in):
    return jnp.roll(tokens_in, (-(WIN_LEVELS // 2), -(WIN_LAT // 2), -(WIN_LON // 2)), axis=(0, 1, 2))

def roll_back(tokens_in):
    return jnp.roll(tokens_in, (WIN_LEVELS // 2, WIN_LAT // 2, WIN_LON // 2), axis=(0, 1, 2))

def attention_front(block_in, gain_pair, input_weight, output_weight, bias_dense, shifted):
    normed = layer_norm(block_in.astype(jnp.float32), gain_pair[0]).astype(jnp.bfloat16)
    framed = roll_fore(normed) if shifted else normed
    attended = attention_forward(framed, bias_dense, input_weight, output_weight)
    if shifted:
        attended = roll_back(attended.astype(jnp.bfloat16)).astype(jnp.float32)
    middle = (block_in.astype(jnp.float32) + attended).astype(jnp.bfloat16)
    return (framed, middle)

def block_forward(block_in, gain_pair, input_weight, output_weight, expand_weight, reduce_weight, bias_dense, shifted):
    framed, middle = attention_front(block_in, gain_pair, input_weight, output_weight, bias_dense, shifted)
    normed_mid = layer_norm(middle.astype(jnp.float32), gain_pair[1]).astype(jnp.bfloat16)
    hidden = gelu_tanh(mix_tokens(normed_mid, expand_weight)).astype(jnp.bfloat16)
    return (middle.astype(jnp.float32) + mix_tokens(hidden, reduce_weight)).astype(jnp.bfloat16)

def block_grad(block_in, grad_in, gain_pair, input_weight, output_weight, expand_weight, reduce_weight, bias_dense, shifted):
    framed, middle = attention_front(block_in, gain_pair, input_weight, output_weight, bias_dense, shifted)
    normed_mid, mid_back = jax.vjp(layer_norm, middle.astype(jnp.float32), gain_pair[1])
    normed_mid_b = normed_mid.astype(jnp.bfloat16)
    hidden, gelu_back = jax.vjp(gelu_tanh, mix_tokens(normed_mid_b, expand_weight))
    hidden_b = hidden.astype(jnp.bfloat16)
    reduce_grad = grad_weight(hidden_b, grad_in)
    grad_pre = gelu_back(mix_back(grad_in, reduce_weight))[0].astype(jnp.bfloat16)
    expand_grad = grad_weight(normed_mid_b, grad_pre)
    grad_mid_norm, gain_mid_grad = mid_back(mix_back(grad_pre, expand_weight))
    grad_middle = grad_in.astype(jnp.float32) + grad_mid_norm
    grad_middle_b = grad_middle.astype(jnp.bfloat16)
    grad_attended = roll_fore(grad_middle_b) if shifted else grad_middle_b
    grad_framed, input_grad, output_grad, bias_grad = attention_backward(framed, bias_dense, input_weight, output_weight, grad_attended)
    grad_normed = grad_framed.astype(jnp.bfloat16)
    if shifted:
        grad_normed = roll_back(grad_normed)
    norm_back = jax.vjp(layer_norm, block_in.astype(jnp.float32), gain_pair[0])[1]
    grad_in_norm, gain_in_grad = norm_back(grad_normed.astype(jnp.float32))
    grad_out = (grad_middle + grad_in_norm).astype(jnp.bfloat16)
    return (grad_out, (input_grad, output_grad, expand_grad, reduce_grad, jnp.stack([gain_in_grad, gain_mid_grad]), bias_grad))

def reference(inputs, grad_output, norm_gains, input_weight, output_weight, expand_weight, reduce_weight, bias_table):
    grad_scale = float(LEVELS * LAT_ROWS * LON_COLS) ** (-0.5)
    section_grads = []
    section_parts = []
    for section_idx in range(SECTIONS):
        denses = [dense_bias(bias_table[section_idx, block], 0, LAT_ROWS, block % 2 == 1) for block in range(BLOCKS)]
        block_inputs = [inputs[section_idx]]
        for block in range(BLOCKS - 1):
            block_inputs.append(block_forward(block_inputs[-1], norm_gains[section_idx, block], input_weight[section_idx, block], output_weight[section_idx, block], expand_weight[section_idx, block], reduce_weight[section_idx, block], denses[block], block % 2 == 1))
        grad_flow = grad_output[section_idx]
        collected = [None] * BLOCKS
        for block in reversed(range(BLOCKS)):
            grad_flow, collected[block] = block_grad(block_inputs[block], grad_flow, norm_gains[section_idx, block], input_weight[section_idx, block], output_weight[section_idx, block], expand_weight[section_idx, block], reduce_weight[section_idx, block], denses[block], block % 2 == 1)
        section_grads.append(grad_flow)
        section_parts.append([jnp.stack([collected[block][index] for block in range(BLOCKS)]) for index in range(6)])
    upstream = jnp.stack(section_grads[1:] + [jnp.zeros_like(section_grads[0])])
    outputs = [jnp.stack([section_parts[section_idx][index] for section_idx in range(SECTIONS)]) for index in range(6)]
    return (upstream, outputs[0] * grad_scale, outputs[1] * grad_scale, outputs[2] * grad_scale, outputs[3] * grad_scale, outputs[4] * grad_scale, outputs[5])
```

```python
import jax
import jax.numpy as jnp
from jax import lax
from jax.sharding import PartitionSpec as P

MODEL_WIDTH = 192
HEADS = 6
HEAD_SIZE = 32
LEVELS = 8
WIN_LEVELS = 2
WIN_LAT = 6
WIN_LON = 12
BLOCKS = 2
LAT_DEV = 6
LON_DEV = 12
WIN_TOKENS = 144
BIAS_SLOTS = 3312


NORM_EPS = 1e-05
MASK_FILL = -10000.0


def swapped(value, axis, stride):
    mask = 2**stride
    pairs = [(source, source ^ mask) for source in range(lax.axis_size(axis))]
    return lax.ppermute(value, axis, pairs)


def from_behind(x, axis, by):
    size = lax.axis_size(axis)
    return lax.ppermute(x, axis, [(i, (i + by) % size) for i in range(size)])


def from_behind_2(x, axis, by):
    size = lax.axis_size(axis)
    pairs = [(i, i + by) for i in range(size) if 0 <= i + by < size]
    return lax.ppermute(x, axis, pairs)


def layer_norm(activity, gain_vec):
    centred = activity - jnp.mean(activity, axis=-1, keepdims=True)
    spread = jnp.mean(centred * centred, axis=-1, keepdims=True)
    return centred * lax.rsqrt(spread + NORM_EPS) * gain_vec


def gelu_tanh(activity):
    return jax.nn.gelu(activity, approximate=True)


def to_windows(tokens_in):
    levels_n, rows_n, cols_n, chans = tokens_in.shape
    shaped = tokens_in.reshape(
        levels_n // WIN_LEVELS,
        WIN_LEVELS,
        rows_n // WIN_LAT,
        WIN_LAT,
        cols_n // WIN_LON,
        WIN_LON,
        chans,
    )
    shaped = shaped.transpose(0, 2, 4, 1, 3, 5, 6)
    return shaped.reshape(
        levels_n // WIN_LEVELS, rows_n // WIN_LAT, cols_n // WIN_LON, WIN_TOKENS, chans
    )


def from_windows(blocks_in):
    level_w, lat_w, lon_w, _, chans = blocks_in.shape
    shaped = blocks_in.reshape(level_w, lat_w, lon_w, WIN_LEVELS, WIN_LAT, WIN_LON, chans)
    shaped = shaped.transpose(0, 3, 1, 4, 2, 5, 6)
    return shaped.reshape(level_w * WIN_LEVELS, lat_w * WIN_LAT, lon_w * WIN_LON, chans)


def pair_map():
    offsets = 2 * WIN_LON - 1
    group_count = WIN_LEVELS * WIN_LAT
    inner = jnp.arange(group_count * offsets, dtype=jnp.int32)
    inner_group = inner // offsets
    inner_off = inner % offsets
    keys_all = jnp.arange(WIN_TOKENS, dtype=jnp.int32)
    key_group = keys_all // WIN_LON
    key_col = keys_all % WIN_LON
    query_col = jnp.arange(WIN_LON, dtype=jnp.int32)
    same_group = inner_group[:, None, None] == key_group[None, None, :]
    same_off = (
        inner_off[:, None, None] == query_col[None, :, None] - key_col[None, None, :] + WIN_LON - 1
    )
    table = jnp.logical_and(same_group, same_off).astype(jnp.float32)
    return table.reshape(group_count * offsets, WIN_LON * WIN_TOKENS)


def region(position, extent, window_len):
    return jnp.where(
        position < extent - window_len, 0, jnp.where(position < extent - window_len // 2, 1, 2)
    ).astype(jnp.int32)


def dense_bias(table_rows, spread_map, first_row, lat_total, shifted):
    leading = table_rows.shape[:-1]
    group_count = WIN_LEVELS * WIN_LAT
    rows = table_rows.reshape(
        leading + (WIN_LEVELS, WIN_LEVELS, WIN_LAT, WIN_LAT * (2 * WIN_LON - 1))
    )
    rows = jnp.swapaxes(rows, -3, -2)
    rows = rows.reshape(leading + (group_count, group_count * (2 * WIN_LON - 1)))
    spread = jnp.einsum("...rg,gm->...rm", rows, spread_map, precision=lax.Precision.HIGHEST)
    bias_dense = spread.reshape(leading + (WIN_TOKENS, WIN_TOKENS))
    if shifted:
        local_rows = table_rows.shape[1] * WIN_LAT
        level_ids = region(jnp.arange(LEVELS, dtype=jnp.int32), LEVELS, WIN_LEVELS)
        row_ids = region(first_row + jnp.arange(local_rows, dtype=jnp.int32), lat_total, WIN_LAT)
        region_ids = level_ids[:, None] * 3 + row_ids[None, :]
        region_grid = jnp.broadcast_to(
            region_ids[:, :, None, None], (LEVELS, local_rows, WIN_LON, 1)
        )
        token_ids = to_windows(region_grid)[:, :, 0, :, 0]
        matched = token_ids[..., :, None] == token_ids[..., None, :]
        bias_dense = bias_dense + jnp.where(matched, 0.0, MASK_FILL).astype(jnp.float32)[:, :, None]
    return bias_dense[:, :, None]


def mix_tokens(tokens_in, weight):
    token_rows = tokens_in.reshape(-1, tokens_in.shape[-1])
    result = jnp.dot(token_rows, weight, preferred_element_type=jnp.float32)
    return result.reshape(tokens_in.shape[:-1] + (weight.shape[1],))


def mix_back(tokens_in, weight):
    token_rows = tokens_in.reshape(-1, tokens_in.shape[-1])
    result = lax.dot_general(
        token_rows, weight, (((1,), (1,)), ((), ())), preferred_element_type=jnp.float32
    )
    return result.reshape(tokens_in.shape[:-1] + (weight.shape[0],))


def grad_weight(tokens_in, grad_in):
    token_rows = tokens_in.reshape(-1, tokens_in.shape[-1])
    grad_rows = grad_in.reshape(-1, grad_in.shape[-1])
    return lax.dot_general(
        token_rows, grad_rows, (((0,), (0,)), ((), ())), preferred_element_type=jnp.float32
    )


def table_grad(grad_scores, spread_map):
    summed = jnp.sum(grad_scores, axis=2)
    leading = summed.shape[:3]
    group_count = WIN_LEVELS * WIN_LAT
    shaped = summed.reshape(leading + (group_count, WIN_LON * WIN_TOKENS))
    folded = jnp.einsum("...rm,gm->...rg", shaped, spread_map, precision=lax.Precision.HIGHEST)
    folded = folded.reshape(
        leading + (WIN_LEVELS, WIN_LAT, WIN_LEVELS, WIN_LAT * (2 * WIN_LON - 1))
    )
    folded = jnp.swapaxes(folded, -3, -2)
    return folded.reshape(leading + (BIAS_SLOTS,))


def token_major(head_major):
    leading = head_major.shape[:-3]
    merged = head_major.reshape(
        leading + (head_major.shape[-3] * head_major.shape[-2], head_major.shape[-1])
    )
    return jnp.swapaxes(merged, -1, -2)


def attend_forward(windows, bias_dense, input_weight, output_weight):
    leading = windows.shape[:-2]
    token_rows = windows.reshape(-1, MODEL_WIDTH)
    projected = jnp.dot(token_rows, input_weight, preferred_element_type=jnp.float32)
    column_scale = jnp.where(
        jnp.arange(3 * MODEL_WIDTH) < MODEL_WIDTH, HEAD_SIZE ** (-0.5), 1.0
    ).astype(jnp.float32)
    projected_b = (projected * column_scale).astype(jnp.bfloat16)
    heads_all = jnp.swapaxes(projected_b.reshape(leading + (WIN_TOKENS, 3 * MODEL_WIDTH)), -1, -2)
    heads_all = heads_all.reshape(leading + (3, HEADS, HEAD_SIZE, WIN_TOKENS))
    queries = heads_all[..., 0, :, :, :]
    key_part = heads_all[..., 1, :, :, :]
    values = heads_all[..., 2, :, :, :]
    scores = (
        jnp.einsum("...heq,...hek->...hqk", queries, key_part, preferred_element_type=jnp.float32)
        + bias_dense
    )
    attention = jax.nn.softmax(scores, axis=-1)
    weights = attention.astype(jnp.bfloat16)
    mixture_heads = jnp.einsum(
        "...hqk,...hek->...heq", weights, values, preferred_element_type=jnp.float32
    ).astype(jnp.bfloat16)
    mixture = token_major(mixture_heads)
    attended = jnp.dot(
        mixture.reshape(-1, MODEL_WIDTH), output_weight, preferred_element_type=jnp.float32
    )
    return (
        attended.reshape(windows.shape),
        (token_rows, queries, key_part, values, attention, weights, mixture),
    )


def attend_backward(saved, grad_windows_in, input_weight, output_weight):
    token_rows, queries, key_part, values, attention, weights, mixture = saved
    leading = grad_windows_in.shape[:-2]
    grad_rows = grad_windows_in.reshape(-1, MODEL_WIDTH)
    output_grad = grad_weight(mixture.reshape(-1, MODEL_WIDTH), grad_rows)
    grad_mixture = (
        mix_back(grad_rows, output_weight)
        .astype(jnp.bfloat16)
        .reshape(leading + (WIN_TOKENS, MODEL_WIDTH))
    )
    grad_mixture = jnp.swapaxes(grad_mixture, -1, -2).reshape(
        leading + (HEADS, HEAD_SIZE, WIN_TOKENS)
    )
    grad_values = jnp.einsum(
        "...hqk,...heq->...hek", weights, grad_mixture, preferred_element_type=jnp.float32
    )
    grad_weights = jnp.einsum(
        "...heq,...hek->...hqk", grad_mixture, values, preferred_element_type=jnp.float32
    )
    grad_scores = attention * (
        grad_weights - jnp.sum(attention * grad_weights, axis=-1, keepdims=True)
    )
    score_part = grad_scores.astype(jnp.bfloat16)
    grad_queries = jnp.einsum(
        "...hqk,...hek->...heq", score_part, key_part, preferred_element_type=jnp.float32
    ) * HEAD_SIZE ** (-0.5)
    grad_keys = jnp.einsum(
        "...hqk,...heq->...hek", score_part, queries, preferred_element_type=jnp.float32
    )
    grad_heads = jnp.stack([grad_queries, grad_keys, grad_values], axis=-4).astype(jnp.bfloat16)
    grad_projected = token_major(
        grad_heads.reshape(leading + (3 * HEADS, HEAD_SIZE, WIN_TOKENS))
    ).reshape(-1, 3 * MODEL_WIDTH)
    input_grad = grad_weight(token_rows, grad_projected)
    grad_windows = mix_back(grad_projected, input_weight).reshape(grad_windows_in.shape)
    return (grad_windows, input_grad, output_grad, grad_scores)


def lat_trade(edge_rows):
    return swapped(edge_rows, "lat", 0)


def roll_fore(tokens_in):
    half_rows = WIN_LAT // 2
    half_cols = WIN_LON // 2
    moved = jnp.roll(tokens_in, -(WIN_LEVELS // 2), axis=0)
    incoming = lat_trade(moved[:, :half_rows])
    moved = jnp.concatenate([moved[:, half_rows:], incoming], axis=1)
    incoming = from_behind(moved[:, :, :half_cols], "lon", -1)
    return jnp.concatenate([moved[:, :, half_cols:], incoming], axis=2)


def roll_back(tokens_in):
    half_rows = WIN_LAT // 2
    half_cols = WIN_LON // 2
    moved = jnp.roll(tokens_in, WIN_LEVELS // 2, axis=0)
    incoming = from_behind(moved[:, :, -half_cols:], "lon", 1)
    moved = jnp.concatenate([incoming, moved[:, :, :-half_cols]], axis=2)
    incoming = lat_trade(moved[:, -half_rows:])
    return jnp.concatenate([incoming, moved[:, :-half_rows]], axis=1)


def block_forward(
    block_in,
    gain_pair,
    input_weight,
    output_weight,
    expand_weight,
    reduce_weight,
    bias_dense,
    shifted,
):
    block_f = block_in.astype(jnp.float32)
    normed, norm_back = jax.vjp(layer_norm, block_f, gain_pair[0])
    normed_b = normed.astype(jnp.bfloat16)
    framed = roll_fore(normed_b) if shifted else normed_b
    attended, attn_saved = attend_forward(
        to_windows(framed), bias_dense, input_weight, output_weight
    )
    attended = from_windows(attended)
    if shifted:
        attended = roll_back(attended.astype(jnp.bfloat16)).astype(jnp.float32)
    middle = (block_f + attended).astype(jnp.bfloat16)
    middle_f = middle.astype(jnp.float32)
    normed_mid, mid_back = jax.vjp(layer_norm, middle_f, gain_pair[1])
    normed_mid_b = normed_mid.astype(jnp.bfloat16)
    hidden, gelu_back = jax.vjp(gelu_tanh, mix_tokens(normed_mid_b, expand_weight))
    hidden_b = hidden.astype(jnp.bfloat16)
    output = (middle_f + mix_tokens(hidden_b, reduce_weight)).astype(jnp.bfloat16)
    return (output, (norm_back, attn_saved, mid_back, normed_mid_b, gelu_back, hidden_b))


def block_backward(
    saved, grad_in, input_weight, output_weight, expand_weight, reduce_weight, spread_map, shifted
):
    norm_back, attn_saved, mid_back, normed_mid_b, gelu_back, hidden_b = saved
    reduce_grad = grad_weight(hidden_b, grad_in)
    grad_pre = gelu_back(mix_back(grad_in, reduce_weight))[0].astype(jnp.bfloat16)
    expand_grad = grad_weight(normed_mid_b, grad_pre)
    grad_mid_norm, gain_mid_grad = mid_back(mix_back(grad_pre, expand_weight))
    grad_middle = grad_in.astype(jnp.float32) + grad_mid_norm
    grad_middle_b = grad_middle.astype(jnp.bfloat16)
    grad_attended = roll_fore(grad_middle_b) if shifted else grad_middle_b
    grad_windows, input_grad, output_grad, grad_scores = attend_backward(
        attn_saved, to_windows(grad_attended), input_weight, output_weight
    )
    grad_normed = from_windows(grad_windows).astype(jnp.bfloat16)
    if shifted:
        grad_normed = roll_back(grad_normed)
    grad_in_norm, gain_in_grad = norm_back(grad_normed.astype(jnp.float32))
    grad_out = (grad_middle + grad_in_norm).astype(jnp.bfloat16)
    return (
        grad_out,
        (
            input_grad,
            output_grad,
            expand_grad,
            reduce_grad,
            jnp.stack([gain_in_grad, gain_mid_grad]),
            table_grad(grad_scores, spread_map),
        ),
    )


def on_device(
    inputs,
    grad_output,
    norm_gains,
    input_weight,
    output_weight,
    expand_weight,
    reduce_weight,
    bias_table,
):
    lat_index = lax.axis_index("lat")
    window_rows = LAT_DEV // WIN_LAT
    lat_total = LAT_DEV * lax.axis_size("lat")
    first_row = lat_index * LAT_DEV
    first_window = lat_index * window_rows
    spread_map = pair_map()
    savings = []
    block_in = inputs[0]
    for block in range(BLOCKS):
        table_rows = lax.dynamic_slice_in_dim(
            bias_table[0, block], first_window, window_rows, axis=1
        )
        bias_dense = dense_bias(table_rows, spread_map, first_row, lat_total, block % 2 == 1)
        block_in, saved = block_forward(
            block_in,
            norm_gains[0, block],
            input_weight[0, block],
            output_weight[0, block],
            expand_weight[0, block],
            reduce_weight[0, block],
            bias_dense,
            block % 2 == 1,
        )
        savings.append(saved)
    grad_flow = grad_output[0]
    collected = [None] * BLOCKS
    for block in reversed(range(BLOCKS)):
        grad_flow, collected[block] = block_backward(
            savings[block],
            grad_flow,
            input_weight[0, block],
            output_weight[0, block],
            expand_weight[0, block],
            reduce_weight[0, block],
            spread_map,
            block % 2 == 1,
        )
    stacked = [
        jnp.stack([collected[block][index] for block in range(BLOCKS)]) for index in range(6)
    ]
    grad_scale = float(LEVELS * lat_total * LON_DEV * lax.axis_size("lon")) ** (-0.5)
    sums = reduce_grads(stacked)
    upstream = from_behind_2(grad_flow, "section", -1)
    return (upstream[None],) + tuple(
        (total * grad_scale)[None] for total in sums[:5]
    ) + (sums[5][None],)


def reduce_grads(stacked):
    ring = lax.axis_size("lon")
    shapes = [piece.shape for piece in stacked]
    sizes = [piece.size for piece in stacked]
    flat = jnp.concatenate([piece.reshape(-1).astype(jnp.bfloat16) for piece in stacked])
    total = flat.size
    chunk = -(-total // (ring * 2048)) * 2048
    flat = jnp.pad(flat, (0, chunk * ring - total)).reshape(ring, chunk // 128, 128)
    spread = lax.all_to_all(flat, "lon", split_axis=0, concat_axis=0, tiled=True)
    mine = jnp.sum(spread.astype(jnp.float32), axis=0).astype(jnp.bfloat16)
    other = lat_trade(mine)
    is_first = lax.axis_index("lat") == 0
    pair = jnp.stack([jnp.where(is_first, mine, other), jnp.where(is_first, other, mine)])
    pair = jnp.broadcast_to(pair[None], (ring,) + pair.shape)
    whole = lax.all_to_all(pair, "lon", split_axis=0, concat_axis=0, tiled=True)
    halves = whole.swapaxes(0, 1).reshape(2, -1)[:, :total].astype(jnp.float32)
    both = halves[0] + halves[1]
    results = []
    offset = 0
    for index in range(5):
        results.append(both[offset : offset + sizes[index]].reshape(shapes[index]))
        offset += sizes[index]
    tables = halves[:, offset : offset + sizes[5]].reshape((2,) + shapes[5])
    results.append(jnp.concatenate([tables[0], tables[1]], axis=2))
    return results


def solution(mesh):
    return jax.shard_map(
        on_device,
        mesh=mesh,
        in_specs=(
            P("section", None, "lat", "lon", None),
            P("section", None, "lat", "lon", None),
            P("section", None, None, None),
            P("section", None, None, None),
            P("section", None, None, None),
            P("section", None, None, None),
            P("section", None, None, None),
            P("section", None, None, None, None, None),
        ),
        out_specs=(
            P("section", None, "lat", "lon", None),
            P("section", None, None, None),
            P("section", None, None, None),
            P("section", None, None, None),
            P("section", None, None, None),
            P("section", None, None, None),
            P("section", None, None, None, None, None),
        ),
        check_vma=False,
    )
```

```python
import functools

import jax
import jax.numpy as jnp
import numpy as np
from jax import lax
from jax.experimental import pallas as pl
from jax.experimental.pallas import tpu as pltpu
from jax.sharding import PartitionSpec as P

MODEL_WIDTH = 192
HEADS = 6
HEAD_SIZE = 32
LEVELS = 8
WIN_LEVELS = 2
WIN_LAT = 6
WIN_LON = 12
BLOCKS = 2
MLP_WIDTH = 768
LAT_DEV = 6
LON_DEV = 12
LEVEL_WINDOWS = 4
WIN_TOKENS = 144
BIAS_SLOTS = 3312

NORM_EPS = 1e-05
MASK_FILL = -10000.0
GELU_C = 0.7978845608028654
GELU_A = 0.044715

TOKENS = LEVELS * LAT_DEV * LON_DEV
QUAD = TOKENS // 4
STACK = HEADS * WIN_TOKENS
GROUPS = WIN_LEVELS * WIN_LAT
OFFSETS = 2 * WIN_LON - 1
PAIR_LANES = GROUPS * OFFSETS
PAIR_PAD = 384
TYPE_ROWS = LEVEL_WINDOWS * HEADS * GROUPS
WEIGHT_ROWS = 3456
TABLE_ROWS = 624
PACK_ROWS = 4096

F32 = jnp.float32
BF16 = jnp.bfloat16


def quad_orders():
    level, row, col = np.meshgrid(
        np.arange(LEVELS), np.arange(LAT_DEV), np.arange(LON_DEV), indexing="ij"
    )
    half_rows, half_cols = WIN_LAT // 2, WIN_LON // 2
    quad = (1 - row // half_rows) * 2 + (1 - col // half_cols)
    place = (quad * LEVELS + level) * (half_rows * half_cols)
    place = place + (row % half_rows) * half_cols + col % half_cols
    split = place.reshape(-1)
    quad_r = (row // half_rows) * 2 + col // half_cols
    from_level = (level + WIN_LEVELS // 2) % LEVELS
    place_r = (quad_r * LEVELS + from_level) * (half_rows * half_cols)
    place_r = place_r + (row % half_rows) * half_cols + col % half_cols
    split_rolled = place_r.reshape(-1)
    join = np.argsort(split)
    join_rolled = np.argsort(split_rolled)
    return [order.astype(np.int32)[None, :] for order in (split, join_rolled, split_rolled, join)]


def dot_nn(a, b):
    return jnp.dot(a, b, preferred_element_type=F32)


def dot_nt(a, b):
    return lax.dot_general(a, b, (((1,), (1,)), ((), ())), preferred_element_type=F32)


def dot_tn(a, b):
    return lax.dot_general(a, b, (((0,), (0,)), ((), ())), preferred_element_type=F32)


def reorder(values, order_row):
    rows = lax.broadcasted_iota(jnp.int32, (TOKENS, TOKENS), 0)
    pick = jnp.where(rows == order_row, 1.0, 0.0).astype(BF16)
    return dot_nn(pick, values).astype(BF16)


def norm_stats(values):
    centred = values - jnp.mean(values, axis=-1, keepdims=True)
    spread = jnp.mean(centred * centred, axis=-1, keepdims=True)
    inv = lax.rsqrt(spread + NORM_EPS)
    return centred * inv, inv


def norm_grad(grad, unit, inv, gain_row):
    gain_grad = jnp.sum(grad * unit, axis=0, keepdims=True)
    grad_unit = grad * gain_row
    first = jnp.mean(grad_unit, axis=-1, keepdims=True)
    second = jnp.mean(grad_unit * unit, axis=-1, keepdims=True)
    return inv * (grad_unit - first - unit * second), gain_grad


def head_masks():
    lane = lax.broadcasted_iota(jnp.int32, (1, MODEL_WIDTH), 1)
    return [
        jnp.logical_and(lane >= h * HEAD_SIZE, lane < (h + 1) * HEAD_SIZE) for h in range(HEADS)
    ]


def stack_heads(values, masks):
    wide = values.astype(F32)
    return jnp.concatenate([jnp.where(m, wide, 0.0) for m in masks], axis=0).astype(BF16)


def fold_heads(stacked, masks):
    total = jnp.where(masks[0], stacked[:WIN_TOKENS], 0.0)
    for h in range(1, HEADS):
        total = jnp.where(masks[h], stacked[h * WIN_TOKENS : (h + 1) * WIN_TOKENS], total)
    return total


def pair_pick(query_col):
    key = lax.broadcasted_iota(jnp.int32, (256, PAIR_PAD), 0)
    lane = lax.broadcasted_iota(jnp.int32, (256, PAIR_PAD), 1)
    group = lax.shift_right_logical(key * 5462, 16)
    key_col = key - group * WIN_LON
    target = group * OFFSETS + (WIN_LON - 1 + query_col) - key_col
    hit = jnp.logical_and(lane == target, key < WIN_TOKENS)
    return jnp.where(hit, 1.0, 0.0).astype(BF16)


def build_bias(table, bias_a, bias_b):
    high = table.astype(BF16)
    rest = table - high.astype(F32)
    middle = rest.astype(BF16)
    low = (rest - middle.astype(F32)).astype(BF16)
    for query_col in range(WIN_LON):
        pick = pair_pick(query_col)
        spread = dot_nt(high, pick) + dot_nt(middle, pick) + dot_nt(low, pick)
        bias_a[pl.ds(query_col, TYPE_ROWS, stride=WIN_LON), :] = spread[:, :128]
        bias_b[pl.ds(query_col, TYPE_ROWS, stride=WIN_LON), :] = spread[:, 128:]


def fold_table(score_a, score_b):
    total = jnp.zeros((TYPE_ROWS, PAIR_PAD), F32)
    for query_col in range(WIN_LON):
        pick = pair_pick(query_col)
        left = score_a[pl.ds(query_col, TYPE_ROWS, stride=WIN_LON), :]
        right = score_b[pl.ds(query_col, TYPE_ROWS, stride=WIN_LON), :]
        total = total + dot_nn(left.astype(BF16), pick[:128])
        total = total + dot_nn(right.astype(BF16), pick[128:])
    return total


def shift_mask(window, lat_row):
    shape = (WIN_TOKENS, WIN_TOKENS)
    half = WIN_TOKENS // 2
    parts = []
    for axis in (0, 1):
        token = lax.broadcasted_iota(jnp.int32, shape, axis)
        upper = token >= half
        inner = jnp.where(upper, token - half, token)
        parts.append((upper, inner >= half // 2))
    rows_differ = jnp.where(parts[0][1] != parts[1][1], 1.0, 0.0) * lat_row
    if window == LEVEL_WINDOWS - 1:
        levels_differ = jnp.where(parts[0][0] != parts[1][0], 1.0, 0.0)
        rows_differ = jnp.maximum(rows_differ, levels_differ)
    return rows_differ * MASK_FILL


def attention_front(unit, gain_row, input_weight, bias_a, bias_b, lat_row, q_ref, k_ref, v_ref, w_ref, mix_ref):
    normed = (unit * gain_row).astype(BF16)
    q_ref[...] = (dot_nn(normed, input_weight[:, :MODEL_WIDTH]) * HEAD_SIZE ** (-0.5)).astype(BF16)
    k_ref[...] = dot_nn(normed, input_weight[:, MODEL_WIDTH : 2 * MODEL_WIDTH]).astype(BF16)
    v_ref[...] = dot_nn(normed, input_weight[:, 2 * MODEL_WIDTH :]).astype(BF16)
    masks = head_masks()
    for window in range(LEVEL_WINDOWS):
        rows = pl.ds(window * WIN_TOKENS, WIN_TOKENS)
        stack_rows = pl.ds(window * STACK, STACK)
        queries = stack_heads(q_ref[rows, :], masks)
        scores = dot_nt(queries, k_ref[rows, :])
        bias = jnp.concatenate(
            [bias_a[stack_rows, :], bias_b[stack_rows, :][:, : WIN_TOKENS - 128]], axis=1
        )
        scores = scores + bias
        if lat_row is not None:
            mask = shift_mask(window, lat_row)
            scores = scores + jnp.concatenate([mask] * HEADS, axis=0)
        scores = jnp.exp(scores - jnp.max(scores, axis=-1, keepdims=True))
        weights = (scores / jnp.sum(scores, axis=-1, keepdims=True)).astype(BF16)
        w_ref[stack_rows, :] = weights
        mixed = dot_nn(weights, v_ref[rows, :])
        mix_ref[rows, :] = fold_heads(mixed, masks).astype(BF16)
    return normed


def gelu_parts(pre):
    square = pre * pre
    tanh = jnp.tanh(GELU_C * (pre + GELU_A * pre * square))
    half = 0.5 * (1.0 + tanh)
    slope = half + 0.5 * pre * (1.0 - tanh * tanh) * (GELU_C * (1.0 + 3.0 * GELU_A * square))
    return pre * half, slope


def pack_columns(out_ref, first, values):
    rows, lanes = values.shape
    for block in range(lanes // 128):
        out_ref[pl.ds(first + block * rows, rows), :] = values[:, block * 128 : (block + 1) * 128].astype(BF16)


def backward(e, x_unit, x_inv, gains, middle, weights4, saved, scores_ab, pack_ref, gproj_ref):
    input_weight, output_weight, expand_weight, reduce_weight = weights4
    q_ref, k_ref, v_ref, w_ref, mix_ref = saved
    score_a, score_b = scores_ab
    masks = head_masks()
    mid_unit, mid_inv = norm_stats(middle.astype(F32))
    gain_mid = gains[1:2, :]
    normed_mid = (mid_unit * gain_mid).astype(BF16)
    hidden, slope = gelu_parts(dot_nn(normed_mid, expand_weight))
    hidden = hidden.astype(BF16)
    grad_pre = (slope * dot_nt(e, reduce_weight)).astype(BF16)
    reduce_grad = dot_tn(hidden, e)
    half_mlp = MLP_WIDTH // 2
    pack_columns(
        pack_ref, 2304, jnp.concatenate([reduce_grad[:half_mlp], reduce_grad[half_mlp:]], axis=1)
    )
    pack_columns(pack_ref, 1152, dot_tn(normed_mid, grad_pre))
    grad_norm, gain_mid_grad = norm_grad(dot_nt(grad_pre, expand_weight), mid_unit, mid_inv, gain_mid)
    grad_middle = e.astype(F32) + grad_norm
    grad_attended = grad_middle.astype(BF16)
    output_grad = dot_tn(mix_ref[...], grad_attended)
    grad_mixture = dot_nt(grad_attended, output_weight).astype(BF16)
    for window in range(LEVEL_WINDOWS):
        base = window * WIN_TOKENS
        rows = pl.ds(base, WIN_TOKENS)
        stack_rows = pl.ds(window * STACK, STACK)
        queries = stack_heads(q_ref[rows, :], masks)
        grads = stack_heads(grad_mixture[base : base + WIN_TOKENS], masks)
        weights = w_ref[stack_rows, :]
        keys = k_ref[rows, :]
        gproj_ref[2, rows, :] = dot_tn(weights, grads).astype(BF16)
        grad_weights = dot_nt(grads, v_ref[rows, :])
        attention = weights.astype(F32)
        moved = attention * grad_weights
        grad_scores = attention * (grad_weights - jnp.sum(moved, axis=-1, keepdims=True))
        score_a[stack_rows, :] = grad_scores[:, :128]
        score_b[stack_rows, :] = jnp.concatenate(
            [grad_scores[:, 128:], jnp.zeros((STACK, 256 - WIN_TOKENS), F32)], axis=1
        )
        score_part = grad_scores.astype(BF16)
        grad_queries = fold_heads(dot_nn(score_part, keys), masks) * HEAD_SIZE ** (-0.5)
        gproj_ref[0, rows, :] = grad_queries.astype(BF16)
        gproj_ref[1, rows, :] = dot_tn(score_part, queries).astype(BF16)
    normed = (x_unit * gains[0:1, :]).astype(BF16)
    parts = [gproj_ref[part] for part in range(3)]
    weight_grads = [dot_tn(normed, part) for part in parts] + [output_grad]
    pack_columns(pack_ref, 0, jnp.concatenate(weight_grads, axis=1))
    grad_normed = dot_nt(parts[0], input_weight[:, :MODEL_WIDTH])
    grad_normed = grad_normed + dot_nt(parts[1], input_weight[:, MODEL_WIDTH : 2 * MODEL_WIDTH])
    grad_normed = grad_normed + dot_nt(parts[2], input_weight[:, 2 * MODEL_WIDTH :])
    grad_normed = grad_normed.astype(BF16).astype(F32)
    grad_in, gain_in_grad = norm_grad(grad_normed, x_unit, x_inv, gains[0:1, :])
    folded = fold_table(score_a, score_b)
    pack_columns(pack_ref, WEIGHT_ROWS, folded[:, :256])
    rest_rows = []
    for window in range(LEVEL_WINDOWS):
        pieces = [
            folded[(window * HEADS + h) * GROUPS : (window * HEADS + h + 1) * GROUPS, 256:PAIR_LANES]
            for h in range(HEADS)
        ]
        pieces.append(jnp.zeros((GROUPS, 128 - HEADS * (PAIR_LANES - 256)), F32))
        rest_rows.append(jnp.concatenate(pieces, axis=1))
    gain_flat = jnp.concatenate([gain_in_grad, gain_mid_grad], axis=1)
    gain_rows = [gain_flat[:, i * 128 : (i + 1) * 128] for i in range(3)]
    tail = rest_rows + gain_rows + [jnp.zeros((13, 128), F32)]
    pack_ref[pl.ds(WEIGHT_ROWS + 2 * TYPE_ROWS, 64), :] = jnp.concatenate(tail, axis=0).astype(BF16)
    return (grad_middle + grad_in).astype(BF16)


def forward_kernel(
    x_ref, gains_ref, wi_ref, wo_ref, we_ref, wr_ref, table_ref, order_ref,
    quad0, quad1, quad2, quad3, q_ref, k_ref, v_ref, w_ref, mix_ref, mid_ref,
    bias_a, bias_b,
):
    build_bias(table_ref[...], bias_a, bias_b)
    gains = gains_ref[...]
    values = x_ref[...].astype(F32)
    unit, _ = norm_stats(values)
    attention_front(
        unit, gains[0:1, :], wi_ref[...], bias_a, bias_b, None, q_ref, k_ref, v_ref, w_ref, mix_ref
    )
    middle = (values + dot_nn(mix_ref[...], wo_ref[...])).astype(BF16)
    mid_ref[...] = middle
    mid_f = middle.astype(F32)
    mid_unit, _ = norm_stats(mid_f)
    normed_mid = (mid_unit * gains[1:2, :]).astype(BF16)
    hidden, _ = gelu_parts(dot_nn(normed_mid, we_ref[...]))
    output = (mid_f + dot_nn(hidden.astype(BF16), wr_ref[...])).astype(BF16)
    quads = reorder(output, order_ref[...])
    for index, quad in enumerate((quad0, quad1, quad2, quad3)):
        quad[...] = quads[index * QUAD : (index + 1) * QUAD]


def turn_kernel(
    x0, x1, x2, x3, e0, e1, e2, e3, lat_ref, gains_ref, wi_ref, wo_ref, we_ref, wr_ref, table_ref,
    join_ref, split_ref, quad0, quad1, quad2, quad3, pack_ref,
    bias_a, bias_b, q_ref, k_ref, v_ref, w_ref, mix_ref, gproj_ref,
):
    build_bias(table_ref[...], bias_a, bias_b)
    gains = gains_ref[...]
    join = join_ref[...]
    block_in = reorder(jnp.concatenate([x0[...], x1[...], x2[...], x3[...]], axis=0), join)
    e = reorder(jnp.concatenate([e0[...], e1[...], e2[...], e3[...]], axis=0), join)
    values = block_in.astype(F32)
    unit, inv = norm_stats(values)
    input_weight, output_weight = wi_ref[...], wo_ref[...]
    attention_front(
        unit, gains[0:1, :], input_weight, bias_a, bias_b, lat_ref[0:1, 0:1], q_ref, k_ref, v_ref,
        w_ref, mix_ref,
    )
    attended = dot_nn(mix_ref[...], output_weight).astype(BF16).astype(F32)
    middle = (values + attended).astype(BF16)
    result = backward(
        e, unit, inv, gains, middle, (input_weight, output_weight, we_ref[...], wr_ref[...]),
        (q_ref, k_ref, v_ref, w_ref, mix_ref), (bias_a, bias_b), pack_ref, gproj_ref,
    )
    quads = reorder(result, split_ref[...])
    for index, quad in enumerate((quad0, quad1, quad2, quad3)):
        quad[...] = quads[index * QUAD : (index + 1) * QUAD]


def backward_kernel(
    x_ref, e0, e1, e2, e3, gains_ref, wi_ref, wo_ref, we_ref, wr_ref, join_ref,
    q_ref, k_ref, v_ref, w_ref, mix_ref, mid_ref, out_ref, pack_ref, score_a, score_b, gproj_ref,
):
    e = reorder(jnp.concatenate([e0[...], e1[...], e2[...], e3[...]], axis=0), join_ref[...])
    unit, inv = norm_stats(x_ref[...].astype(F32))
    out_ref[...] = backward(
        e, unit, inv, gains_ref[...], mid_ref[...],
        (wi_ref[...], wo_ref[...], we_ref[...], wr_ref[...]),
        (q_ref, k_ref, v_ref, w_ref, mix_ref), (score_a, score_b), pack_ref, gproj_ref,
    )


LIMIT = 60 * 1024 * 1024
TOKEN_SHAPE = jax.ShapeDtypeStruct((TOKENS, MODEL_WIDTH), BF16)
QUAD_SHAPE = jax.ShapeDtypeStruct((QUAD, MODEL_WIDTH), BF16)
WEIGHT_SHAPE = jax.ShapeDtypeStruct((LEVEL_WINDOWS * STACK, WIN_TOKENS), BF16)
PACK_SHAPE = jax.ShapeDtypeStruct((PACK_ROWS, 128), BF16)


def tall_scratch():
    return pltpu.VMEM((LEVEL_WINDOWS * STACK, 128), F32)


def token_scratch():
    return pltpu.VMEM((TOKENS, MODEL_WIDTH), BF16)


def call(kernel, outs, scratch, *args):
    return pl.pallas_call(
        kernel,
        out_shape=outs,
        scratch_shapes=scratch,
        compiler_params=pltpu.CompilerParams(vmem_limit_bytes=LIMIT),
    )(*args)


def exchange(quads, by):
    ring, sides = lax.axis_size("lon"), lax.axis_size("lat")
    lon_pairs = [(i, (i + by) % ring) for i in range(ring)]
    swap = [(i, i ^ 1) for i in range(sides)]
    both = [
        (i * sides + j, ((i + by) % ring) * sides + (j ^ 1)) for i in range(ring) for j in range(sides)
    ]
    return (
        quads[0],
        lax.ppermute(quads[1], "lon", lon_pairs),
        lax.ppermute(quads[2], "lat", swap),
        lax.ppermute(quads[3], ("lon", "lat"), both),
    )


def pair_rows(tables):
    shaped = tables.reshape(
        BLOCKS, LEVEL_WINDOWS, HEADS, WIN_LEVELS, WIN_LEVELS, WIN_LAT, WIN_LAT * OFFSETS
    )
    shaped = shaped.swapaxes(4, 5).reshape(BLOCKS, TYPE_ROWS, PAIR_LANES)
    return jnp.pad(shaped, ((0, 0), (0, 0), (0, PAIR_PAD - PAIR_LANES)))


def reduce_packs(pack):
    ring = lax.axis_size("lon")
    spread = lax.all_to_all(
        pack.reshape(ring, PACK_ROWS // ring, 128), "lon", split_axis=0, concat_axis=0, tiled=True
    )
    mine = jnp.sum(spread.astype(F32), axis=0).astype(BF16)
    other = lax.ppermute(mine, "lat", [(0, 1), (1, 0)])
    first = lax.axis_index("lat") == 0
    pair = jnp.stack([jnp.where(first, mine, other), jnp.where(first, other, mine)])
    pair = jnp.broadcast_to(pair[None], (ring,) + pair.shape)
    whole = lax.all_to_all(pair, "lon", split_axis=0, concat_axis=0, tiled=True)
    return whole.swapaxes(0, 1).reshape(2, PACK_ROWS, 128).astype(F32)


def columns(values, first, rows, blocks):
    part = values[first : first + rows * blocks].reshape(blocks, rows, 128)
    return part.swapaxes(0, 1).reshape(rows, blocks * 128)


def unpack(halves):
    both = halves[0, :WEIGHT_ROWS] + halves[1, :WEIGHT_ROWS]
    front = columns(both, 0, MODEL_WIDTH, 6)
    expand = columns(both, 1152, MODEL_WIDTH, 6)
    tall = columns(both, 2304, MLP_WIDTH // 2, 3)
    reduce = jnp.concatenate([tall[:, :MODEL_WIDTH], tall[:, MODEL_WIDTH:]], axis=0)
    tables = []
    for side in range(2):
        wide = columns(halves[side], WEIGHT_ROWS, TYPE_ROWS, 2)
        rest = halves[side, WEIGHT_ROWS + 2 * TYPE_ROWS : WEIGHT_ROWS + TABLE_ROWS]
        rest = rest[:, :120].reshape(LEVEL_WINDOWS, GROUPS, HEADS, 20).swapaxes(1, 2)
        full = jnp.concatenate([wide, rest.reshape(TYPE_ROWS, 20)], axis=1)
        full = full.reshape(
            LEVEL_WINDOWS, HEADS, WIN_LEVELS, WIN_LAT, WIN_LEVELS, WIN_LAT * OFFSETS
        )
        tables.append(full.swapaxes(3, 4).reshape(LEVEL_WINDOWS, HEADS, BIAS_SLOTS))
    table = jnp.stack(tables, axis=1)
    gain = halves[0] + halves[1]
    gain = gain[WEIGHT_ROWS + TABLE_ROWS : WEIGHT_ROWS + TABLE_ROWS + 3].reshape(2, MODEL_WIDTH)
    return front[:, : 3 * MODEL_WIDTH], front[:, 3 * MODEL_WIDTH :], expand, reduce, gain, table


def on_device(
    inputs, grad_output, norm_gains, input_weight, output_weight, expand_weight, reduce_weight,
    bias_table,
):
    lat_index = lax.axis_index("lat")
    orders = [jnp.asarray(order) for order in quad_orders()]
    split, join_rolled, split_rolled, join = orders
    tables = pair_rows(
        lax.dynamic_index_in_dim(bias_table[0], lat_index, axis=2, keepdims=False)
    )
    weights = [
        (norm_gains[0, b], input_weight[0, b], output_weight[0, b], expand_weight[0, b], reduce_weight[0, b])
        for b in range(BLOCKS)
    ]
    tokens = inputs[0].reshape(TOKENS, MODEL_WIDTH)
    grads = grad_output[0].reshape(TOKENS, MODEL_WIDTH)

    def split_kernel(x_ref, order_ref, *quads):
        parts = reorder(x_ref[...], order_ref[...])
        for index, quad in enumerate(quads):
            quad[...] = parts[index * QUAD : (index + 1) * QUAD]

    grad_quads = exchange(call(split_kernel, (QUAD_SHAPE,) * 4, [], grads, split), -1)
    outs = call(
        forward_kernel,
        (QUAD_SHAPE,) * 4 + (TOKEN_SHAPE,) * 3 + (WEIGHT_SHAPE,) + (TOKEN_SHAPE,) * 2,
        [tall_scratch(), tall_scratch()],
        tokens, *weights[0], tables[0], split,
    )
    saved = outs[4:]
    block_quads = exchange(outs[:4], -1)
    lat_row = jnp.full((8, 128), lat_index, F32)
    outs = call(
        turn_kernel,
        (QUAD_SHAPE,) * 4 + (PACK_SHAPE,),
        [tall_scratch(), tall_scratch()] + [token_scratch() for _ in range(3)]
        + [pltpu.VMEM(WEIGHT_SHAPE.shape, BF16), token_scratch(),
           pltpu.VMEM((3, TOKENS, MODEL_WIDTH), BF16)],
        *block_quads, *grad_quads, lat_row, *weights[1], tables[1], join_rolled, split_rolled,
    )
    pack_late = outs[4]
    flow_quads = exchange(outs[:4], 1)
    grad_flow, pack_early = call(
        backward_kernel,
        (TOKEN_SHAPE, PACK_SHAPE),
        [tall_scratch(), tall_scratch(), pltpu.VMEM((3, TOKENS, MODEL_WIDTH), BF16)],
        tokens, *flow_quads, *weights[0], join, *saved,
    )
    upstream = lax.ppermute(
        grad_flow, "section", [(i, i - 1) for i in range(1, lax.axis_size("section"))]
    )
    upstream = upstream.reshape(1, LEVELS, LAT_DEV, LON_DEV, MODEL_WIDTH)
    lat_total = LAT_DEV * lax.axis_size("lat")
    grad_scale = float(LEVELS * lat_total * LON_DEV * lax.axis_size("lon")) ** (-0.5)
    results = [unpack(reduce_packs(pack)) for pack in (pack_early, pack_late)]
    stacked = [jnp.stack([results[b][index] for b in range(BLOCKS)])[None] for index in range(6)]
    return (upstream,) + tuple(total * grad_scale for total in stacked[:5]) + (stacked[5],)


def solution(mesh):
    return jax.shard_map(
        on_device,
        mesh=mesh,
        in_specs=(
            P("section", None, "lat", "lon", None),
            P("section", None, "lat", "lon", None),
            P("section", None, None, None),
            P("section", None, None, None),
            P("section", None, None, None),
            P("section", None, None, None),
            P("section", None, None, None),
            P("section", None, None, None, None, None),
        ),
        out_specs=(
            P("section", None, "lat", "lon", None),
            P("section", None, None, None),
            P("section", None, None, None),
            P("section", None, None, None),
            P("section", None, None, None),
            P("section", None, None, None),
            P("section", None, None, None, None, None),
        ),
        check_vma=False,
    )
```

```python
import functools

import jax
import jax.numpy as jnp
import numpy as np
from jax import lax
from jax.experimental import pallas as pl
from jax.experimental.pallas import tpu as pltpu
from jax.sharding import Mesh
from jax.sharding import PartitionSpec as P

MODEL_WIDTH = 192
HEADS = 6
HEAD_SIZE = 32
LEVELS = 8
WIN_LEVELS = 2
WIN_LAT = 6
WIN_LON = 12
BLOCKS = 2
MLP_WIDTH = 768
LAT_DEV = 6
LON_DEV = 12
LEVEL_WINDOWS = 4
WIN_TOKENS = 144
BIAS_SLOTS = 3312

NORM_EPS = 1e-05
MASK_FILL = -10000.0
GELU_C = 0.7978845608028654
GELU_A = 0.044715

TOKENS = LEVELS * LAT_DEV * LON_DEV
QUAD = TOKENS // 4
STACK = HEADS * WIN_TOKENS
GROUPS = WIN_LEVELS * WIN_LAT
OFFSETS = 2 * WIN_LON - 1
PAIR_LANES = GROUPS * OFFSETS
PAIR_PAD = 384
TYPE_ROWS = LEVEL_WINDOWS * HEADS * GROUPS
X_SIZE = 4
WEIGHT_ROWS = 3584
TABLE_ROWS = 640
GAIN_ROW = 3456
WEIGHT_SLAB = WEIGHT_ROWS // X_SIZE
TABLE_SLAB = TABLE_ROWS // X_SIZE
WEIGHT_PART = 56
TABLE_PART = 10
PART = 80

F32 = jnp.float32
BF16 = jnp.bfloat16


def quad_orders():
    level, row, col = np.meshgrid(
        np.arange(LEVELS), np.arange(LAT_DEV), np.arange(LON_DEV), indexing="ij"
    )
    half_rows, half_cols = WIN_LAT // 2, WIN_LON // 2
    quad = (1 - row // half_rows) * 2 + (1 - col // half_cols)
    place = (quad * LEVELS + level) * (half_rows * half_cols)
    place = place + (row % half_rows) * half_cols + col % half_cols
    split = place.reshape(-1)
    quad_r = (row // half_rows) * 2 + col // half_cols
    from_level = (level + WIN_LEVELS // 2) % LEVELS
    place_r = (quad_r * LEVELS + from_level) * (half_rows * half_cols)
    place_r = place_r + (row % half_rows) * half_cols + col % half_cols
    split_rolled = place_r.reshape(-1)
    join = np.argsort(split)
    join_rolled = np.argsort(split_rolled)
    return [order.astype(np.int32)[None, :] for order in (split, join_rolled, split_rolled, join)]


def dot_nn(a, b):
    return jnp.dot(a, b, preferred_element_type=F32)


def dot_nt(a, b):
    return lax.dot_general(a, b, (((1,), (1,)), ((), ())), preferred_element_type=F32)


def dot_tn(a, b):
    return lax.dot_general(a, b, (((0,), (0,)), ((), ())), preferred_element_type=F32)


def reorder(values, order_row):
    rows = lax.broadcasted_iota(jnp.int32, (TOKENS, TOKENS), 0)
    pick = jnp.where(rows == order_row, 1.0, 0.0).astype(BF16)
    return dot_nn(pick, values).astype(BF16)


def norm_stats(values):
    centred = values - jnp.mean(values, axis=-1, keepdims=True)
    spread = jnp.mean(centred * centred, axis=-1, keepdims=True)
    inv = lax.rsqrt(spread + NORM_EPS)
    return centred * inv, inv


def norm_grad(grad, unit, inv, gain_row):
    gain_grad = jnp.sum(grad * unit, axis=0, keepdims=True)
    grad_unit = grad * gain_row
    first = jnp.mean(grad_unit, axis=-1, keepdims=True)
    second = jnp.mean(grad_unit * unit, axis=-1, keepdims=True)
    return inv * (grad_unit - first - unit * second), gain_grad


def head_masks():
    lane = lax.broadcasted_iota(jnp.int32, (1, MODEL_WIDTH), 1)
    return [
        jnp.logical_and(lane >= h * HEAD_SIZE, lane < (h + 1) * HEAD_SIZE) for h in range(HEADS)
    ]


def stack_heads(values, masks):
    wide = values.astype(F32)
    return jnp.concatenate([jnp.where(m, wide, 0.0) for m in masks], axis=0).astype(BF16)


def fold_heads(stacked, masks):
    total = jnp.where(masks[0], stacked[:WIN_TOKENS], 0.0)
    for h in range(1, HEADS):
        total = jnp.where(masks[h], stacked[h * WIN_TOKENS : (h + 1) * WIN_TOKENS], total)
    return total


def pair_pick(query_col):
    key = lax.broadcasted_iota(jnp.int32, (256, PAIR_PAD), 0)
    lane = lax.broadcasted_iota(jnp.int32, (256, PAIR_PAD), 1)
    group = lax.shift_right_logical(key * 5462, 16)
    key_col = key - group * WIN_LON
    target = group * OFFSETS + (WIN_LON - 1 + query_col) - key_col
    hit = jnp.logical_and(lane == target, key < WIN_TOKENS)
    return jnp.where(hit, 1.0, 0.0).astype(BF16)


def segment_start(group, key_level):
    query_level, query_row = group // WIN_LAT, group % WIN_LAT
    return ((query_level * WIN_LEVELS + key_level) * WIN_LAT + query_row) * WIN_LAT * OFFSETS


def load_table(table_ref, parts):
    width = WIN_LAT * OFFSETS
    for window in range(LEVEL_WINDOWS):
        rows = table_ref[0, 0, window, 0]
        for group in range(GROUPS):
            pieces = []
            for key_level in range(WIN_LEVELS):
                start = segment_start(group, key_level)
                pieces.append(rows[:, start : start + width])
            pieces.append(jnp.zeros((HEADS, PAIR_PAD - PAIR_LANES), F32))
            line = jnp.concatenate(pieces, axis=1)
            place = pl.ds(window * HEADS * GROUPS + group, HEADS, stride=GROUPS)
            for index, part in enumerate(parts):
                part[place, :] = line[:, index * 128 : (index + 1) * 128]
    return jnp.concatenate([part[...] for part in parts], axis=1)


def load_tokens(ref, flat):
    for line in range(LEVELS * LAT_DEV):
        level, row = line // LAT_DEV, line % LAT_DEV
        flat[pl.ds(line * LON_DEV, LON_DEV), :] = ref[0, level, row].astype(F32)
    return flat[...]


def build_bias(table, bias_a, bias_b):
    high = table.astype(BF16)
    rest = table - high.astype(F32)
    middle = rest.astype(BF16)
    low = (rest - middle.astype(F32)).astype(BF16)
    for query_col in range(WIN_LON):
        pick = pair_pick(query_col)
        spread = dot_nt(high, pick) + dot_nt(middle, pick) + dot_nt(low, pick)
        bias_a[pl.ds(query_col, TYPE_ROWS, stride=WIN_LON), :] = spread[:, :128]
        bias_b[pl.ds(query_col, TYPE_ROWS, stride=WIN_LON), :] = spread[:, 128:]


def fold_table(score_a, score_b):
    total = jnp.zeros((TYPE_ROWS, PAIR_PAD), F32)
    for query_col in range(WIN_LON):
        pick = pair_pick(query_col)
        left = score_a[pl.ds(query_col, TYPE_ROWS, stride=WIN_LON), :]
        right = score_b[pl.ds(query_col, TYPE_ROWS, stride=WIN_LON), :]
        total = total + dot_nn(left.astype(BF16), pick[:128])
        total = total + dot_nn(right.astype(BF16), pick[128:])
    return total


def shift_mask(window, lat_row):
    shape = (WIN_TOKENS, WIN_TOKENS)
    half = WIN_TOKENS // 2
    parts = []
    for axis in (0, 1):
        token = lax.broadcasted_iota(jnp.int32, shape, axis)
        upper = token >= half
        inner = jnp.where(upper, token - half, token)
        parts.append((upper, inner >= half // 2))
    rows_differ = jnp.where(parts[0][1] != parts[1][1], 1.0, 0.0) * lat_row
    if window == LEVEL_WINDOWS - 1:
        levels_differ = jnp.where(parts[0][0] != parts[1][0], 1.0, 0.0)
        rows_differ = jnp.maximum(rows_differ, levels_differ)
    return rows_differ * MASK_FILL


def attention_front(unit, gain_row, input_weight, bias_a, bias_b, lat_row, q_ref, k_ref, v_ref, w_ref, mix_ref):
    normed = (unit * gain_row).astype(BF16)
    q_ref[...] = (dot_nn(normed, input_weight[:, :MODEL_WIDTH]) * HEAD_SIZE ** (-0.5)).astype(BF16)
    k_ref[...] = dot_nn(normed, input_weight[:, MODEL_WIDTH : 2 * MODEL_WIDTH]).astype(BF16)
    v_ref[...] = dot_nn(normed, input_weight[:, 2 * MODEL_WIDTH :]).astype(BF16)
    masks = head_masks()
    for window in range(LEVEL_WINDOWS):
        rows = pl.ds(window * WIN_TOKENS, WIN_TOKENS)
        stack_rows = pl.ds(window * STACK, STACK)
        queries = stack_heads(q_ref[rows, :], masks)
        scores = dot_nt(queries, k_ref[rows, :])
        bias = jnp.concatenate(
            [bias_a[stack_rows, :], bias_b[stack_rows, :][:, : WIN_TOKENS - 128]], axis=1
        )
        scores = scores + bias
        if lat_row is not None:
            mask = shift_mask(window, lat_row)
            scores = scores + jnp.concatenate([mask] * HEADS, axis=0)
        scores = jnp.exp(scores - jnp.max(scores, axis=-1, keepdims=True))
        weights = (scores / jnp.sum(scores, axis=-1, keepdims=True)).astype(BF16)
        w_ref[stack_rows, :] = weights
        mixed = dot_nn(weights, v_ref[rows, :])
        mix_ref[rows, :] = fold_heads(mixed, masks).astype(BF16)
    return normed


def gelu_parts(pre):
    square = pre * pre
    tanh = jnp.tanh(GELU_C * (pre + GELU_A * pre * square))
    half = 0.5 * (1.0 + tanh)
    slope = half + 0.5 * pre * (1.0 - tanh * tanh) * (GELU_C * (1.0 + 3.0 * GELU_A * square))
    return pre * half, slope


def pack_rows(out_ref, first, values, slab, base):
    done = 0
    while done < values.shape[0]:
        side, inner = (first + done) // slab, (first + done) % slab
        count = min(values.shape[0] - done, slab - inner)
        out_ref[side, pl.ds(base + inner, count), :] = values[done : done + count].astype(BF16)
        done += count


def pack_columns(out_ref, first, values, slab=WEIGHT_SLAB, base=0):
    rows, lanes = values.shape
    for block in range(lanes // 128):
        pack_rows(
            out_ref, first + block * rows, values[:, block * 128 : (block + 1) * 128], slab, base
        )


def backward(e, x_unit, x_inv, gains, middle, weights4, saved, scores_ab, pack_ref, gproj_ref):
    input_weight, output_weight, expand_weight, reduce_weight = weights4
    q_ref, k_ref, v_ref, w_ref, mix_ref = saved
    score_a, score_b = scores_ab
    masks = head_masks()
    mid_unit, mid_inv = norm_stats(middle.astype(F32))
    gain_mid = gains[1:2, :]
    normed_mid = (mid_unit * gain_mid).astype(BF16)
    hidden, slope = gelu_parts(dot_nn(normed_mid, expand_weight))
    hidden = hidden.astype(BF16)
    grad_pre = (slope * dot_nt(e, reduce_weight)).astype(BF16)
    reduce_grad = dot_tn(hidden, e)
    half_mlp = MLP_WIDTH // 2
    pack_columns(
        pack_ref, 2304, jnp.concatenate([reduce_grad[:half_mlp], reduce_grad[half_mlp:]], axis=1)
    )
    pack_columns(pack_ref, 1152, dot_tn(normed_mid, grad_pre))
    grad_norm, gain_mid_grad = norm_grad(dot_nt(grad_pre, expand_weight), mid_unit, mid_inv, gain_mid)
    grad_middle = e.astype(F32) + grad_norm
    grad_attended = grad_middle.astype(BF16)
    output_grad = dot_tn(mix_ref[...], grad_attended)
    grad_mixture = dot_nt(grad_attended, output_weight).astype(BF16)
    for window in range(LEVEL_WINDOWS):
        base = window * WIN_TOKENS
        rows = pl.ds(base, WIN_TOKENS)
        stack_rows = pl.ds(window * STACK, STACK)
        queries = stack_heads(q_ref[rows, :], masks)
        grads = stack_heads(grad_mixture[base : base + WIN_TOKENS], masks)
        weights = w_ref[stack_rows, :]
        keys = k_ref[rows, :]
        gproj_ref[2, rows, :] = dot_tn(weights, grads).astype(BF16)
        grad_weights = dot_nt(grads, v_ref[rows, :])
        attention = weights.astype(F32)
        moved = attention * grad_weights
        grad_scores = attention * (grad_weights - jnp.sum(moved, axis=-1, keepdims=True))
        score_a[stack_rows, :] = grad_scores[:, :128]
        score_b[stack_rows, :] = jnp.concatenate(
            [grad_scores[:, 128:], jnp.zeros((STACK, 256 - WIN_TOKENS), F32)], axis=1
        )
        score_part = grad_scores.astype(BF16)
        grad_queries = fold_heads(dot_nn(score_part, keys), masks) * HEAD_SIZE ** (-0.5)
        gproj_ref[0, rows, :] = grad_queries.astype(BF16)
        gproj_ref[1, rows, :] = dot_tn(score_part, queries).astype(BF16)
    normed = (x_unit * gains[0:1, :]).astype(BF16)
    parts = [gproj_ref[part] for part in range(3)]
    weight_grads = [dot_tn(normed, part) for part in parts] + [output_grad]
    pack_columns(pack_ref, 0, jnp.concatenate(weight_grads, axis=1))
    grad_normed = dot_nt(parts[0], input_weight[:, :MODEL_WIDTH])
    grad_normed = grad_normed + dot_nt(parts[1], input_weight[:, MODEL_WIDTH : 2 * MODEL_WIDTH])
    grad_normed = grad_normed + dot_nt(parts[2], input_weight[:, 2 * MODEL_WIDTH :])
    grad_normed = grad_normed.astype(BF16).astype(F32)
    grad_in, gain_in_grad = norm_grad(grad_normed, x_unit, x_inv, gains[0:1, :])
    folded = fold_table(score_a, score_b)
    pack_columns(pack_ref, 0, folded[:, :256], TABLE_SLAB, WEIGHT_SLAB)
    tail = TYPE_ROWS // HEADS
    pieces = [folded[h * tail : (h + 1) * tail, 256:PAIR_LANES] for h in range(HEADS)]
    pieces.append(jnp.zeros((tail, 128 - HEADS * (PAIR_LANES - 256)), F32))
    rest = jnp.concatenate([jnp.concatenate(pieces, axis=1), jnp.zeros((16, 128), F32)], axis=0)
    pack_rows(pack_ref, 2 * TYPE_ROWS, rest, TABLE_SLAB, WEIGHT_SLAB)
    gain_flat = jnp.concatenate([gain_in_grad, gain_mid_grad], axis=1)
    gain_rows = [gain_flat[:, i * 128 : (i + 1) * 128] for i in range(3)]
    gain_rows.append(jnp.zeros((WEIGHT_ROWS - GAIN_ROW - 3, 128), F32))
    pack_rows(pack_ref, GAIN_ROW, jnp.concatenate(gain_rows, axis=0), WEIGHT_SLAB, 0)
    return (grad_middle + grad_in).astype(BF16)


def forward_kernel(
    lat_ref, x_ref, e_ref, gains_ref, wi_ref, wo_ref, we_ref, wr_ref, table_ref, order_ref,
    quad0, quad1, quad2, quad3, q_ref, k_ref, v_ref, w_ref, mix_ref, mid_ref, tok_ref,
    bias_a, bias_b, part_a, part_b, part_c, flat,
):
    build_bias(load_table(table_ref, (part_a, part_b, part_c)), bias_a, bias_b)
    gains = gains_ref[0, 0]
    order = order_ref[...]
    quads = (quad0, quad1, quad2, quad3)
    moved = reorder(load_tokens(e_ref, flat).astype(BF16), order)
    for index, quad in enumerate(quads):
        quad[1] = moved[index * QUAD : (index + 1) * QUAD]
    values = load_tokens(x_ref, flat)
    tok_ref[...] = values.astype(BF16)
    unit, _ = norm_stats(values)
    attention_front(
        unit, gains[0:1, :], wi_ref[0, 0], bias_a, bias_b, None, q_ref, k_ref, v_ref, w_ref, mix_ref
    )
    middle = (values + dot_nn(mix_ref[...], wo_ref[0, 0])).astype(BF16)
    mid_ref[...] = middle
    mid_f = middle.astype(F32)
    mid_unit, _ = norm_stats(mid_f)
    normed_mid = (mid_unit * gains[1:2, :]).astype(BF16)
    hidden, _ = gelu_parts(dot_nn(normed_mid, we_ref[0, 0]))
    output = (mid_f + dot_nn(hidden.astype(BF16), wr_ref[0, 0])).astype(BF16)
    moved = reorder(output, order)
    for index, quad in enumerate(quads):
        quad[0] = moved[index * QUAD : (index + 1) * QUAD]


def turn_kernel(
    lat_ref, x0, x1, x2, x3, gains_ref, wi_ref, wo_ref, we_ref, wr_ref, table_ref,
    join_ref, split_ref, quad0, quad1, quad2, quad3, pack_ref,
    bias_a, bias_b, part_a, part_b, part_c, q_ref, k_ref, v_ref, w_ref, mix_ref, gproj_ref,
):
    build_bias(load_table(table_ref, (part_a, part_b, part_c)), bias_a, bias_b)
    gains = gains_ref[0, 0]
    join = join_ref[...]
    pieces = (x0, x1, x2, x3)
    block_in = reorder(jnp.concatenate([piece[0] for piece in pieces], axis=0), join)
    e = reorder(jnp.concatenate([piece[1] for piece in pieces], axis=0), join)
    values = block_in.astype(F32)
    unit, inv = norm_stats(values)
    input_weight, output_weight = wi_ref[0, 0], wo_ref[0, 0]
    attention_front(
        unit, gains[0:1, :], input_weight, bias_a, bias_b, lat_ref[0].astype(F32), q_ref, k_ref,
        v_ref, w_ref, mix_ref,
    )
    attended = dot_nn(mix_ref[...], output_weight).astype(BF16).astype(F32)
    middle = (values + attended).astype(BF16)
    result = backward(
        e, unit, inv, gains, middle, (input_weight, output_weight, we_ref[0, 0], wr_ref[0, 0]),
        (q_ref, k_ref, v_ref, w_ref, mix_ref), (bias_a, bias_b), pack_ref, gproj_ref,
    )
    moved = reorder(result, split_ref[...])
    for index, quad in enumerate((quad0, quad1, quad2, quad3)):
        quad[...] = moved[index * QUAD : (index + 1) * QUAD]


def backward_kernel(
    lat_ref, x_ref, e0, e1, e2, e3, gains_ref, wi_ref, wo_ref, we_ref, wr_ref, join_ref,
    q_ref, k_ref, v_ref, w_ref, mix_ref, mid_ref, out_ref, pack_ref, score_a, score_b, gproj_ref,
):
    e = reorder(jnp.concatenate([e0[...], e1[...], e2[...], e3[...]], axis=0), join_ref[...])
    unit, inv = norm_stats(x_ref[...].astype(F32))
    out_ref[...] = backward(
        e, unit, inv, gains_ref[0, 0], mid_ref[...],
        (wi_ref[0, 0], wo_ref[0, 0], we_ref[0, 0], wr_ref[0, 0]),
        (q_ref, k_ref, v_ref, w_ref, mix_ref), (score_a, score_b), pack_ref, gproj_ref,
    )


def unpack_kernel(
    scale, lat_ref, parts_ref, *refs
):
    gi_ref, go_ref, ge_ref, gr_ref, gn_ref, gt_ref, rows, t0, t1, part_a, part_b, part_c = refs[-12:]
    for index in range(parts_ref.shape[0]):
        part = parts_ref[index].astype(F32)
        rows[pl.ds(index * WEIGHT_PART, WEIGHT_PART), :] = part[:WEIGHT_PART] * scale
        for side, table in enumerate((t0, t1)):
            first = WEIGHT_PART + side * TABLE_PART
            table[pl.ds(index * TABLE_PART, TABLE_PART), :] = part[first : first + TABLE_PART]

    def block(first, count):
        return rows[pl.ds(first, count), :]

    for index in range(4):
        gi_ref[0, 0, :, pl.ds(index * 128, 128)] = block(index * 192, 192)
    mixed = block(4 * 192, 192)
    gi_ref[0, 0, :, pl.ds(512, 64)] = mixed[:, :64]
    go_ref[0, 0] = jnp.concatenate([mixed[:, 64:], block(5 * 192, 192)], axis=1)
    for index in range(6):
        ge_ref[0, 0, :, pl.ds(index * 128, 128)] = block(1152 + index * 192, 192)
    half = MLP_WIDTH // 2
    mixed = block(2304 + half, half)
    gr_ref[0, 0, pl.ds(0, half), pl.ds(0, 128)] = block(2304, half)
    gr_ref[0, 0, pl.ds(0, half), pl.ds(128, 64)] = mixed[:, :64]
    gr_ref[0, 0, pl.ds(half, half), :] = jnp.concatenate(
        [mixed[:, 64:], block(2304 + 2 * half, half)], axis=1
    )
    gain = block(GAIN_ROW, 8)
    gn_ref[0, 0, 0:1, :] = jnp.concatenate([gain[0:1], gain[1:2, :64]], axis=1)
    gn_ref[0, 0, 1:2, :] = jnp.concatenate([gain[1:2, 64:], gain[2:3]], axis=1)
    tail, width = TYPE_ROWS // HEADS, PAIR_LANES - 256
    for side, table in enumerate((t0, t1)):
        rest = table[pl.ds(2 * TYPE_ROWS, tail), :]
        for h in range(HEADS):
            part_c[pl.ds(h * tail, tail), pl.ds(0, width)] = rest[:, h * width : (h + 1) * width]
        for window in range(LEVEL_WINDOWS):
            lines = []
            for group in range(GROUPS):
                first = window * HEADS * GROUPS + group
                place = pl.ds(first, HEADS, stride=GROUPS)
                upper = pl.ds(TYPE_ROWS + first, HEADS, stride=GROUPS)
                lines.append(
                    jnp.concatenate([table[place, :], table[upper, :], part_c[place, :]], axis=1)
                )
            span = WIN_LAT * OFFSETS
            ordered = []
            for query_level in range(WIN_LEVELS):
                for key_level in range(WIN_LEVELS):
                    for row in range(WIN_LAT):
                        line = lines[query_level * WIN_LAT + row]
                        ordered.append(line[:, key_level * span : (key_level + 1) * span])
            gt_ref[0, 0, window, side] = jnp.concatenate(ordered, axis=1)


LIMIT = 60 * 1024 * 1024
TOKEN_SHAPE = jax.ShapeDtypeStruct((TOKENS, MODEL_WIDTH), BF16)
QUAD_SHAPE = jax.ShapeDtypeStruct((QUAD, MODEL_WIDTH), BF16)
WEIGHT_SHAPE = jax.ShapeDtypeStruct((LEVEL_WINDOWS * STACK, WIN_TOKENS), BF16)
PACK_SHAPE = jax.ShapeDtypeStruct((X_SIZE, WEIGHT_SLAB + TABLE_SLAB, 128), BF16)
PAIR_SHAPE = jax.ShapeDtypeStruct((2, QUAD, MODEL_WIDTH), BF16)
GRAD_SHAPES = tuple(
    jax.ShapeDtypeStruct((1, BLOCKS) + shape, F32)
    for shape in (
        (MODEL_WIDTH, 3 * MODEL_WIDTH), (MODEL_WIDTH, MODEL_WIDTH), (MODEL_WIDTH, MLP_WIDTH),
        (MLP_WIDTH, MODEL_WIDTH), (2, MODEL_WIDTH), (LEVEL_WINDOWS, 2, HEADS, BIAS_SLOTS),
    )
)


def tall_scratch():
    return pltpu.VMEM((LEVEL_WINDOWS * STACK, 128), F32)


def token_scratch():
    return pltpu.VMEM((TOKENS, MODEL_WIDTH), BF16)


def whole(array):
    rank = len(array.shape)
    return pl.BlockSpec(array.shape, lambda i, lat: (0,) * rank)


def one_block(array, index):
    rank = len(array.shape)
    return pl.BlockSpec((1, 1) + array.shape[2:], lambda i, lat: (0, index) + (0,) * (rank - 2))


def one_table(array, index):
    shape = (1, 1, LEVEL_WINDOWS, 1, HEADS, BIAS_SLOTS)
    return pl.BlockSpec(shape, lambda i, lat: (0, index, 0, lat[0], 0, 0))


def call(kernel, lat, ins, outs, scratch, aliases=None):
    arrays = [array for array, _ in ins]
    return pl.pallas_call(
        kernel,
        out_shape=tuple(shape for shape, _ in outs),
        grid_spec=pltpu.PrefetchScalarGridSpec(
            num_scalar_prefetch=1,
            grid=(1,),
            in_specs=[spec for _, spec in ins],
            out_specs=tuple(spec for _, spec in outs),
            scratch_shapes=scratch,
        ),
        input_output_aliases=aliases or {},
        compiler_params=pltpu.CompilerParams(vmem_limit_bytes=LIMIT),
    )(lat, *arrays)


def plain(*arrays):
    return [(array, whole(array)) for array in arrays]


def exchange(quads, by):
    lon = ("z", "x")
    ring, sides = lax.axis_size(lon), lax.axis_size("lat")
    lon_pairs = [(i, (i + by) % ring) for i in range(ring)]
    swap = [(i, i ^ 1) for i in range(sides)]
    both = [
        (i * sides + j, ((i + by) % ring) * sides + (j ^ 1)) for i in range(ring) for j in range(sides)
    ]
    return (
        quads[0],
        lax.ppermute(quads[1], lon, lon_pairs),
        lax.ppermute(quads[2], "lat", swap),
        lax.ppermute(quads[3], lon + ("lat",), both),
    )


def swap_all(values, axes):
    return lax.all_to_all(values, axes, split_axis=0, concat_axis=0, tiled=True)


def scatter_x(pack):
    return swap_all(pack, "x")


def scatter_rest(spread, first_side):
    total = jnp.sum(spread.astype(F32), axis=0)
    count = lax.axis_size("z") * lax.axis_size("lat")
    weights = total[:WEIGHT_SLAB].reshape(count, WEIGHT_PART, 128)
    table = total[WEIGHT_SLAB:].reshape(count, TABLE_PART, 128)
    spare = jnp.zeros((count, PART - WEIGHT_PART - 2 * TABLE_PART, 128), F32)
    sides = [jnp.where(first_side, table, 0.0), jnp.where(first_side, 0.0, table)]
    parts = jnp.concatenate([weights] + sides + [spare], axis=1).astype(BF16)
    return swap_all(parts, ("z", "lat"))


def gather_rest(spread):
    mine = jnp.sum(spread.astype(F32), axis=0).astype(BF16)
    return swap_all(jnp.broadcast_to(mine[None], spread.shape), ("z", "lat"))


def gather_x(parts):
    wide = jnp.broadcast_to(parts[None], (X_SIZE,) + parts.shape)
    return swap_all(wide, "x").reshape((-1,) + parts.shape[1:])


def unpack(parts, lat, index, scale, previous):
    ins = plain(parts)
    aliases = {}
    if previous is not None:
        ins = ins + [(array, pl.BlockSpec(memory_space=pl.ANY)) for array in previous]
        aliases = {2 + place: place for place in range(6)}
    outs = [(shape, one_block(shape, index)) for shape in GRAD_SHAPES]
    tables = [pltpu.VMEM((TABLE_ROWS, 128), F32) for _ in range(2)]
    scratch = [pltpu.VMEM((WEIGHT_ROWS, 128), F32)] + tables + type_scratch()
    return call(functools.partial(unpack_kernel, scale), lat, ins, outs, scratch, aliases)


def type_scratch():
    return [pltpu.VMEM((TYPE_ROWS, 128), F32) for _ in range(3)]


def on_device(
    inputs, grad_output, norm_gains, input_weight, output_weight, expand_weight, reduce_weight,
    bias_table,
):
    lat_index = lax.axis_index("lat")
    lat = jnp.full((1,), lat_index, jnp.int32)
    orders = [jnp.asarray(order) for order in quad_orders()]
    split, join_rolled, split_rolled, join = orders
    weights = [
        [(array, one_block(array, block)) for array in
         (norm_gains, input_weight, output_weight, expand_weight, reduce_weight)]
        for block in range(BLOCKS)
    ]
    tables = [[(bias_table, one_table(bias_table, block))] for block in range(BLOCKS)]
    outs = call(
        forward_kernel,
        lat,
        plain(inputs, grad_output) + weights[0] + tables[0] + plain(split),
        plain(*((PAIR_SHAPE,) * 4 + (TOKEN_SHAPE,) * 3 + (WEIGHT_SHAPE,) + (TOKEN_SHAPE,) * 3)),
        [tall_scratch(), tall_scratch()] + type_scratch() + [pltpu.VMEM((TOKENS, MODEL_WIDTH), F32)],
    )
    saved = outs[4:10]
    tokens = outs[10]
    quads = exchange(outs[:4], -1)
    outs = call(
        turn_kernel,
        lat,
        plain(*quads) + weights[1] + tables[1] + plain(join_rolled, split_rolled),
        plain(*((QUAD_SHAPE,) * 4 + (PACK_SHAPE,))),
        [tall_scratch(), tall_scratch()] + type_scratch() + [token_scratch() for _ in range(3)]
        + [pltpu.VMEM(WEIGHT_SHAPE.shape, BF16), token_scratch(),
           pltpu.VMEM((3, TOKENS, MODEL_WIDTH), BF16)],
    )
    flow_quads = exchange(outs[:4], 1)
    flow_quads, pack_late = lax.optimization_barrier((flow_quads, outs[4]))
    late = scatter_x(pack_late)
    grad_flow, pack_early = call(
        backward_kernel,
        lat,
        plain(tokens, *flow_quads) + weights[0] + plain(join, *saved),
        plain(TOKEN_SHAPE, PACK_SHAPE),
        [tall_scratch(), tall_scratch(), pltpu.VMEM((3, TOKENS, MODEL_WIDTH), BF16)],
    )
    early = scatter_x(pack_early)
    first_side = lat_index == 0
    lat_total = LAT_DEV * lax.axis_size("lat")
    scale = float(LEVELS * lat_total * LON_DEV * lax.axis_size(("z", "x"))) ** (-0.5)
    late = gather_x(gather_rest(scatter_rest(late, first_side)))
    early = gather_x(gather_rest(scatter_rest(early, first_side)))
    upstream = lax.ppermute(
        grad_flow, "section", [(i, i - 1) for i in range(1, lax.axis_size("section"))]
    )
    upstream = upstream.reshape(1, LEVELS, LAT_DEV, LON_DEV, MODEL_WIDTH)
    grads = unpack(late, lat, 1, scale, None)
    grads = unpack(early, lat, 0, scale, grads)
    return (upstream,) + tuple(grads)


def solution(mesh):
    sizes = mesh.shape
    grid = mesh.devices.reshape(
        sizes["section"], sizes["lon"] // X_SIZE, X_SIZE, sizes["lat"]
    )
    mesh = Mesh(grid, ("section", "z", "x", "lat"))
    return jax.shard_map(
        on_device,
        mesh=mesh,
        in_specs=(
            P("section", None, "lat", ("z", "x"), None),
            P("section", None, "lat", ("z", "x"), None),
            P("section", None, None, None),
            P("section", None, None, None),
            P("section", None, None, None),
            P("section", None, None, None),
            P("section", None, None, None),
            P("section", None, None, None, None, None),
        ),
        out_specs=(
            P("section", None, "lat", ("z", "x"), None),
            P("section", None, None, None),
            P("section", None, None, None),
            P("section", None, None, None),
            P("section", None, None, None),
            P("section", None, None, None),
            P("section", None, None, None, None, None),
        ),
        check_vma=False,
    )
```

```python
import functools

import jax
import jax.numpy as jnp
import numpy as np
from jax import lax
from jax.experimental import pallas as pl
from jax.experimental.pallas import tpu as pltpu
from jax.sharding import Mesh
from jax.sharding import PartitionSpec as P

MODEL_WIDTH = 192
HEADS = 6
HEAD_SIZE = 32
LEVELS = 8
WIN_LEVELS = 2
WIN_LAT = 6
WIN_LON = 12
BLOCKS = 2
MLP_WIDTH = 768
LAT_DEV = 6
LON_DEV = 12
LEVEL_WINDOWS = 4
WIN_TOKENS = 144
BIAS_SLOTS = 3312

NORM_EPS = 1e-05
MASK_FILL = -10000.0
GELU_C = 0.7978845608028654
GELU_A = 0.044715

TOKENS = LEVELS * LAT_DEV * LON_DEV
QUAD = TOKENS // 4
STACK = HEADS * WIN_TOKENS
GROUPS = WIN_LEVELS * WIN_LAT
OFFSETS = 2 * WIN_LON - 1
PAIR_LANES = GROUPS * OFFSETS
PAIR_PAD = 384
TYPE_ROWS = LEVEL_WINDOWS * HEADS * GROUPS
X_SIZE = 4
WEIGHT_ROWS = 3584
TABLE_ROWS = 640
GAIN_ROW = 3456
WEIGHT_SLAB = WEIGHT_ROWS // X_SIZE
TABLE_SLAB = TABLE_ROWS // X_SIZE
WEIGHT_PART = 56
TABLE_PART = 10
PART = 80

F32 = jnp.float32
BF16 = jnp.bfloat16


def quad_orders():
    level, row, col = np.meshgrid(
        np.arange(LEVELS), np.arange(LAT_DEV), np.arange(LON_DEV), indexing="ij"
    )
    half_rows, half_cols = WIN_LAT // 2, WIN_LON // 2
    quad = (1 - row // half_rows) * 2 + (1 - col // half_cols)
    place = (quad * LEVELS + level) * (half_rows * half_cols)
    place = place + (row % half_rows) * half_cols + col % half_cols
    split = place.reshape(-1)
    quad_r = (row // half_rows) * 2 + col // half_cols
    from_level = (level + WIN_LEVELS // 2) % LEVELS
    place_r = (quad_r * LEVELS + from_level) * (half_rows * half_cols)
    place_r = place_r + (row % half_rows) * half_cols + col % half_cols
    split_rolled = place_r.reshape(-1)
    join = np.argsort(split)
    join_rolled = np.argsort(split_rolled)
    natural = np.arange(TOKENS).reshape(LEVELS, LAT_DEV, LON_DEV).transpose(1, 2, 0).reshape(-1)
    stored = np.argsort(natural)
    orders = (split, join_rolled, split_rolled, join, natural, split[natural], stored)
    return [order.astype(np.int32)[None, :] for order in orders]


def dot_nn(a, b):
    return jnp.dot(a, b, preferred_element_type=F32)


def dot_nt(a, b):
    return lax.dot_general(a, b, (((1,), (1,)), ((), ())), preferred_element_type=F32)


def dot_tn(a, b):
    return lax.dot_general(a, b, (((0,), (0,)), ((), ())), preferred_element_type=F32)


def reorder(values, order_row):
    rows = lax.broadcasted_iota(jnp.int32, (TOKENS, TOKENS), 0)
    pick = jnp.where(rows == order_row, 1.0, 0.0).astype(BF16)
    return dot_nn(pick, values).astype(BF16)


def norm_stats(values):
    centred = values - jnp.mean(values, axis=-1, keepdims=True)
    spread = jnp.mean(centred * centred, axis=-1, keepdims=True)
    inv = lax.rsqrt(spread + NORM_EPS)
    return centred * inv, inv


def norm_grad(grad, unit, inv, gain_row):
    gain_grad = jnp.sum(grad * unit, axis=0, keepdims=True)
    grad_unit = grad * gain_row
    first = jnp.mean(grad_unit, axis=-1, keepdims=True)
    second = jnp.mean(grad_unit * unit, axis=-1, keepdims=True)
    return inv * (grad_unit - first - unit * second), gain_grad


def head_masks():
    lane = lax.broadcasted_iota(jnp.int32, (1, MODEL_WIDTH), 1)
    return [
        jnp.logical_and(lane >= h * HEAD_SIZE, lane < (h + 1) * HEAD_SIZE) for h in range(HEADS)
    ]


def stack_heads(values, masks):
    wide = values.astype(F32)
    return jnp.concatenate([jnp.where(m, wide, 0.0) for m in masks], axis=0).astype(BF16)


def fold_heads(stacked, masks):
    total = jnp.where(masks[0], stacked[:WIN_TOKENS], 0.0)
    for h in range(1, HEADS):
        total = jnp.where(masks[h], stacked[h * WIN_TOKENS : (h + 1) * WIN_TOKENS], total)
    return total


def pair_pick(query_col):
    key = lax.broadcasted_iota(jnp.int32, (256, PAIR_PAD), 0)
    lane = lax.broadcasted_iota(jnp.int32, (256, PAIR_PAD), 1)
    group = lax.shift_right_logical(key * 5462, 16)
    key_col = key - group * WIN_LON
    target = group * OFFSETS + (WIN_LON - 1 + query_col) - key_col
    hit = jnp.logical_and(lane == target, key < WIN_TOKENS)
    return jnp.where(hit, 1.0, 0.0).astype(BF16)


def segment_start(group, key_level):
    query_level, query_row = group // WIN_LAT, group % WIN_LAT
    return ((query_level * WIN_LEVELS + key_level) * WIN_LAT + query_row) * WIN_LAT * OFFSETS


def load_table(table_ref, side, parts, lines):
    width = WIN_LAT * OFFSETS
    for window in range(LEVEL_WINDOWS):
        for h in range(HEADS):
            lines[h : h + 1, :] = table_ref[0, 0, window, h, pl.ds(side, 1), :]
        rows = lines[:HEADS, :]
        for group in range(GROUPS):
            pieces = []
            for key_level in range(WIN_LEVELS):
                start = segment_start(group, key_level)
                pieces.append(rows[:, start : start + width])
            pieces.append(jnp.zeros((HEADS, PAIR_PAD - PAIR_LANES), F32))
            line = jnp.concatenate(pieces, axis=1)
            place = pl.ds(window * HEADS * GROUPS + group, HEADS, stride=GROUPS)
            for index, part in enumerate(parts):
                part[place, :] = line[:, index * 128 : (index + 1) * 128]
    return jnp.concatenate([part[...] for part in parts], axis=1)


def build_bias(table, bias_a, bias_b):
    high = table.astype(BF16)
    rest = table - high.astype(F32)
    middle = rest.astype(BF16)
    low = (rest - middle.astype(F32)).astype(BF16)
    for query_col in range(WIN_LON):
        pick = pair_pick(query_col)
        spread = dot_nt(high, pick) + dot_nt(middle, pick) + dot_nt(low, pick)
        bias_a[pl.ds(query_col, TYPE_ROWS, stride=WIN_LON), :] = spread[:, :128]
        bias_b[pl.ds(query_col, TYPE_ROWS, stride=WIN_LON), :] = spread[:, 128:]


def fold_table(score_a, score_b):
    total = jnp.zeros((TYPE_ROWS, PAIR_PAD), F32)
    for query_col in range(WIN_LON):
        pick = pair_pick(query_col)
        left = score_a[pl.ds(query_col, TYPE_ROWS, stride=WIN_LON), :]
        right = score_b[pl.ds(query_col, TYPE_ROWS, stride=WIN_LON), :]
        total = total + dot_nn(left.astype(BF16), pick[:128])
        total = total + dot_nn(right.astype(BF16), pick[128:])
    return total


def shift_mask(window, lat_row):
    shape = (WIN_TOKENS, WIN_TOKENS)
    half = WIN_TOKENS // 2
    parts = []
    for axis in (0, 1):
        token = lax.broadcasted_iota(jnp.int32, shape, axis)
        upper = token >= half
        inner = jnp.where(upper, token - half, token)
        parts.append((upper, inner >= half // 2))
    rows_differ = jnp.where(parts[0][1] != parts[1][1], 1.0, 0.0) * lat_row
    if window == LEVEL_WINDOWS - 1:
        levels_differ = jnp.where(parts[0][0] != parts[1][0], 1.0, 0.0)
        rows_differ = jnp.maximum(rows_differ, levels_differ)
    return rows_differ * MASK_FILL


def attention_front(unit, gain_row, input_weight, bias_a, bias_b, lat_row, q_ref, k_ref, v_ref, w_ref, mix_ref):
    normed = (unit * gain_row).astype(BF16)
    q_ref[...] = (dot_nn(normed, input_weight[:, :MODEL_WIDTH]) * HEAD_SIZE ** (-0.5)).astype(BF16)
    k_ref[...] = dot_nn(normed, input_weight[:, MODEL_WIDTH : 2 * MODEL_WIDTH]).astype(BF16)
    v_ref[...] = dot_nn(normed, input_weight[:, 2 * MODEL_WIDTH :]).astype(BF16)
    masks = head_masks()
    for window in range(LEVEL_WINDOWS):
        rows = pl.ds(window * WIN_TOKENS, WIN_TOKENS)
        stack_rows = pl.ds(window * STACK, STACK)
        queries = stack_heads(q_ref[rows, :], masks)
        scores = dot_nt(queries, k_ref[rows, :])
        bias = jnp.concatenate(
            [bias_a[stack_rows, :], bias_b[stack_rows, :][:, : WIN_TOKENS - 128]], axis=1
        )
        scores = scores + bias
        if lat_row is not None:
            mask = shift_mask(window, lat_row)
            scores = scores + jnp.concatenate([mask] * HEADS, axis=0)
        scores = jnp.exp(scores - jnp.max(scores, axis=-1, keepdims=True))
        weights = (scores / jnp.sum(scores, axis=-1, keepdims=True)).astype(BF16)
        w_ref[stack_rows, :] = weights
        mixed = dot_nn(weights, v_ref[rows, :])
        mix_ref[rows, :] = fold_heads(mixed, masks).astype(BF16)
    return normed


def gelu_parts(pre):
    square = pre * pre
    tanh = jnp.tanh(GELU_C * (pre + GELU_A * pre * square))
    half = 0.5 * (1.0 + tanh)
    slope = half + 0.5 * pre * (1.0 - tanh * tanh) * (GELU_C * (1.0 + 3.0 * GELU_A * square))
    return pre * half, slope


def pack_rows(out_ref, first, values, slab, base):
    done = 0
    while done < values.shape[0]:
        side, inner = (first + done) // slab, (first + done) % slab
        count = min(values.shape[0] - done, slab - inner)
        out_ref[side, pl.ds(base + inner, count), :] = values[done : done + count].astype(BF16)
        done += count


def pack_columns(out_ref, first, values, slab=WEIGHT_SLAB, base=0):
    rows, lanes = values.shape
    for block in range(lanes // 128):
        pack_rows(
            out_ref, first + block * rows, values[:, block * 128 : (block + 1) * 128], slab, base
        )


def backward(e, x_unit, x_inv, gains, middle, weights4, saved, scores_ab, pack_ref, gproj_ref):
    input_weight, output_weight, expand_weight, reduce_weight = weights4
    q_ref, k_ref, v_ref, w_ref, mix_ref = saved
    score_a, score_b = scores_ab
    masks = head_masks()
    mid_unit, mid_inv = norm_stats(middle.astype(F32))
    gain_mid = gains[1:2, :]
    normed_mid = (mid_unit * gain_mid).astype(BF16)
    hidden, slope = gelu_parts(dot_nn(normed_mid, expand_weight))
    hidden = hidden.astype(BF16)
    grad_pre = (slope * dot_nn(e, reduce_weight)).astype(BF16)
    pack_columns(pack_ref, 2304, dot_tn(e, hidden))
    pack_columns(pack_ref, 1152, dot_tn(normed_mid, grad_pre))
    grad_norm, gain_mid_grad = norm_grad(dot_nt(grad_pre, expand_weight), mid_unit, mid_inv, gain_mid)
    grad_middle = e.astype(F32) + grad_norm
    grad_attended = grad_middle.astype(BF16)
    output_grad = dot_tn(mix_ref[...], grad_attended)
    grad_mixture = dot_nt(grad_attended, output_weight).astype(BF16)
    for window in range(LEVEL_WINDOWS):
        base = window * WIN_TOKENS
        rows = pl.ds(base, WIN_TOKENS)
        stack_rows = pl.ds(window * STACK, STACK)
        queries = stack_heads(q_ref[rows, :], masks)
        grads = stack_heads(grad_mixture[base : base + WIN_TOKENS], masks)
        weights = w_ref[stack_rows, :]
        keys = k_ref[rows, :]
        gproj_ref[2, rows, :] = dot_tn(weights, grads).astype(BF16)
        grad_weights = dot_nt(grads, v_ref[rows, :])
        attention = weights.astype(F32)
        moved = attention * grad_weights
        grad_scores = attention * (grad_weights - jnp.sum(moved, axis=-1, keepdims=True))
        score_a[stack_rows, :] = grad_scores[:, :128]
        score_b[stack_rows, :] = jnp.concatenate(
            [grad_scores[:, 128:], jnp.zeros((STACK, 256 - WIN_TOKENS), F32)], axis=1
        )
        score_part = grad_scores.astype(BF16)
        grad_queries = fold_heads(dot_nn(score_part, keys), masks) * HEAD_SIZE ** (-0.5)
        gproj_ref[0, rows, :] = grad_queries.astype(BF16)
        gproj_ref[1, rows, :] = dot_tn(score_part, queries).astype(BF16)
    normed = (x_unit * gains[0:1, :]).astype(BF16)
    parts = [gproj_ref[part] for part in range(3)]
    weight_grads = [dot_tn(normed, part) for part in parts] + [output_grad]
    pack_columns(pack_ref, 0, jnp.concatenate(weight_grads, axis=1))
    grad_normed = dot_nt(parts[0], input_weight[:, :MODEL_WIDTH])
    grad_normed = grad_normed + dot_nt(parts[1], input_weight[:, MODEL_WIDTH : 2 * MODEL_WIDTH])
    grad_normed = grad_normed + dot_nt(parts[2], input_weight[:, 2 * MODEL_WIDTH :])
    grad_normed = grad_normed.astype(BF16).astype(F32)
    grad_in, gain_in_grad = norm_grad(grad_normed, x_unit, x_inv, gains[0:1, :])
    folded = fold_table(score_a, score_b)
    pack_columns(pack_ref, 0, folded[:, :256], TABLE_SLAB, WEIGHT_SLAB)
    tail = TYPE_ROWS // HEADS
    pieces = [folded[h * tail : (h + 1) * tail, 256:PAIR_LANES] for h in range(HEADS)]
    pieces.append(jnp.zeros((tail, 128 - HEADS * (PAIR_LANES - 256)), F32))
    rest = jnp.concatenate([jnp.concatenate(pieces, axis=1), jnp.zeros((16, 128), F32)], axis=0)
    pack_rows(pack_ref, 2 * TYPE_ROWS, rest, TABLE_SLAB, WEIGHT_SLAB)
    gain_flat = jnp.concatenate([gain_in_grad, gain_mid_grad], axis=1)
    gain_rows = [gain_flat[:, i * 128 : (i + 1) * 128] for i in range(3)]
    gain_rows.append(jnp.zeros((WEIGHT_ROWS - GAIN_ROW - 3, 128), F32))
    pack_rows(pack_ref, GAIN_ROW, jnp.concatenate(gain_rows, axis=0), WEIGHT_SLAB, 0)
    return (grad_middle + grad_in).astype(BF16)


def forward_kernel(
    here_ref, x_ref, e_ref, gains_ref, wi_ref, wo_ref, we_ref, wr_ref, table_ref, order_ref,
    natural_ref, early_ref, quad0, quad1, quad2, quad3, q_ref, k_ref, v_ref, w_ref, mix_ref, mid_ref, tok_ref,
    bias_a, bias_b, part_a, part_b, part_c, lines,
):
    build_bias(load_table(table_ref, here_ref[0], (part_a, part_b, part_c), lines), bias_a, bias_b)
    gains = gains_ref[0, 0]
    order = order_ref[...]
    quads = (quad0, quad1, quad2, quad3)
    moved = reorder(e_ref[...], early_ref[...])
    for index, quad in enumerate(quads):
        quad[1] = moved[index * QUAD : (index + 1) * QUAD]
    tokens = reorder(x_ref[...], natural_ref[...])
    tok_ref[...] = tokens
    values = tokens.astype(F32)
    unit, _ = norm_stats(values)
    attention_front(
        unit, gains[0:1, :], wi_ref[0, 0], bias_a, bias_b, None, q_ref, k_ref, v_ref, w_ref, mix_ref
    )
    middle = (values + dot_nn(mix_ref[...], wo_ref[0, 0])).astype(BF16)
    mid_ref[...] = middle
    mid_f = middle.astype(F32)
    mid_unit, _ = norm_stats(mid_f)
    normed_mid = (mid_unit * gains[1:2, :]).astype(BF16)
    hidden, _ = gelu_parts(dot_nn(normed_mid, we_ref[0, 0]))
    output = (mid_f + dot_nt(hidden.astype(BF16), wr_ref[0, 0])).astype(BF16)
    moved = reorder(output, order)
    for index, quad in enumerate(quads):
        quad[0] = moved[index * QUAD : (index + 1) * QUAD]


def turn_kernel(
    here_ref, x0, x1, x2, x3, gains_ref, wi_ref, wo_ref, we_ref, wr_ref, table_ref,
    join_ref, split_ref, quad0, quad1, quad2, quad3, send0, send1, send2, send3,
    bias_a, bias_b, part_a, part_b, part_c, lines, pack_ref, q_ref, k_ref, v_ref, w_ref, mix_ref, gproj_ref,
):
    build_bias(load_table(table_ref, here_ref[0], (part_a, part_b, part_c), lines), bias_a, bias_b)
    gains = gains_ref[0, 0]
    join = join_ref[...]
    pieces = (x0, x1, x2, x3)
    block_in = reorder(jnp.concatenate([piece[0] for piece in pieces], axis=0), join)
    e = reorder(jnp.concatenate([piece[1] for piece in pieces], axis=0), join)
    values = block_in.astype(F32)
    unit, inv = norm_stats(values)
    input_weight, output_weight = wi_ref[0, 0], wo_ref[0, 0]
    attention_front(
        unit, gains[0:1, :], input_weight, bias_a, bias_b, here_ref[0].astype(F32), q_ref, k_ref,
        v_ref, w_ref, mix_ref,
    )
    attended = dot_nn(mix_ref[...], output_weight).astype(BF16).astype(F32)
    middle = (values + attended).astype(BF16)
    result = backward(
        e, unit, inv, gains, middle, (input_weight, output_weight, we_ref[0, 0], wr_ref[0, 0]),
        (q_ref, k_ref, v_ref, w_ref, mix_ref), (bias_a, bias_b), pack_ref, gproj_ref,
    )
    moved = reorder(result, split_ref[...])
    for index, quad in enumerate((quad0, quad1, quad2, quad3)):
        quad[...] = moved[index * QUAD : (index + 1) * QUAD]
    send_slabs(here_ref, pack_ref, (send0, send1, send2, send3))


def send_slabs(here_ref, pack_ref, sends):
    for step, send in enumerate(sends):
        send[...] = pack_ref[lax.rem(here_ref[1] + step, X_SIZE)]


def backward_kernel(
    here_ref, x_ref, e0, e1, e2, e3, gains_ref, wi_ref, wo_ref, we_ref, wr_ref, join_ref,
    stored_ref, q_ref, k_ref, v_ref, w_ref, mix_ref, mid_ref, out_ref, send0, send1, send2, send3,
    score_a, score_b, pack_ref, gproj_ref,
):
    e = reorder(jnp.concatenate([e0[...], e1[...], e2[...], e3[...]], axis=0), join_ref[...])
    unit, inv = norm_stats(x_ref[...].astype(F32))
    result = backward(
        e, unit, inv, gains_ref[0, 0], mid_ref[...],
        (wi_ref[0, 0], wo_ref[0, 0], we_ref[0, 0], wr_ref[0, 0]),
        (q_ref, k_ref, v_ref, w_ref, mix_ref), (score_a, score_b), pack_ref, gproj_ref,
    )
    out_ref[...] = reorder(result, stored_ref[...])
    send_slabs(here_ref, pack_ref, (send0, send1, send2, send3))


def unpack_kernel(scale, here_ref, got0, got1, got2, got3, *refs):
    gi_ref, go_ref, ge_ref, gr_ref, gn_ref, gt_ref = refs[-14:-8]
    rows, slab0, slab1, t0, t1, part_a, part_b, part_c = refs[-8:]
    for step, got in enumerate((got0, got1, got2, got3)):
        origin = lax.rem(here_ref[1] + X_SIZE - step, X_SIZE)
        for index in range(got.shape[0]):
            part = got[index].astype(F32)
            rows[origin, pl.ds(index * WEIGHT_PART, WEIGHT_PART), :] = part[:WEIGHT_PART] * scale
            for side, table in enumerate((slab0, slab1)):
                first = WEIGHT_PART + side * TABLE_PART
                table[origin, pl.ds(index * TABLE_PART, TABLE_PART), :] = part[
                    first : first + TABLE_PART
                ]
    for slab, table in ((slab0, t0), (slab1, t1)):
        for origin in range(X_SIZE):
            table[pl.ds(origin * TABLE_SLAB, TABLE_SLAB), :] = slab[origin]

    def block(first, count):
        pieces = []
        while count:
            origin, inner = first // WEIGHT_SLAB, first % WEIGHT_SLAB
            here = min(count, WEIGHT_SLAB - inner)
            pieces.append(rows[origin, pl.ds(inner, here), :])
            first, count = first + here, count - here
        return pieces[0] if len(pieces) == 1 else jnp.concatenate(pieces, axis=0)

    for index in range(4):
        gi_ref[0, 0, :, pl.ds(index * 128, 128)] = block(index * 192, 192)
    mixed = block(4 * 192, 192)
    gi_ref[0, 0, :, pl.ds(512, 64)] = mixed[:, :64]
    go_ref[0, 0] = jnp.concatenate([mixed[:, 64:], block(5 * 192, 192)], axis=1)
    for index in range(6):
        ge_ref[0, 0, :, pl.ds(index * 128, 128)] = block(1152 + index * 192, 192)
    for index in range(6):
        gr_ref[0, 0, :, pl.ds(index * 128, 128)] = block(2304 + index * 192, 192)
    gain = block(GAIN_ROW, 8)
    gn_ref[0, 0, 0:1, :] = jnp.concatenate([gain[0:1], gain[1:2, :64]], axis=1)
    gn_ref[0, 0, 1:2, :] = jnp.concatenate([gain[1:2, 64:], gain[2:3]], axis=1)
    tail, width = TYPE_ROWS // HEADS, PAIR_LANES - 256
    for side, table in enumerate((t0, t1)):
        rest = table[pl.ds(2 * TYPE_ROWS, tail), :]
        for h in range(HEADS):
            part_c[pl.ds(h * tail, tail), pl.ds(0, width)] = rest[:, h * width : (h + 1) * width]
        for window in range(LEVEL_WINDOWS):
            lines = []
            for group in range(GROUPS):
                first = window * HEADS * GROUPS + group
                place = pl.ds(first, HEADS, stride=GROUPS)
                upper = pl.ds(TYPE_ROWS + first, HEADS, stride=GROUPS)
                lines.append(
                    jnp.concatenate([table[place, :], table[upper, :], part_c[place, :]], axis=1)
                )
            span = WIN_LAT * OFFSETS
            ordered = []
            for query_level in range(WIN_LEVELS):
                for key_level in range(WIN_LEVELS):
                    for row in range(WIN_LAT):
                        line = lines[query_level * WIN_LAT + row]
                        ordered.append(line[:, key_level * span : (key_level + 1) * span])
            result = jnp.concatenate(ordered, axis=1)
            for h in range(HEADS):
                gt_ref[0, 0, window, h, side : side + 1, :] = result[h : h + 1]


LIMIT = 60 * 1024 * 1024
TOKEN_SHAPE = jax.ShapeDtypeStruct((TOKENS, MODEL_WIDTH), BF16)
QUAD_SHAPE = jax.ShapeDtypeStruct((QUAD, MODEL_WIDTH), BF16)
WEIGHT_SHAPE = jax.ShapeDtypeStruct((LEVEL_WINDOWS * STACK, WIN_TOKENS), BF16)
SLAB_SHAPE = jax.ShapeDtypeStruct((WEIGHT_SLAB + TABLE_SLAB, 128), BF16)
PAIR_SHAPE = jax.ShapeDtypeStruct((2, QUAD, MODEL_WIDTH), BF16)
GRAD_SHAPES = tuple(
    jax.ShapeDtypeStruct((1, BLOCKS) + shape, F32)
    for shape in (
        (MODEL_WIDTH, 3 * MODEL_WIDTH), (MODEL_WIDTH, MODEL_WIDTH), (MODEL_WIDTH, MLP_WIDTH),
        (MODEL_WIDTH, MLP_WIDTH), (2, MODEL_WIDTH), (LEVEL_WINDOWS, HEADS, 2, BIAS_SLOTS),
    )
)


def tall_scratch():
    return pltpu.VMEM((LEVEL_WINDOWS * STACK, 128), F32)


def token_scratch():
    return pltpu.VMEM((TOKENS, MODEL_WIDTH), BF16)


def whole(array):
    rank = len(array.shape)
    return pl.BlockSpec(array.shape, lambda i, lat: (0,) * rank)


def one_block(array, index):
    rank = len(array.shape)
    return pl.BlockSpec((1, 1) + array.shape[2:], lambda i, lat: (0, index) + (0,) * (rank - 2))


def call(kernel, lat, ins, outs, scratch, aliases=None):
    arrays = [array for array, _ in ins]
    return pl.pallas_call(
        kernel,
        out_shape=tuple(shape for shape, _ in outs),
        grid_spec=pltpu.PrefetchScalarGridSpec(
            num_scalar_prefetch=1,
            grid=(1,),
            in_specs=[spec for _, spec in ins],
            out_specs=tuple(spec for _, spec in outs),
            scratch_shapes=scratch,
        ),
        input_output_aliases=aliases or {},
        compiler_params=pltpu.CompilerParams(vmem_limit_bytes=LIMIT),
    )(lat, *arrays)


def plain(*arrays):
    return [(array, whole(array)) for array in arrays]


def exchange(quads, by):
    lon = ("z", "x")
    ring, sides = lax.axis_size(lon), lax.axis_size("lat")
    lon_pairs = [(i, (i + by) % ring) for i in range(ring)]
    swap = [(i, i ^ 1) for i in range(sides)]
    both = [
        (i * sides + j, ((i + by) % ring) * sides + (j ^ 1)) for i in range(ring) for j in range(sides)
    ]
    return (
        quads[0],
        lax.ppermute(quads[1], lon, lon_pairs),
        lax.ppermute(quads[2], "lat", swap),
        lax.ppermute(quads[3], lon + ("lat",), both),
    )


def swap_all(values, axes):
    return lax.all_to_all(values, axes, split_axis=0, concat_axis=0, tiled=True)


def pass_x(sends):
    size = lax.axis_size("x")
    return (sends[0],) + tuple(
        lax.ppermute(sends[step], "x", [(i, (i + step) % size) for i in range(size)])
        for step in range(1, size)
    )


def slab_sum(slabs):
    total = slabs[0][...].astype(F32)
    for slab in slabs[1:]:
        total = total + slab[...].astype(F32)
    return total


def write_parts(total, side, out_ref, first):
    lower = jnp.where(side == 0, 1.0, 0.0)
    for index in range(out_ref.shape[0]):
        weights = total[index * WEIGHT_PART : (index + 1) * WEIGHT_PART]
        start = WEIGHT_SLAB + index * TABLE_PART
        table = total[start : start + TABLE_PART]
        spare = jnp.zeros((PART - WEIGHT_PART - 2 * TABLE_PART, 128), F32)
        part = jnp.concatenate([weights, table * lower, table * (1.0 - lower), spare], axis=0)
        out_ref[index, pl.ds(first, PART), :] = part.astype(BF16)


def part_sum(spread_ref, first):
    total = spread_ref[0, pl.ds(first, PART), :].astype(F32)
    for index in range(1, spread_ref.shape[0]):
        total = total + spread_ref[index, pl.ds(first, PART), :].astype(F32)
    return total.astype(BF16)


def first_kernel(here_ref, slab0, slab1, slab2, slab3, out_ref):
    write_parts(slab_sum((slab0, slab1, slab2, slab3)), here_ref[0], out_ref, 0)


def second_kernel(here_ref, late_ref, slab0, slab1, slab2, slab3, out_ref):
    late = part_sum(late_ref, 0)
    for index in range(out_ref.shape[0]):
        out_ref[index, pl.ds(0, PART), :] = late
    write_parts(slab_sum((slab0, slab1, slab2, slab3)), here_ref[0], out_ref, PART)


def third_kernel(here_ref, both_ref, late_ref, early_ref):
    early = part_sum(both_ref, PART)
    for index in range(late_ref.shape[0]):
        late_ref[index] = both_ref[index, pl.ds(0, PART), :]
        early_ref[index] = early


def parts_shape(count, width):
    return jax.ShapeDtypeStruct((count, width, 128), BF16)


def unpack(parts, here, index, scale, previous):
    ins = plain(*parts)
    aliases = {}
    if previous is not None:
        ins = ins + [(array, pl.BlockSpec(memory_space=pl.ANY)) for array in previous]
        aliases = {1 + len(parts) + place: place for place in range(6)}
    outs = [(shape, one_block(shape, index)) for shape in GRAD_SHAPES]
    scratch = [pltpu.VMEM((X_SIZE, WEIGHT_SLAB, 128), F32)]
    scratch += [pltpu.VMEM((X_SIZE, TABLE_SLAB, 128), F32) for _ in range(2)]
    scratch += [pltpu.VMEM((TABLE_ROWS, 128), F32) for _ in range(2)] + type_scratch()
    return call(functools.partial(unpack_kernel, scale), here, ins, outs, scratch, aliases)


def type_scratch():
    return [pltpu.VMEM((TYPE_ROWS, 128), F32) for _ in range(3)]


def pack_scratch():
    return pltpu.VMEM((X_SIZE,) + SLAB_SHAPE.shape, BF16)


def stored_tokens(array):
    return array[0].transpose(1, 2, 0, 3).reshape(TOKENS, MODEL_WIDTH)


def on_device(
    inputs, grad_output, norm_gains, input_weight, output_weight, expand_weight, reduce_weight,
    bias_table,
):
    lat_index = lax.axis_index("lat")
    here = jnp.stack([lat_index, lax.axis_index("x")]).astype(jnp.int32)
    orders = [jnp.asarray(order) for order in quad_orders()]
    split, join_rolled, split_rolled, join, natural, early_split, stored = orders
    reduce_weight = reduce_weight.swapaxes(2, 3)
    bias_table = bias_table.swapaxes(3, 4)
    weights = [
        [(array, one_block(array, block)) for array in
         (norm_gains, input_weight, output_weight, expand_weight, reduce_weight)]
        for block in range(BLOCKS)
    ]
    tables = [[(bias_table, one_block(bias_table, block))] for block in range(BLOCKS)]
    front_scratch = [tall_scratch(), tall_scratch()] + type_scratch()
    front_scratch.append(pltpu.VMEM((8, BIAS_SLOTS), F32))
    outs = call(
        forward_kernel,
        here,
        plain(stored_tokens(inputs), stored_tokens(grad_output)) + weights[0] + tables[0]
        + plain(split, natural, early_split),
        plain(*((PAIR_SHAPE,) * 4 + (TOKEN_SHAPE,) * 3 + (WEIGHT_SHAPE,) + (TOKEN_SHAPE,) * 3)),
        front_scratch,
    )
    saved = outs[4:10]
    tokens = outs[10]
    quads = exchange(outs[:4], -1)
    outs = call(
        turn_kernel,
        here,
        plain(*quads) + weights[1] + tables[1] + plain(join_rolled, split_rolled),
        plain(*((QUAD_SHAPE,) * 4 + (SLAB_SHAPE,) * 4)),
        front_scratch + [pack_scratch()] + [token_scratch() for _ in range(3)]
        + [pltpu.VMEM(WEIGHT_SHAPE.shape, BF16), token_scratch(),
           pltpu.VMEM((3, TOKENS, MODEL_WIDTH), BF16)],
    )
    flow_quads = exchange(outs[:4], 1)
    flow_quads, late = lax.optimization_barrier((flow_quads, outs[4:]))
    late = pass_x(late)
    outs = call(
        backward_kernel,
        here,
        plain(tokens, *flow_quads) + weights[0] + plain(join, stored, *saved),
        plain(*((TOKEN_SHAPE,) + (SLAB_SHAPE,) * 4)),
        [tall_scratch(), tall_scratch(), pack_scratch(),
         pltpu.VMEM((3, TOKENS, MODEL_WIDTH), BF16)],
    )
    grad_flow = outs[0]
    late, early = lax.optimization_barrier((late, outs[1:]))
    early = pass_x(early)
    rest = ("z", "lat")
    count = lax.axis_size(rest)
    lat_total = LAT_DEV * lax.axis_size("lat")
    scale = float(LEVELS * lat_total * LON_DEV * lax.axis_size(("z", "x"))) ** (-0.5)
    (late,) = call(first_kernel, here, plain(*late), plain(parts_shape(count, PART)), [])
    late = swap_all(late, rest)
    (both,) = call(
        second_kernel, here, plain(late, *early), plain(parts_shape(count, 2 * PART)), []
    )
    late, early = call(
        third_kernel, here, plain(swap_all(both, rest)), plain(*(parts_shape(count, PART),) * 2), []
    )
    late = pass_x((late,) * X_SIZE)
    early = pass_x((swap_all(early, rest),) * X_SIZE)
    upstream = lax.ppermute(
        grad_flow, "section", [(i, i - 1) for i in range(1, lax.axis_size("section"))]
    )
    upstream = upstream.reshape(LAT_DEV, LON_DEV, LEVELS, MODEL_WIDTH).transpose(2, 0, 1, 3)[None]
    grads = unpack(late, here, 1, scale, None)
    grads = list(unpack(early, here, 0, scale, grads))
    grads[3] = grads[3].swapaxes(2, 3)
    grads[5] = grads[5].swapaxes(3, 4)
    return (upstream,) + tuple(grads)


def solution(mesh):
    sizes = mesh.shape
    grid = mesh.devices.reshape(
        sizes["section"], sizes["lon"] // X_SIZE, X_SIZE, sizes["lat"]
    )
    mesh = Mesh(grid, ("section", "z", "x", "lat"))
    return jax.shard_map(
        on_device,
        mesh=mesh,
        in_specs=(
            P("section", None, "lat", ("z", "x"), None),
            P("section", None, "lat", ("z", "x"), None),
            P("section", None, None, None),
            P("section", None, None, None),
            P("section", None, None, None),
            P("section", None, None, None),
            P("section", None, None, None),
            P("section", None, None, None, None, None),
        ),
        out_specs=(
            P("section", None, "lat", ("z", "x"), None),
            P("section", None, None, None),
            P("section", None, None, None),
            P("section", None, None, None),
            P("section", None, None, None),
            P("section", None, None, None),
            P("section", None, None, None, None, None),
        ),
        check_vma=False,
    )
```

```python
import functools

import jax
import jax.numpy as jnp
import numpy as np
from jax import lax
from jax.experimental import pallas as pl
from jax.experimental.pallas import tpu as pltpu
from jax.sharding import Mesh
from jax.sharding import PartitionSpec as P

MODEL_WIDTH = 192
HEADS = 6
HEAD_SIZE = 32
LEVELS = 8
WIN_LEVELS = 2
WIN_LAT = 6
WIN_LON = 12
BLOCKS = 2
MLP_WIDTH = 768
LAT_DEV = 6
LON_DEV = 12
LEVEL_WINDOWS = 4
WIN_TOKENS = 144
BIAS_SLOTS = 3312

NORM_EPS = 1e-05
MASK_FILL = -10000.0
GELU_C = 0.7978845608028654
GELU_A = 0.044715

TOKENS = LEVELS * LAT_DEV * LON_DEV
QUAD = TOKENS // 4
STACK = HEADS * WIN_TOKENS
GROUPS = WIN_LEVELS * WIN_LAT
OFFSETS = 2 * WIN_LON - 1
PAIR_LANES = GROUPS * OFFSETS
PAIR_PAD = 384
TYPE_ROWS = LEVEL_WINDOWS * HEADS * GROUPS
X_SIZE = 4
WEIGHT_ROWS = 3456
TABLE_ROWS = 640
GAIN_ROW = 624
WEIGHT_SLAB = WEIGHT_ROWS // X_SIZE
TABLE_SLAB = TABLE_ROWS // X_SIZE
WEIGHT_PART = 54
TABLE_PART = 10
SENT = WEIGHT_PART + TABLE_PART
PART = 80

F32 = jnp.float32
BF16 = jnp.bfloat16


def quad_orders():
    level, row, col = np.meshgrid(
        np.arange(LEVELS), np.arange(LAT_DEV), np.arange(LON_DEV), indexing="ij"
    )
    half_rows, half_cols = WIN_LAT // 2, WIN_LON // 2
    quad = (1 - row // half_rows) * 2 + (1 - col // half_cols)
    place = (quad * LEVELS + level) * (half_rows * half_cols)
    place = place + (row % half_rows) * half_cols + col % half_cols
    split = place.reshape(-1)
    quad_r = (row // half_rows) * 2 + col // half_cols
    from_level = (level + WIN_LEVELS // 2) % LEVELS
    place_r = (quad_r * LEVELS + from_level) * (half_rows * half_cols)
    place_r = place_r + (row % half_rows) * half_cols + col % half_cols
    split_rolled = place_r.reshape(-1)
    join = np.argsort(split)
    join_rolled = np.argsort(split_rolled)
    natural = np.arange(TOKENS).reshape(LEVELS, LAT_DEV, LON_DEV).transpose(1, 2, 0).reshape(-1)
    stored = np.argsort(natural)
    orders = (split, join_rolled, split_rolled, join, natural, split[natural], stored)
    return [order.astype(np.int32)[None, :] for order in orders]


def dot_nn(a, b):
    return jnp.dot(a, b, preferred_element_type=F32)


def dot_nt(a, b):
    return lax.dot_general(a, b, (((1,), (1,)), ((), ())), preferred_element_type=F32)


def dot_tn(a, b):
    return lax.dot_general(a, b, (((0,), (0,)), ((), ())), preferred_element_type=F32)


def reorder(values, order_row):
    rows = lax.broadcasted_iota(jnp.int32, (TOKENS, TOKENS), 0)
    pick = jnp.where(rows == order_row, 1.0, 0.0).astype(BF16)
    return dot_nn(pick, values).astype(BF16)


def norm_stats(values):
    centred = values - jnp.mean(values, axis=-1, keepdims=True)
    spread = jnp.mean(centred * centred, axis=-1, keepdims=True)
    inv = lax.rsqrt(spread + NORM_EPS)
    return centred * inv, inv


def norm_grad(grad, unit, inv, gain_row):
    gain_grad = jnp.sum(grad * unit, axis=0, keepdims=True)
    grad_unit = grad * gain_row
    first = jnp.mean(grad_unit, axis=-1, keepdims=True)
    second = jnp.mean(grad_unit * unit, axis=-1, keepdims=True)
    return inv * (grad_unit - first - unit * second), gain_grad


def head_masks():
    lane = lax.broadcasted_iota(jnp.int32, (1, MODEL_WIDTH), 1)
    return [
        jnp.logical_and(lane >= h * HEAD_SIZE, lane < (h + 1) * HEAD_SIZE) for h in range(HEADS)
    ]


def stack_heads(values, masks):
    wide = values.astype(F32)
    return jnp.concatenate([jnp.where(m, wide, 0.0) for m in masks], axis=0).astype(BF16)


def fold_heads(stacked, masks):
    total = jnp.where(masks[0], stacked[:WIN_TOKENS], 0.0)
    for h in range(1, HEADS):
        total = jnp.where(masks[h], stacked[h * WIN_TOKENS : (h + 1) * WIN_TOKENS], total)
    return total


def pair_pick(query_col):
    key = lax.broadcasted_iota(jnp.int32, (256, PAIR_PAD), 0)
    lane = lax.broadcasted_iota(jnp.int32, (256, PAIR_PAD), 1)
    group = lax.shift_right_logical(key * 5462, 16)
    key_col = key - group * WIN_LON
    target = group * OFFSETS + (WIN_LON - 1 + query_col) - key_col
    hit = jnp.logical_and(lane == target, key < WIN_TOKENS)
    return jnp.where(hit, 1.0, 0.0).astype(BF16)


def segment_start(group, key_level):
    query_level, query_row = group // WIN_LAT, group % WIN_LAT
    return ((query_level * WIN_LEVELS + key_level) * WIN_LAT + query_row) * WIN_LAT * OFFSETS


def load_table(table_ref, side, parts, lines):
    width = WIN_LAT * OFFSETS
    for window in range(LEVEL_WINDOWS):
        for h in range(HEADS):
            lines[h : h + 1, :] = table_ref[0, 0, window, h, pl.ds(side, 1), :]
        rows = lines[:HEADS, :]
        for group in range(GROUPS):
            pieces = []
            for key_level in range(WIN_LEVELS):
                start = segment_start(group, key_level)
                pieces.append(rows[:, start : start + width])
            pieces.append(jnp.zeros((HEADS, PAIR_PAD - PAIR_LANES), F32))
            line = jnp.concatenate(pieces, axis=1)
            place = pl.ds(window * HEADS * GROUPS + group, HEADS, stride=GROUPS)
            for index, part in enumerate(parts):
                part[place, :] = line[:, index * 128 : (index + 1) * 128]
    return jnp.concatenate([part[...] for part in parts], axis=1)


def build_bias(table, bias_a, bias_b):
    high = table.astype(BF16)
    rest = table - high.astype(F32)
    middle = rest.astype(BF16)
    low = (rest - middle.astype(F32)).astype(BF16)
    for query_col in range(WIN_LON):
        pick = pair_pick(query_col)
        spread = dot_nt(high, pick) + dot_nt(middle, pick) + dot_nt(low, pick)
        bias_a[pl.ds(query_col, TYPE_ROWS, stride=WIN_LON), :] = spread[:, :128]
        bias_b[pl.ds(query_col, TYPE_ROWS, stride=WIN_LON), :] = spread[:, 128:]


def fold_table(score_a, score_b):
    total = jnp.zeros((TYPE_ROWS, PAIR_PAD), F32)
    for query_col in range(WIN_LON):
        pick = pair_pick(query_col)
        left = score_a[pl.ds(query_col, TYPE_ROWS, stride=WIN_LON), :]
        right = score_b[pl.ds(query_col, TYPE_ROWS, stride=WIN_LON), :]
        total = total + dot_nn(jnp.concatenate([left, right], axis=1).astype(BF16), pick)
    return total


def shift_mask(window, lat_row):
    shape = (WIN_TOKENS, WIN_TOKENS)
    half = WIN_TOKENS // 2
    parts = []
    for axis in (0, 1):
        token = lax.broadcasted_iota(jnp.int32, shape, axis)
        upper = token >= half
        inner = jnp.where(upper, token - half, token)
        parts.append((upper, inner >= half // 2))
    rows_differ = jnp.where(parts[0][1] != parts[1][1], 1.0, 0.0) * lat_row
    if window == LEVEL_WINDOWS - 1:
        levels_differ = jnp.where(parts[0][0] != parts[1][0], 1.0, 0.0)
        rows_differ = jnp.maximum(rows_differ, levels_differ)
    return rows_differ * MASK_FILL


def attention_front(unit, gain_row, input_weight, bias_a, bias_b, lat_row, q_ref, k_ref, v_ref, w_ref, mix_ref):
    normed = (unit * gain_row).astype(BF16)
    q_ref[...] = (dot_nn(normed, input_weight[:, :MODEL_WIDTH]) * HEAD_SIZE ** (-0.5)).astype(BF16)
    k_ref[...] = dot_nn(normed, input_weight[:, MODEL_WIDTH : 2 * MODEL_WIDTH]).astype(BF16)
    v_ref[...] = dot_nn(normed, input_weight[:, 2 * MODEL_WIDTH :]).astype(BF16)
    masks = head_masks()
    for window in range(LEVEL_WINDOWS):
        rows = pl.ds(window * WIN_TOKENS, WIN_TOKENS)
        stack_rows = pl.ds(window * STACK, STACK)
        queries = stack_heads(q_ref[rows, :], masks)
        scores = dot_nt(queries, k_ref[rows, :])
        bias = jnp.concatenate(
            [bias_a[stack_rows, :], bias_b[stack_rows, :][:, : WIN_TOKENS - 128]], axis=1
        )
        scores = scores + bias
        if lat_row is not None:
            mask = shift_mask(window, lat_row)
            scores = scores + jnp.concatenate([mask] * HEADS, axis=0)
        scores = jnp.exp(scores - jnp.max(scores, axis=-1, keepdims=True))
        weights = (scores / jnp.sum(scores, axis=-1, keepdims=True)).astype(BF16)
        w_ref[stack_rows, :] = weights
        mixed = dot_nn(weights, v_ref[rows, :])
        mix_ref[rows, :] = fold_heads(mixed, masks).astype(BF16)
    return normed


def gelu_parts(pre):
    square = pre * pre
    tanh = jnp.tanh(GELU_C * (pre + GELU_A * pre * square))
    half = 0.5 * (1.0 + tanh)
    slope = half + 0.5 * pre * (1.0 - tanh * tanh) * (GELU_C * (1.0 + 3.0 * GELU_A * square))
    return pre * half, slope


def pack_rows(out_ref, first, values, slab, base):
    done = 0
    while done < values.shape[0]:
        side, inner = (first + done) // slab, (first + done) % slab
        count = min(values.shape[0] - done, slab - inner)
        out_ref[side, pl.ds(base + inner, count), :] = values[done : done + count].astype(BF16)
        done += count


def pack_columns(out_ref, first, values, slab=WEIGHT_SLAB, base=0):
    rows, lanes = values.shape
    for block in range(lanes // 128):
        pack_rows(
            out_ref, first + block * rows, values[:, block * 128 : (block + 1) * 128], slab, base
        )


def backward(e, x_unit, x_inv, gains, middle, weights4, saved, keep_scores, pack_ref, gproj_ref):
    input_weight, output_weight, expand_weight, reduce_weight = weights4
    q_ref, k_ref, v_ref, w_ref, mix_ref = saved
    masks = head_masks()
    mid_unit, mid_inv = norm_stats(middle.astype(F32))
    gain_mid = gains[1:2, :]
    normed_mid = (mid_unit * gain_mid).astype(BF16)
    hidden, slope = gelu_parts(dot_nn(normed_mid, expand_weight))
    hidden = hidden.astype(BF16)
    grad_pre = (slope * dot_nn(e, reduce_weight)).astype(BF16)
    pack_columns(pack_ref, 2304, dot_tn(e, hidden))
    pack_columns(pack_ref, 1152, dot_tn(normed_mid, grad_pre))
    grad_norm, gain_mid_grad = norm_grad(dot_nt(grad_pre, expand_weight), mid_unit, mid_inv, gain_mid)
    grad_middle = e.astype(F32) + grad_norm
    grad_attended = grad_middle.astype(BF16)
    output_grad = dot_tn(mix_ref[...], grad_attended)
    grad_mixture = dot_nt(grad_attended, output_weight).astype(BF16)
    for window in range(LEVEL_WINDOWS):
        base = window * WIN_TOKENS
        rows = pl.ds(base, WIN_TOKENS)
        stack_rows = pl.ds(window * STACK, STACK)
        queries = stack_heads(q_ref[rows, :], masks)
        grads = stack_heads(grad_mixture[base : base + WIN_TOKENS], masks)
        weights = w_ref[stack_rows, :]
        keys = k_ref[rows, :]
        gproj_ref[2, rows, :] = dot_tn(weights, grads).astype(BF16)
        grad_weights = dot_nt(grads, v_ref[rows, :])
        attention = weights.astype(F32)
        moved = attention * grad_weights
        grad_scores = attention * (grad_weights - jnp.sum(moved, axis=-1, keepdims=True))
        score_part = grad_scores.astype(BF16)
        keep_scores(stack_rows, grad_scores, score_part)
        grad_queries = fold_heads(dot_nn(score_part, keys), masks) * HEAD_SIZE ** (-0.5)
        gproj_ref[0, rows, :] = grad_queries.astype(BF16)
        gproj_ref[1, rows, :] = dot_tn(score_part, queries).astype(BF16)
    normed = (x_unit * gains[0:1, :]).astype(BF16)
    parts = [gproj_ref[part] for part in range(3)]
    weight_grads = [dot_tn(normed, part) for part in parts] + [output_grad]
    pack_columns(pack_ref, 0, jnp.concatenate(weight_grads, axis=1))
    grad_normed = dot_nt(parts[0], input_weight[:, :MODEL_WIDTH])
    grad_normed = grad_normed + dot_nt(parts[1], input_weight[:, MODEL_WIDTH : 2 * MODEL_WIDTH])
    grad_normed = grad_normed + dot_nt(parts[2], input_weight[:, 2 * MODEL_WIDTH :])
    grad_normed = grad_normed.astype(BF16).astype(F32)
    grad_in, gain_in_grad = norm_grad(grad_normed, x_unit, x_inv, gains[0:1, :])
    gain_flat = jnp.concatenate([gain_in_grad, gain_mid_grad], axis=1)
    gain_rows = [gain_flat[:, i * 128 : (i + 1) * 128] for i in range(3)]
    gain_rows.append(jnp.zeros((TABLE_ROWS - GAIN_ROW - 3, 128), F32))
    result = (grad_middle + grad_in).astype(BF16)
    return result, jnp.concatenate(gain_rows, axis=0)


def keep_split(score_a, score_b):
    def keep(stack_rows, grad_scores, score_part):
        score_a[stack_rows, :] = grad_scores[:, :128]
        score_b[stack_rows, :] = jnp.concatenate(
            [grad_scores[:, 128:], jnp.zeros((STACK, 256 - WIN_TOKENS), F32)], axis=1
        )

    return keep


def pack_table(pack_ref, score_a, score_b, gain_rows, base):
    folded = fold_table(score_a, score_b)
    pack_columns(pack_ref, 0, folded[:, :256], TABLE_SLAB, base)
    tail = TYPE_ROWS // HEADS
    pieces = [folded[h * tail : (h + 1) * tail, 256:PAIR_LANES] for h in range(HEADS)]
    pieces.append(jnp.zeros((tail, 128 - HEADS * (PAIR_LANES - 256)), F32))
    rest = jnp.concatenate([jnp.concatenate(pieces, axis=1), gain_rows], axis=0)
    pack_rows(pack_ref, 2 * TYPE_ROWS, rest, TABLE_SLAB, base)


def forward_kernel(
    here_ref, x_ref, e_ref, gains_ref, wi_ref, wo_ref, we_ref, wr_ref, table_ref, order_ref,
    natural_ref, early_ref, quad0, quad1, quad2, quad3, q_ref, k_ref, v_ref, w_ref, mix_ref, mid_ref, tok_ref,
    bias_a, bias_b, part_a, part_b, part_c, lines,
):
    build_bias(load_table(table_ref, here_ref[0], (part_a, part_b, part_c), lines), bias_a, bias_b)
    gains = gains_ref[0, 0]
    order = order_ref[...]
    quads = (quad0, quad1, quad2, quad3)
    moved = reorder(e_ref[...], early_ref[...])
    for index, quad in enumerate(quads):
        quad[1] = moved[index * QUAD : (index + 1) * QUAD]
    tokens = reorder(x_ref[...], natural_ref[...])
    tok_ref[...] = tokens
    values = tokens.astype(F32)
    unit, _ = norm_stats(values)
    attention_front(
        unit, gains[0:1, :], wi_ref[0, 0], bias_a, bias_b, None, q_ref, k_ref, v_ref, w_ref, mix_ref
    )
    middle = (values + dot_nn(mix_ref[...], wo_ref[0, 0])).astype(BF16)
    mid_ref[...] = middle
    mid_f = middle.astype(F32)
    mid_unit, _ = norm_stats(mid_f)
    normed_mid = (mid_unit * gains[1:2, :]).astype(BF16)
    hidden, _ = gelu_parts(dot_nn(normed_mid, we_ref[0, 0]))
    output = (mid_f + dot_nt(hidden.astype(BF16), wr_ref[0, 0])).astype(BF16)
    moved = reorder(output, order)
    for index, quad in enumerate(quads):
        quad[0] = moved[index * QUAD : (index + 1) * QUAD]


def bias_kernel(here_ref, table_ref, gate_ref, bias_a, bias_b, part_a, part_b, part_c, lines):
    build_bias(load_table(table_ref, here_ref[0], (part_a, part_b, part_c), lines), bias_a, bias_b)


def turn_kernel(
    here_ref, x0, x1, x2, x3, gains_ref, wi_ref, wo_ref, we_ref, wr_ref, bias_a, bias_b,
    join_ref, split_ref, quad0, quad1, quad2, quad3, pack_ref, score_ref, gain_ref,
    q_ref, k_ref, v_ref, w_ref, mix_ref, gproj_ref,
):
    gains = gains_ref[0, 0]
    join = join_ref[...]
    pieces = (x0, x1, x2, x3)
    block_in = reorder(jnp.concatenate([piece[0] for piece in pieces], axis=0), join)
    e = reorder(jnp.concatenate([piece[1] for piece in pieces], axis=0), join)
    values = block_in.astype(F32)
    unit, inv = norm_stats(values)
    input_weight, output_weight = wi_ref[0, 0], wo_ref[0, 0]
    attention_front(
        unit, gains[0:1, :], input_weight, bias_a, bias_b, here_ref[0].astype(F32), q_ref, k_ref,
        v_ref, w_ref, mix_ref,
    )
    attended = dot_nn(mix_ref[...], output_weight).astype(BF16).astype(F32)
    middle = (values + attended).astype(BF16)

    def keep(stack_rows, grad_scores, score_part):
        score_ref[stack_rows, :] = score_part

    result, gain_ref[...] = backward(
        e, unit, inv, gains, middle, (input_weight, output_weight, we_ref[0, 0], wr_ref[0, 0]),
        (q_ref, k_ref, v_ref, w_ref, mix_ref), keep, pack_ref, gproj_ref,
    )
    moved = reorder(result, split_ref[...])
    for index, quad in enumerate((quad0, quad1, quad2, quad3)):
        quad[...] = moved[index * QUAD : (index + 1) * QUAD]


def late_kernel(
    here_ref, pack_ref, score_ref, gain_ref, send0, send1, send2, send3, score_a, score_b, table_ref
):
    keep = keep_split(score_a, score_b)
    for window in range(LEVEL_WINDOWS):
        stack_rows = pl.ds(window * STACK, STACK)
        keep(stack_rows, score_ref[stack_rows, :].astype(F32), None)
    pack_table(table_ref, score_a, score_b, gain_ref[...], 0)
    for step, send in enumerate((send0, send1, send2, send3)):
        owner = lax.rem(here_ref[1] + step, X_SIZE)
        send[pl.ds(0, WEIGHT_SLAB), :] = pack_ref[owner]
        send[pl.ds(WEIGHT_SLAB, TABLE_SLAB), :] = table_ref[owner]


def send_slabs(here_ref, pack_ref, sends):
    for step, send in enumerate(sends):
        send[...] = pack_ref[lax.rem(here_ref[1] + step, X_SIZE)]


def backward_kernel(
    here_ref, x_ref, e0, e1, e2, e3, gains_ref, wi_ref, wo_ref, we_ref, wr_ref, join_ref,
    stored_ref, q_ref, k_ref, v_ref, w_ref, mix_ref, mid_ref, out_ref, send0, send1, send2, send3,
    score_a, score_b, pack_ref, gproj_ref,
):
    e = reorder(jnp.concatenate([e0[...], e1[...], e2[...], e3[...]], axis=0), join_ref[...])
    unit, inv = norm_stats(x_ref[...].astype(F32))
    result, gain_rows = backward(
        e, unit, inv, gains_ref[0, 0], mid_ref[...],
        (wi_ref[0, 0], wo_ref[0, 0], we_ref[0, 0], wr_ref[0, 0]),
        (q_ref, k_ref, v_ref, w_ref, mix_ref), keep_split(score_a, score_b), pack_ref, gproj_ref,
    )
    pack_table(pack_ref, score_a, score_b, gain_rows, WEIGHT_SLAB)
    out_ref[...] = reorder(result, stored_ref[...])
    send_slabs(here_ref, pack_ref, (send0, send1, send2, send3))


def unpack_kernel(scale, here_ref, got0, got1, got2, got3, *refs):
    gi_ref, go_ref, ge_ref, gr_ref, gn_ref, gt_ref = refs[-14:-8]
    rows, slab0, slab1, t0, t1, part_a, part_b, part_c = refs[-8:]
    for step, got in enumerate((got0, got1, got2, got3)):
        origin = lax.rem(here_ref[1] + X_SIZE - step, X_SIZE)
        for index in range(got.shape[0]):
            part = got[index].astype(F32)
            rows[origin, pl.ds(index * WEIGHT_PART, WEIGHT_PART), :] = part[:WEIGHT_PART] * scale
            for side, table in enumerate((slab0, slab1)):
                first = WEIGHT_PART + side * TABLE_PART
                table[origin, pl.ds(index * TABLE_PART, TABLE_PART), :] = part[
                    first : first + TABLE_PART
                ]
    for slab, table in ((slab0, t0), (slab1, t1)):
        for origin in range(X_SIZE):
            table[pl.ds(origin * TABLE_SLAB, TABLE_SLAB), :] = slab[origin]

    def block(first, count):
        pieces = []
        while count:
            origin, inner = first // WEIGHT_SLAB, first % WEIGHT_SLAB
            here = min(count, WEIGHT_SLAB - inner)
            pieces.append(rows[origin, pl.ds(inner, here), :])
            first, count = first + here, count - here
        return pieces[0] if len(pieces) == 1 else jnp.concatenate(pieces, axis=0)

    for index in range(4):
        gi_ref[0, 0, :, pl.ds(index * 128, 128)] = block(index * 192, 192)
    mixed = block(4 * 192, 192)
    gi_ref[0, 0, :, pl.ds(512, 64)] = mixed[:, :64]
    go_ref[0, 0] = jnp.concatenate([mixed[:, 64:], block(5 * 192, 192)], axis=1)
    for index in range(6):
        ge_ref[0, 0, :, pl.ds(index * 128, 128)] = block(1152 + index * 192, 192)
    for index in range(6):
        gr_ref[0, 0, :, pl.ds(index * 128, 128)] = block(2304 + index * 192, 192)
    gain = (t0[pl.ds(GAIN_ROW, 8), :] + t1[pl.ds(GAIN_ROW, 8), :]) * scale
    gn_ref[0, 0, 0:1, :] = jnp.concatenate([gain[0:1], gain[1:2, :64]], axis=1)
    gn_ref[0, 0, 1:2, :] = jnp.concatenate([gain[1:2, 64:], gain[2:3]], axis=1)
    tail, width = TYPE_ROWS // HEADS, PAIR_LANES - 256
    for side, table in enumerate((t0, t1)):
        rest = table[pl.ds(2 * TYPE_ROWS, tail), :]
        for h in range(HEADS):
            part_c[pl.ds(h * tail, tail), pl.ds(0, width)] = rest[:, h * width : (h + 1) * width]
        for window in range(LEVEL_WINDOWS):
            lines = []
            for group in range(GROUPS):
                first = window * HEADS * GROUPS + group
                place = pl.ds(first, HEADS, stride=GROUPS)
                upper = pl.ds(TYPE_ROWS + first, HEADS, stride=GROUPS)
                lines.append(
                    jnp.concatenate([table[place, :], table[upper, :], part_c[place, :]], axis=1)
                )
            span = WIN_LAT * OFFSETS
            ordered = []
            for query_level in range(WIN_LEVELS):
                for key_level in range(WIN_LEVELS):
                    for row in range(WIN_LAT):
                        line = lines[query_level * WIN_LAT + row]
                        ordered.append(line[:, key_level * span : (key_level + 1) * span])
            result = jnp.concatenate(ordered, axis=1)
            for h in range(HEADS):
                gt_ref[0, 0, window, h, side : side + 1, :] = result[h : h + 1]


LIMIT = 32 * 1024 * 1024
TOKEN_SHAPE = jax.ShapeDtypeStruct((TOKENS, MODEL_WIDTH), BF16)
QUAD_SHAPE = jax.ShapeDtypeStruct((QUAD, MODEL_WIDTH), BF16)
WEIGHT_SHAPE = jax.ShapeDtypeStruct((LEVEL_WINDOWS * STACK, WIN_TOKENS), BF16)
BIAS_SHAPE = jax.ShapeDtypeStruct((LEVEL_WINDOWS * STACK, 128), F32)
GAIN_SHAPE = jax.ShapeDtypeStruct((TABLE_ROWS - GAIN_ROW, 128), F32)
HALF_PACK_SHAPE = jax.ShapeDtypeStruct((X_SIZE, WEIGHT_SLAB, 128), BF16)
SLAB_SHAPE = jax.ShapeDtypeStruct((WEIGHT_SLAB + TABLE_SLAB, 128), BF16)
PAIR_SHAPE = jax.ShapeDtypeStruct((2, QUAD, MODEL_WIDTH), BF16)
GRAD_SHAPES = tuple(
    jax.ShapeDtypeStruct((1, BLOCKS) + shape, F32)
    for shape in (
        (MODEL_WIDTH, 3 * MODEL_WIDTH), (MODEL_WIDTH, MODEL_WIDTH), (MODEL_WIDTH, MLP_WIDTH),
        (MODEL_WIDTH, MLP_WIDTH), (2, MODEL_WIDTH), (LEVEL_WINDOWS, HEADS, 2, BIAS_SLOTS),
    )
)


def tall_scratch():
    return pltpu.VMEM((LEVEL_WINDOWS * STACK, 128), F32)


def token_scratch():
    return pltpu.VMEM((TOKENS, MODEL_WIDTH), BF16)


def whole(array):
    rank = len(array.shape)
    return pl.BlockSpec(array.shape, lambda i, lat: (0,) * rank)


def one_block(array, index):
    rank = len(array.shape)
    return pl.BlockSpec((1, 1) + array.shape[2:], lambda i, lat: (0, index) + (0,) * (rank - 2))


def call(kernel, lat, ins, outs, scratch, aliases=None):
    arrays = [array for array, _ in ins]
    return pl.pallas_call(
        kernel,
        out_shape=tuple(shape for shape, _ in outs),
        grid_spec=pltpu.PrefetchScalarGridSpec(
            num_scalar_prefetch=1,
            grid=(1,),
            in_specs=[spec for _, spec in ins],
            out_specs=tuple(spec for _, spec in outs),
            scratch_shapes=scratch,
        ),
        input_output_aliases=aliases or {},
        compiler_params=pltpu.CompilerParams(vmem_limit_bytes=LIMIT),
    )(lat, *arrays)


def plain(*arrays):
    return [(array, whole(array)) for array in arrays]


def exchange(quads, by):
    lon = ("z", "x")
    ring, sides = lax.axis_size(lon), lax.axis_size("lat")
    lon_pairs = [(i, (i + by) % ring) for i in range(ring)]
    swap = [(i, i ^ 1) for i in range(sides)]
    both = [
        (i * sides + j, ((i + by) % ring) * sides + (j ^ 1)) for i in range(ring) for j in range(sides)
    ]
    return (
        quads[0],
        lax.ppermute(quads[1], lon, lon_pairs),
        lax.ppermute(quads[2], "lat", swap),
        lax.ppermute(quads[3], lon + ("lat",), both),
    )


def swap_all(values, axes):
    return lax.all_to_all(values, axes, split_axis=0, concat_axis=0, tiled=True)


def pass_x(sends):
    size = lax.axis_size("x")
    return (sends[0],) + tuple(
        lax.ppermute(sends[step], "x", [(i, (i + step) % size) for i in range(size)])
        for step in range(1, size)
    )


def slab_sum(slabs):
    total = slabs[0][...].astype(F32)
    for slab in slabs[1:]:
        total = total + slab[...].astype(F32)
    return total


def write_parts(total, out_ref, first):
    for index in range(out_ref.shape[0]):
        weights = total[index * WEIGHT_PART : (index + 1) * WEIGHT_PART]
        start = WEIGHT_SLAB + index * TABLE_PART
        part = jnp.concatenate([weights, total[start : start + TABLE_PART]], axis=0)
        out_ref[index, pl.ds(first, SENT), :] = part.astype(BF16)


def part_sum(spread_ref, first):
    sides = []
    for side in range(2):
        total = spread_ref[side, pl.ds(first, SENT), :].astype(F32)
        for index in range(side + 2, spread_ref.shape[0], 2):
            total = total + spread_ref[index, pl.ds(first, SENT), :].astype(F32)
        sides.append(total)
    weights = sides[0][:WEIGHT_PART] + sides[1][:WEIGHT_PART]
    spare = jnp.zeros((PART - SENT - TABLE_PART, 128), F32)
    rows = [weights, sides[0][WEIGHT_PART:], sides[1][WEIGHT_PART:], spare]
    return jnp.concatenate(rows, axis=0).astype(BF16)


def first_kernel(here_ref, slab0, slab1, slab2, slab3, out_ref):
    write_parts(slab_sum((slab0, slab1, slab2, slab3)), out_ref, 0)


def second_kernel(here_ref, late_ref, slab0, slab1, slab2, slab3, out_ref):
    late = part_sum(late_ref, 0)
    for index in range(out_ref.shape[0]):
        out_ref[index, pl.ds(0, PART), :] = late
    write_parts(slab_sum((slab0, slab1, slab2, slab3)), out_ref, PART)


def third_kernel(here_ref, both_ref, late_ref, early_ref):
    early = part_sum(both_ref, PART)
    for index in range(late_ref.shape[0]):
        late_ref[index] = both_ref[index, pl.ds(0, PART), :]
        early_ref[index] = early


def parts_shape(count, width):
    return jax.ShapeDtypeStruct((count, width, 128), BF16)


def unpack(parts, here, index, scale, previous):
    ins = plain(*parts)
    aliases = {}
    if previous is not None:
        ins = ins + [(array, pl.BlockSpec(memory_space=pl.ANY)) for array in previous]
        aliases = {1 + len(parts) + place: place for place in range(6)}
    outs = [(shape, one_block(shape, index)) for shape in GRAD_SHAPES]
    scratch = [pltpu.VMEM((X_SIZE, WEIGHT_SLAB, 128), F32)]
    scratch += [pltpu.VMEM((X_SIZE, TABLE_SLAB, 128), F32) for _ in range(2)]
    scratch += [pltpu.VMEM((TABLE_ROWS, 128), F32) for _ in range(2)] + type_scratch()
    return call(functools.partial(unpack_kernel, scale), here, ins, outs, scratch, aliases)


def type_scratch():
    return [pltpu.VMEM((TYPE_ROWS, 128), F32) for _ in range(3)]


def pack_scratch():
    return pltpu.VMEM((X_SIZE,) + SLAB_SHAPE.shape, BF16)


def stored_tokens(array):
    return array[0].transpose(1, 2, 0, 3).reshape(TOKENS, MODEL_WIDTH)


def on_device(
    inputs, grad_output, norm_gains, input_weight, output_weight, expand_weight, reduce_weight,
    bias_table,
):
    lat_index = lax.axis_index("lat")
    here = jnp.stack([lat_index, lax.axis_index("x")]).astype(jnp.int32)
    orders = [jnp.asarray(order) for order in quad_orders()]
    split, join_rolled, split_rolled, join, natural, early_split, stored = orders
    reduce_weight = reduce_weight.swapaxes(2, 3)
    bias_table = bias_table.swapaxes(3, 4)
    weights = [
        [(array, one_block(array, block)) for array in
         (norm_gains, input_weight, output_weight, expand_weight, reduce_weight)]
        for block in range(BLOCKS)
    ]
    tables = [[(bias_table, one_block(bias_table, block))] for block in range(BLOCKS)]
    front_scratch = [tall_scratch(), tall_scratch()] + type_scratch()
    front_scratch.append(pltpu.VMEM((8, BIAS_SLOTS), F32))
    outs = call(
        forward_kernel,
        here,
        plain(stored_tokens(inputs), stored_tokens(grad_output)) + weights[0] + tables[0]
        + plain(split, natural, early_split),
        plain(*((PAIR_SHAPE,) * 4 + (TOKEN_SHAPE,) * 3 + (WEIGHT_SHAPE,) + (TOKEN_SHAPE,) * 3)),
        front_scratch,
    )
    saved = outs[4:10]
    tokens = outs[10]
    quads = exchange(outs[:4], -1)
    gate = outs[0]
    bias = call(
        bias_kernel,
        here,
        tables[1] + [(gate, pl.BlockSpec(memory_space=pl.ANY))],
        plain(BIAS_SHAPE, BIAS_SHAPE),
        front_scratch[2:],
    )
    outs = call(
        turn_kernel,
        here,
        plain(*quads) + weights[1] + plain(*bias, join_rolled, split_rolled),
        plain(*((QUAD_SHAPE,) * 4 + (HALF_PACK_SHAPE, WEIGHT_SHAPE, GAIN_SHAPE))),
        [token_scratch() for _ in range(3)]
        + [pltpu.VMEM(WEIGHT_SHAPE.shape, BF16), token_scratch(),
           pltpu.VMEM((3, TOKENS, MODEL_WIDTH), BF16)],
    )
    flow_quads = exchange(outs[:4], 1)
    late = call(
        late_kernel,
        here,
        plain(*outs[4:]),
        plain(*(SLAB_SHAPE,) * 4),
        [tall_scratch(), tall_scratch(), pltpu.VMEM((X_SIZE, TABLE_SLAB, 128), BF16)],
    )
    flow_quads, late = lax.optimization_barrier((flow_quads, late))
    late = pass_x(late)
    outs = call(
        backward_kernel,
        here,
        plain(tokens, *flow_quads) + weights[0] + plain(join, stored, *saved),
        plain(*((TOKEN_SHAPE,) + (SLAB_SHAPE,) * 4)),
        [tall_scratch(), tall_scratch(), pack_scratch(),
         pltpu.VMEM((3, TOKENS, MODEL_WIDTH), BF16)],
    )
    grad_flow = outs[0]
    late, early = lax.optimization_barrier((late, outs[1:]))
    early = pass_x(early)
    rest = ("z", "lat")
    count = lax.axis_size(rest)
    lat_total = LAT_DEV * lax.axis_size("lat")
    scale = float(LEVELS * lat_total * LON_DEV * lax.axis_size(("z", "x"))) ** (-0.5)
    (late,) = call(first_kernel, here, plain(*late), plain(parts_shape(count, SENT)), [])
    late = swap_all(late, rest)
    (both,) = call(
        second_kernel, here, plain(late, *early), plain(parts_shape(count, PART + SENT)), []
    )
    late, early = call(
        third_kernel, here, plain(swap_all(both, rest)), plain(*(parts_shape(count, PART),) * 2), []
    )
    late = pass_x((late,) * X_SIZE)
    early = pass_x((swap_all(early, rest),) * X_SIZE)
    upstream = lax.ppermute(
        grad_flow, "section", [(i, i - 1) for i in range(1, lax.axis_size("section"))]
    )
    upstream = upstream.reshape(LAT_DEV, LON_DEV, LEVELS, MODEL_WIDTH).transpose(2, 0, 1, 3)[None]
    grads = unpack(late, here, 1, scale, None)
    grads = list(unpack(early, here, 0, scale, grads))
    grads[3] = grads[3].swapaxes(2, 3)
    grads[5] = grads[5].swapaxes(3, 4)
    return (upstream,) + tuple(grads)


def solution(mesh):
    sizes = mesh.shape
    grid = mesh.devices.reshape(
        sizes["section"], sizes["lon"] // X_SIZE, X_SIZE, sizes["lat"]
    )
    mesh = Mesh(grid, ("section", "z", "x", "lat"))
    return jax.shard_map(
        on_device,
        mesh=mesh,
        in_specs=(
            P("section", None, "lat", ("z", "x"), None),
            P("section", None, "lat", ("z", "x"), None),
            P("section", None, None, None),
            P("section", None, None, None),
            P("section", None, None, None),
            P("section", None, None, None),
            P("section", None, None, None),
            P("section", None, None, None, None, None),
        ),
        out_specs=(
            P("section", None, "lat", ("z", "x"), None),
            P("section", None, None, None),
            P("section", None, None, None),
            P("section", None, None, None),
            P("section", None, None, None),
            P("section", None, None, None),
            P("section", None, None, None, None, None),
        ),
        check_vma=False,
    )
```

```python
import functools

import jax
import jax.numpy as jnp
import numpy as np
from jax import lax
from jax.experimental import pallas as pl
from jax.experimental.pallas import tpu as pltpu
from jax.sharding import Mesh
from jax.sharding import PartitionSpec as P

MODEL_WIDTH = 192
HEADS = 6
HEAD_SIZE = 32
LEVELS = 8
WIN_LEVELS = 2
WIN_LAT = 6
WIN_LON = 12
BLOCKS = 2
MLP_WIDTH = 768
LAT_DEV = 6
LON_DEV = 12
LEVEL_WINDOWS = 4
WIN_TOKENS = 144
BIAS_SLOTS = 3312

NORM_EPS = 1e-05
MASK_FILL = -10000.0
GELU_C = 0.7978845608028654
GELU_A = 0.044715

TOKENS = LEVELS * LAT_DEV * LON_DEV
QUAD = TOKENS // 4
STACK = HEADS * WIN_TOKENS
GROUPS = WIN_LEVELS * WIN_LAT
OFFSETS = 2 * WIN_LON - 1
PAIR_LANES = GROUPS * OFFSETS
PAIR_PAD = 384
TYPE_ROWS = LEVEL_WINDOWS * HEADS * GROUPS
X_SIZE = 4
WEIGHT_ROWS = 3456
TABLE_ROWS = 640
GAIN_ROW = 624
WEIGHT_SLAB = WEIGHT_ROWS // X_SIZE
TABLE_SLAB = TABLE_ROWS // X_SIZE
WEIGHT_PART = 54
TABLE_PART = 10
SENT = WEIGHT_PART + TABLE_PART
PART = 80

F32 = jnp.float32
BF16 = jnp.bfloat16


def quad_orders():
    level, row, col = np.meshgrid(
        np.arange(LEVELS), np.arange(LAT_DEV), np.arange(LON_DEV), indexing="ij"
    )
    half_rows, half_cols = WIN_LAT // 2, WIN_LON // 2
    quad = (1 - row // half_rows) * 2 + (1 - col // half_cols)
    place = (quad * LEVELS + level) * (half_rows * half_cols)
    place = place + (row % half_rows) * half_cols + col % half_cols
    split = place.reshape(-1)
    quad_r = (row // half_rows) * 2 + col // half_cols
    from_level = (level + WIN_LEVELS // 2) % LEVELS
    place_r = (quad_r * LEVELS + from_level) * (half_rows * half_cols)
    place_r = place_r + (row % half_rows) * half_cols + col % half_cols
    split_rolled = place_r.reshape(-1)
    join = np.argsort(split)
    join_rolled = np.argsort(split_rolled)
    natural = np.arange(TOKENS).reshape(LEVELS, LAT_DEV, LON_DEV).transpose(1, 2, 0).reshape(-1)
    stored = np.argsort(natural)
    orders = (split, join_rolled, split_rolled, join, natural, split[natural], stored)
    return [order.astype(np.int32)[None, :] for order in orders]


def dot_nn(a, b):
    return jnp.dot(a, b, preferred_element_type=F32)


def dot_nt(a, b):
    return lax.dot_general(a, b, (((1,), (1,)), ((), ())), preferred_element_type=F32)


def dot_tn(a, b):
    return lax.dot_general(a, b, (((0,), (0,)), ((), ())), preferred_element_type=F32)


def reorder(values, order_row):
    rows = lax.broadcasted_iota(jnp.int32, (TOKENS, TOKENS), 0)
    pick = jnp.where(rows == order_row, 1.0, 0.0).astype(BF16)
    return dot_nn(pick, values).astype(BF16)


def norm_stats(values):
    centred = values - jnp.mean(values, axis=-1, keepdims=True)
    spread = jnp.mean(centred * centred, axis=-1, keepdims=True)
    inv = lax.rsqrt(spread + NORM_EPS)
    return centred * inv, inv


def norm_grad(grad, unit, inv, gain_row):
    gain_grad = jnp.sum(grad * unit, axis=0, keepdims=True)
    grad_unit = grad * gain_row
    first = jnp.mean(grad_unit, axis=-1, keepdims=True)
    second = jnp.mean(grad_unit * unit, axis=-1, keepdims=True)
    return inv * (grad_unit - first - unit * second), gain_grad


def head_masks():
    lane = lax.broadcasted_iota(jnp.int32, (1, MODEL_WIDTH), 1)
    return [
        jnp.logical_and(lane >= h * HEAD_SIZE, lane < (h + 1) * HEAD_SIZE) for h in range(HEADS)
    ]


def stack_heads(values, masks):
    wide = values.astype(F32)
    return jnp.concatenate([jnp.where(m, wide, 0.0) for m in masks], axis=0).astype(BF16)


def fold_heads(stacked, masks):
    total = jnp.where(masks[0], stacked[:WIN_TOKENS], 0.0)
    for h in range(1, HEADS):
        total = jnp.where(masks[h], stacked[h * WIN_TOKENS : (h + 1) * WIN_TOKENS], total)
    return total


def pair_pick(query_col):
    key = lax.broadcasted_iota(jnp.int32, (256, PAIR_PAD), 0)
    lane = lax.broadcasted_iota(jnp.int32, (256, PAIR_PAD), 1)
    group = lax.shift_right_logical(key * 5462, 16)
    key_col = key - group * WIN_LON
    target = group * OFFSETS + (WIN_LON - 1 + query_col) - key_col
    hit = jnp.logical_and(lane == target, key < WIN_TOKENS)
    return jnp.where(hit, 1.0, 0.0).astype(BF16)


def segment_start(group, key_level):
    query_level, query_row = group // WIN_LAT, group % WIN_LAT
    return ((query_level * WIN_LEVELS + key_level) * WIN_LAT + query_row) * WIN_LAT * OFFSETS


def load_table(table_ref, side, parts, lines):
    width = WIN_LAT * OFFSETS
    for window in range(LEVEL_WINDOWS):
        for h in range(HEADS):
            lines[h : h + 1, :] = table_ref[0, 0, window, h, pl.ds(side, 1), :]
        rows = lines[:HEADS, :]
        for group in range(GROUPS):
            pieces = []
            for key_level in range(WIN_LEVELS):
                start = segment_start(group, key_level)
                pieces.append(rows[:, start : start + width])
            pieces.append(jnp.zeros((HEADS, PAIR_PAD - PAIR_LANES), F32))
            line = jnp.concatenate(pieces, axis=1)
            place = pl.ds(window * HEADS * GROUPS + group, HEADS, stride=GROUPS)
            for index, part in enumerate(parts):
                part[place, :] = line[:, index * 128 : (index + 1) * 128]
    return jnp.concatenate([part[...] for part in parts], axis=1)


def build_bias(table, bias_a, bias_b):
    high = table.astype(BF16)
    rest = table - high.astype(F32)
    middle = rest.astype(BF16)
    low = (rest - middle.astype(F32)).astype(BF16)
    for query_col in range(WIN_LON):
        pick = pair_pick(query_col)
        spread = dot_nt(high, pick) + dot_nt(middle, pick) + dot_nt(low, pick)
        bias_a[pl.ds(query_col, TYPE_ROWS, stride=WIN_LON), :] = spread[:, :128]
        bias_b[pl.ds(query_col, TYPE_ROWS, stride=WIN_LON), :] = spread[:, 128:]


def fold_table(score_a, score_b):
    total = jnp.zeros((TYPE_ROWS, PAIR_PAD), F32)
    for query_col in range(WIN_LON):
        pick = pair_pick(query_col)
        left = score_a[pl.ds(query_col, TYPE_ROWS, stride=WIN_LON), :]
        right = score_b[pl.ds(query_col, TYPE_ROWS, stride=WIN_LON), :]
        total = total + dot_nn(jnp.concatenate([left, right], axis=1).astype(BF16), pick)
    return total


def shift_mask(window, lat_row):
    shape = (WIN_TOKENS, WIN_TOKENS)
    half = WIN_TOKENS // 2
    parts = []
    for axis in (0, 1):
        token = lax.broadcasted_iota(jnp.int32, shape, axis)
        upper = token >= half
        inner = jnp.where(upper, token - half, token)
        parts.append((upper, inner >= half // 2))
    rows_differ = jnp.where(parts[0][1] != parts[1][1], 1.0, 0.0) * lat_row
    if window == LEVEL_WINDOWS - 1:
        levels_differ = jnp.where(parts[0][0] != parts[1][0], 1.0, 0.0)
        rows_differ = jnp.maximum(rows_differ, levels_differ)
    return rows_differ * MASK_FILL


def attention_front(unit, gain_row, input_weight, bias_a, bias_b, lat_row, q_ref, k_ref, v_ref, w_ref, mix_ref):
    normed = (unit * gain_row).astype(BF16)
    q_ref[...] = (dot_nn(normed, input_weight[:, :MODEL_WIDTH]) * HEAD_SIZE ** (-0.5)).astype(BF16)
    k_ref[...] = dot_nn(normed, input_weight[:, MODEL_WIDTH : 2 * MODEL_WIDTH]).astype(BF16)
    v_ref[...] = dot_nn(normed, input_weight[:, 2 * MODEL_WIDTH :]).astype(BF16)
    masks = head_masks()
    for window in range(LEVEL_WINDOWS):
        rows = pl.ds(window * WIN_TOKENS, WIN_TOKENS)
        stack_rows = pl.ds(window * STACK, STACK)
        queries = stack_heads(q_ref[rows, :], masks)
        scores = dot_nt(queries, k_ref[rows, :])
        bias = jnp.concatenate(
            [bias_a[stack_rows, :], bias_b[stack_rows, :][:, : WIN_TOKENS - 128]], axis=1
        )
        scores = scores + bias
        if lat_row is not None:
            mask = shift_mask(window, lat_row)
            scores = scores + jnp.concatenate([mask] * HEADS, axis=0)
        scores = jnp.exp(scores - jnp.max(scores, axis=-1, keepdims=True))
        weights = (scores / jnp.sum(scores, axis=-1, keepdims=True)).astype(BF16)
        w_ref[stack_rows, :] = weights
        mixed = dot_nn(weights, v_ref[rows, :])
        mix_ref[rows, :] = fold_heads(mixed, masks).astype(BF16)
    return normed


def gelu_parts(pre):
    square = pre * pre
    tanh = jnp.tanh(GELU_C * (pre + GELU_A * pre * square))
    half = 0.5 * (1.0 + tanh)
    slope = half + 0.5 * pre * (1.0 - tanh * tanh) * (GELU_C * (1.0 + 3.0 * GELU_A * square))
    return pre * half, slope


def pack_rows(out_ref, first, values, slab, base):
    done = 0
    while done < values.shape[0]:
        side, inner = (first + done) // slab, (first + done) % slab
        count = min(values.shape[0] - done, slab - inner)
        out_ref[side, pl.ds(base + inner, count), :] = values[done : done + count].astype(BF16)
        done += count


def pack_columns(out_ref, first, values, slab=WEIGHT_SLAB, base=0):
    rows, lanes = values.shape
    for block in range(lanes // 128):
        pack_rows(
            out_ref, first + block * rows, values[:, block * 128 : (block + 1) * 128], slab, base
        )


def backward(e, x_unit, x_inv, gains, middle, weights4, saved, keep_scores, pack_ref, gproj_ref):
    input_weight, output_weight, expand_weight, reduce_weight = weights4
    q_ref, k_ref, v_ref, w_ref, mix_ref = saved
    masks = head_masks()
    mid_unit, mid_inv = norm_stats(middle.astype(F32))
    gain_mid = gains[1:2, :]
    normed_mid = (mid_unit * gain_mid).astype(BF16)
    hidden, slope = gelu_parts(dot_nn(normed_mid, expand_weight))
    hidden = hidden.astype(BF16)
    grad_pre = (slope * dot_nn(e, reduce_weight)).astype(BF16)
    pack_columns(pack_ref, 2304, dot_tn(e, hidden))
    pack_columns(pack_ref, 1152, dot_tn(normed_mid, grad_pre))
    grad_norm, gain_mid_grad = norm_grad(dot_nt(grad_pre, expand_weight), mid_unit, mid_inv, gain_mid)
    grad_middle = e.astype(F32) + grad_norm
    grad_attended = grad_middle.astype(BF16)
    output_grad = dot_tn(mix_ref[...], grad_attended)
    grad_mixture = dot_nt(grad_attended, output_weight).astype(BF16)
    for window in range(LEVEL_WINDOWS):
        base = window * WIN_TOKENS
        rows = pl.ds(base, WIN_TOKENS)
        stack_rows = pl.ds(window * STACK, STACK)
        queries = stack_heads(q_ref[rows, :], masks)
        grads = stack_heads(grad_mixture[base : base + WIN_TOKENS], masks)
        weights = w_ref[stack_rows, :]
        keys = k_ref[rows, :]
        gproj_ref[2, rows, :] = dot_tn(weights, grads).astype(BF16)
        grad_weights = dot_nt(grads, v_ref[rows, :])
        attention = weights.astype(F32)
        moved = attention * grad_weights
        grad_scores = attention * (grad_weights - jnp.sum(moved, axis=-1, keepdims=True))
        score_part = grad_scores.astype(BF16)
        keep_scores(stack_rows, grad_scores, score_part)
        grad_queries = fold_heads(dot_nn(score_part, keys), masks) * HEAD_SIZE ** (-0.5)
        gproj_ref[0, rows, :] = grad_queries.astype(BF16)
        gproj_ref[1, rows, :] = dot_tn(score_part, queries).astype(BF16)
    normed = (x_unit * gains[0:1, :]).astype(BF16)
    parts = [gproj_ref[part] for part in range(3)]
    weight_grads = [dot_tn(normed, part) for part in parts] + [output_grad]
    pack_columns(pack_ref, 0, jnp.concatenate(weight_grads, axis=1))
    grad_normed = dot_nt(parts[0], input_weight[:, :MODEL_WIDTH])
    grad_normed = grad_normed + dot_nt(parts[1], input_weight[:, MODEL_WIDTH : 2 * MODEL_WIDTH])
    grad_normed = grad_normed + dot_nt(parts[2], input_weight[:, 2 * MODEL_WIDTH :])
    grad_normed = grad_normed.astype(BF16).astype(F32)
    grad_in, gain_in_grad = norm_grad(grad_normed, x_unit, x_inv, gains[0:1, :])
    gain_flat = jnp.concatenate([gain_in_grad, gain_mid_grad], axis=1)
    gain_rows = [gain_flat[:, i * 128 : (i + 1) * 128] for i in range(3)]
    gain_rows.append(jnp.zeros((TABLE_ROWS - GAIN_ROW - 3, 128), F32))
    result = (grad_middle + grad_in).astype(BF16)
    return result, jnp.concatenate(gain_rows, axis=0)


def keep_split(score_a, score_b):
    def keep(stack_rows, grad_scores, score_part):
        score_a[stack_rows, :] = grad_scores[:, :128]
        score_b[stack_rows, :] = jnp.concatenate(
            [grad_scores[:, 128:], jnp.zeros((STACK, 256 - WIN_TOKENS), F32)], axis=1
        )

    return keep


def pack_table(pack_ref, score_a, score_b, gain_rows, base):
    folded = fold_table(score_a, score_b)
    pack_columns(pack_ref, 0, folded[:, :256], TABLE_SLAB, base)
    tail = TYPE_ROWS // HEADS
    pieces = [folded[h * tail : (h + 1) * tail, 256:PAIR_LANES] for h in range(HEADS)]
    pieces.append(jnp.zeros((tail, 128 - HEADS * (PAIR_LANES - 256)), F32))
    rest = jnp.concatenate([jnp.concatenate(pieces, axis=1), gain_rows], axis=0)
    pack_rows(pack_ref, 2 * TYPE_ROWS, rest, TABLE_SLAB, base)


def forward_kernel(
    here_ref, x_ref, e_ref, gains_ref, wi_ref, wo_ref, we_ref, wr_ref, table_ref, order_ref,
    natural_ref, early_ref, quad0, quad1, quad2, quad3, q_ref, k_ref, v_ref, w_ref, mix_ref, mid_ref, tok_ref,
    bias_a, bias_b, part_a, part_b, part_c, lines,
):
    build_bias(load_table(table_ref, here_ref[0], (part_a, part_b, part_c), lines), bias_a, bias_b)
    gains = gains_ref[0, 0]
    order = order_ref[...]
    quads = (quad0, quad1, quad2, quad3)
    moved = reorder(e_ref[...], early_ref[...])
    for index, quad in enumerate(quads):
        quad[1] = moved[index * QUAD : (index + 1) * QUAD]
    tokens = reorder(x_ref[...], natural_ref[...])
    tok_ref[...] = tokens
    values = tokens.astype(F32)
    unit, _ = norm_stats(values)
    attention_front(
        unit, gains[0:1, :], wi_ref[0, 0], bias_a, bias_b, None, q_ref, k_ref, v_ref, w_ref, mix_ref
    )
    middle = (values + dot_nn(mix_ref[...], wo_ref[0, 0])).astype(BF16)
    mid_ref[...] = middle
    mid_f = middle.astype(F32)
    mid_unit, _ = norm_stats(mid_f)
    normed_mid = (mid_unit * gains[1:2, :]).astype(BF16)
    hidden, _ = gelu_parts(dot_nn(normed_mid, we_ref[0, 0]))
    output = (mid_f + dot_nt(hidden.astype(BF16), wr_ref[0, 0])).astype(BF16)
    moved = reorder(output, order)
    for index, quad in enumerate(quads):
        quad[0] = moved[index * QUAD : (index + 1) * QUAD]


def bias_kernel(here_ref, table_ref, gate_ref, bias_a, bias_b, part_a, part_b, part_c, lines):
    build_bias(load_table(table_ref, here_ref[0], (part_a, part_b, part_c), lines), bias_a, bias_b)


def turn_kernel(
    here_ref, x0, x1, x2, x3, gains_ref, wi_ref, wo_ref, we_ref, wr_ref, bias_a, bias_b,
    join_ref, split_ref, quad0, quad1, quad2, quad3, pack_ref, score_ref, gain_ref,
    q_ref, k_ref, v_ref, w_ref, mix_ref, gproj_ref,
):
    gains = gains_ref[0, 0]
    join = join_ref[...]
    pieces = (x0, x1, x2, x3)
    block_in = reorder(jnp.concatenate([piece[0] for piece in pieces], axis=0), join)
    e = reorder(jnp.concatenate([piece[1] for piece in pieces], axis=0), join)
    values = block_in.astype(F32)
    unit, inv = norm_stats(values)
    input_weight, output_weight = wi_ref[0, 0], wo_ref[0, 0]
    attention_front(
        unit, gains[0:1, :], input_weight, bias_a, bias_b, here_ref[0].astype(F32), q_ref, k_ref,
        v_ref, w_ref, mix_ref,
    )
    attended = dot_nn(mix_ref[...], output_weight).astype(BF16).astype(F32)
    middle = (values + attended).astype(BF16)

    def keep(stack_rows, grad_scores, score_part):
        score_ref[stack_rows, :] = score_part

    result, gain_ref[...] = backward(
        e, unit, inv, gains, middle, (input_weight, output_weight, we_ref[0, 0], wr_ref[0, 0]),
        (q_ref, k_ref, v_ref, w_ref, mix_ref), keep, pack_ref, gproj_ref,
    )
    moved = reorder(result, split_ref[...])
    for index, quad in enumerate((quad0, quad1, quad2, quad3)):
        quad[...] = moved[index * QUAD : (index + 1) * QUAD]


def late_kernel(
    here_ref, pack_ref, score_ref, gain_ref, send0, send1, send2, send3, score_a, score_b, table_ref
):
    keep = keep_split(score_a, score_b)
    for window in range(LEVEL_WINDOWS):
        stack_rows = pl.ds(window * STACK, STACK)
        keep(stack_rows, score_ref[stack_rows, :].astype(F32), None)
    pack_table(table_ref, score_a, score_b, gain_ref[...], 0)
    for step, send in enumerate((send0, send1, send2, send3)):
        owner = lax.rem(here_ref[1] + step, X_SIZE)
        send[pl.ds(0, WEIGHT_SLAB), :] = pack_ref[owner]
        send[pl.ds(WEIGHT_SLAB, TABLE_SLAB), :] = table_ref[owner]


def send_slabs(here_ref, pack_ref, sends):
    for step, send in enumerate(sends):
        send[...] = pack_ref[lax.rem(here_ref[1] + step, X_SIZE)]


def backward_kernel(
    here_ref, x_ref, e0, e1, e2, e3, gains_ref, wi_ref, wo_ref, we_ref, wr_ref, join_ref,
    stored_ref, q_ref, k_ref, v_ref, w_ref, mix_ref, mid_ref, out_ref, send0, send1, send2, send3,
    score_a, score_b, pack_ref, gproj_ref,
):
    e = reorder(jnp.concatenate([e0[...], e1[...], e2[...], e3[...]], axis=0), join_ref[...])
    unit, inv = norm_stats(x_ref[...].astype(F32))
    result, gain_rows = backward(
        e, unit, inv, gains_ref[0, 0], mid_ref[...],
        (wi_ref[0, 0], wo_ref[0, 0], we_ref[0, 0], wr_ref[0, 0]),
        (q_ref, k_ref, v_ref, w_ref, mix_ref), keep_split(score_a, score_b), pack_ref, gproj_ref,
    )
    pack_table(pack_ref, score_a, score_b, gain_rows, WEIGHT_SLAB)
    out_ref[...] = reorder(result, stored_ref[...])
    send_slabs(here_ref, pack_ref, (send0, send1, send2, send3))


def unpack_kernel(scale, here_ref, got0, got1, got2, got3, *refs):
    gi_ref, go_ref, ge_ref, gr_ref, gn_ref, gt_ref = refs[-14:-8]
    rows, slab0, slab1, t0, t1, part_a, part_b, part_c = refs[-8:]
    for step, got in enumerate((got0, got1, got2, got3)):
        origin = lax.rem(here_ref[1] + X_SIZE - step, X_SIZE)
        for index in range(got.shape[0]):
            part = got[index].astype(F32)
            rows[origin, pl.ds(index * WEIGHT_PART, WEIGHT_PART), :] = part[:WEIGHT_PART] * scale
            for side, table in enumerate((slab0, slab1)):
                first = WEIGHT_PART + side * TABLE_PART
                table[origin, pl.ds(index * TABLE_PART, TABLE_PART), :] = part[
                    first : first + TABLE_PART
                ]
    for slab, table in ((slab0, t0), (slab1, t1)):
        for origin in range(X_SIZE):
            table[pl.ds(origin * TABLE_SLAB, TABLE_SLAB), :] = slab[origin]

    def block(first, count):
        pieces = []
        while count:
            origin, inner = first // WEIGHT_SLAB, first % WEIGHT_SLAB
            here = min(count, WEIGHT_SLAB - inner)
            pieces.append(rows[origin, pl.ds(inner, here), :])
            first, count = first + here, count - here
        return pieces[0] if len(pieces) == 1 else jnp.concatenate(pieces, axis=0)

    for index in range(4):
        gi_ref[0, 0, :, pl.ds(index * 128, 128)] = block(index * 192, 192)
    mixed = block(4 * 192, 192)
    gi_ref[0, 0, :, pl.ds(512, 64)] = mixed[:, :64]
    go_ref[0, 0] = jnp.concatenate([mixed[:, 64:], block(5 * 192, 192)], axis=1)
    for index in range(6):
        ge_ref[0, 0, :, pl.ds(index * 128, 128)] = block(1152 + index * 192, 192)
    for index in range(6):
        gr_ref[0, 0, :, pl.ds(index * 128, 128)] = block(2304 + index * 192, 192)
    gain = (t0[pl.ds(GAIN_ROW, 8), :] + t1[pl.ds(GAIN_ROW, 8), :]) * scale
    gn_ref[0, 0, 0:1, :] = jnp.concatenate([gain[0:1], gain[1:2, :64]], axis=1)
    gn_ref[0, 0, 1:2, :] = jnp.concatenate([gain[1:2, 64:], gain[2:3]], axis=1)
    tail, width = TYPE_ROWS // HEADS, PAIR_LANES - 256
    for side, table in enumerate((t0, t1)):
        rest = table[pl.ds(2 * TYPE_ROWS, tail), :]
        for h in range(HEADS):
            part_c[pl.ds(h * tail, tail), pl.ds(0, width)] = rest[:, h * width : (h + 1) * width]
        for window in range(LEVEL_WINDOWS):
            lines = []
            for group in range(GROUPS):
                first = window * HEADS * GROUPS + group
                place = pl.ds(first, HEADS, stride=GROUPS)
                upper = pl.ds(TYPE_ROWS + first, HEADS, stride=GROUPS)
                lines.append(
                    jnp.concatenate([table[place, :], table[upper, :], part_c[place, :]], axis=1)
                )
            span = WIN_LAT * OFFSETS
            ordered = []
            for query_level in range(WIN_LEVELS):
                for key_level in range(WIN_LEVELS):
                    for row in range(WIN_LAT):
                        line = lines[query_level * WIN_LAT + row]
                        ordered.append(line[:, key_level * span : (key_level + 1) * span])
            result = jnp.concatenate(ordered, axis=1)
            for h in range(HEADS):
                gt_ref[0, 0, window, h, side : side + 1, :] = result[h : h + 1]


LIMIT = 32 * 1024 * 1024
FULL_LIMIT = 60 * 1024 * 1024
TOKEN_SHAPE = jax.ShapeDtypeStruct((TOKENS, MODEL_WIDTH), BF16)
QUAD_SHAPE = jax.ShapeDtypeStruct((QUAD, MODEL_WIDTH), BF16)
WEIGHT_SHAPE = jax.ShapeDtypeStruct((LEVEL_WINDOWS * STACK, WIN_TOKENS), BF16)
BIAS_SHAPE = jax.ShapeDtypeStruct((LEVEL_WINDOWS * STACK, 128), F32)
GAIN_SHAPE = jax.ShapeDtypeStruct((TABLE_ROWS - GAIN_ROW, 128), F32)
HALF_PACK_SHAPE = jax.ShapeDtypeStruct((X_SIZE, WEIGHT_SLAB, 128), BF16)
SLAB_SHAPE = jax.ShapeDtypeStruct((WEIGHT_SLAB + TABLE_SLAB, 128), BF16)
PAIR_SHAPE = jax.ShapeDtypeStruct((2, QUAD, MODEL_WIDTH), BF16)
GRAD_SHAPES = tuple(
    jax.ShapeDtypeStruct((1, BLOCKS) + shape, F32)
    for shape in (
        (MODEL_WIDTH, 3 * MODEL_WIDTH), (MODEL_WIDTH, MODEL_WIDTH), (MODEL_WIDTH, MLP_WIDTH),
        (MODEL_WIDTH, MLP_WIDTH), (2, MODEL_WIDTH), (LEVEL_WINDOWS, HEADS, 2, BIAS_SLOTS),
    )
)


def tall_scratch():
    return pltpu.VMEM((LEVEL_WINDOWS * STACK, 128), F32)


def token_scratch():
    return pltpu.VMEM((TOKENS, MODEL_WIDTH), BF16)


def whole(array):
    rank = len(array.shape)
    return pl.BlockSpec(array.shape, lambda i, lat: (0,) * rank)


def one_block(array, index):
    rank = len(array.shape)
    return pl.BlockSpec((1, 1) + array.shape[2:], lambda i, lat: (0, index) + (0,) * (rank - 2))


def call(kernel, lat, ins, outs, scratch, aliases=None, limit=LIMIT):
    arrays = [array for array, _ in ins]
    return pl.pallas_call(
        kernel,
        out_shape=tuple(shape for shape, _ in outs),
        grid_spec=pltpu.PrefetchScalarGridSpec(
            num_scalar_prefetch=1,
            grid=(1,),
            in_specs=[spec for _, spec in ins],
            out_specs=tuple(spec for _, spec in outs),
            scratch_shapes=scratch,
        ),
        input_output_aliases=aliases or {},
        compiler_params=pltpu.CompilerParams(vmem_limit_bytes=limit),
    )(lat, *arrays)


def plain(*arrays):
    return [(array, whole(array)) for array in arrays]


def exchange(quads, by):
    lon = ("z", "x")
    ring, sides = lax.axis_size(lon), lax.axis_size("lat")
    lon_pairs = [(i, (i + by) % ring) for i in range(ring)]
    swap = [(i, i ^ 1) for i in range(sides)]
    both = [
        (i * sides + j, ((i + by) % ring) * sides + (j ^ 1)) for i in range(ring) for j in range(sides)
    ]
    return (
        quads[0],
        lax.ppermute(quads[1], lon, lon_pairs),
        lax.ppermute(quads[2], "lat", swap),
        lax.ppermute(quads[3], lon + ("lat",), both),
    )


def swap_all(values, axes):
    return lax.all_to_all(values, axes, split_axis=0, concat_axis=0, tiled=True)


def pass_x(sends):
    size = lax.axis_size("x")
    return (sends[0],) + tuple(
        lax.ppermute(sends[step], "x", [(i, (i + step) % size) for i in range(size)])
        for step in range(1, size)
    )


def slab_sum(slabs):
    total = slabs[0][...].astype(F32)
    for slab in slabs[1:]:
        total = total + slab[...].astype(F32)
    return total


def write_parts(total, out_ref, first):
    for index in range(out_ref.shape[0]):
        weights = total[index * WEIGHT_PART : (index + 1) * WEIGHT_PART]
        start = WEIGHT_SLAB + index * TABLE_PART
        part = jnp.concatenate([weights, total[start : start + TABLE_PART]], axis=0)
        out_ref[index, pl.ds(first, SENT), :] = part.astype(BF16)


def part_sum(spread_ref, first):
    sides = []
    for side in range(2):
        total = spread_ref[side, pl.ds(first, SENT), :].astype(F32)
        for index in range(side + 2, spread_ref.shape[0], 2):
            total = total + spread_ref[index, pl.ds(first, SENT), :].astype(F32)
        sides.append(total)
    weights = sides[0][:WEIGHT_PART] + sides[1][:WEIGHT_PART]
    spare = jnp.zeros((PART - SENT - TABLE_PART, 128), F32)
    rows = [weights, sides[0][WEIGHT_PART:], sides[1][WEIGHT_PART:], spare]
    return jnp.concatenate(rows, axis=0).astype(BF16)


def first_kernel(here_ref, slab0, slab1, slab2, slab3, out_ref):
    write_parts(slab_sum((slab0, slab1, slab2, slab3)), out_ref, 0)


def sum_kernel(here_ref, spread_ref, out_ref):
    total = part_sum(spread_ref, 0)
    for index in range(out_ref.shape[0]):
        out_ref[index] = total


def parts_shape(count, width):
    return jax.ShapeDtypeStruct((count, width, 128), BF16)


def unpack(parts, here, index, scale, previous):
    ins = plain(*parts)
    aliases = {}
    if previous is not None:
        ins = ins + [(array, pl.BlockSpec(memory_space=pl.ANY)) for array in previous]
        aliases = {1 + len(parts) + place: place for place in range(6)}
    outs = [(shape, one_block(shape, index)) for shape in GRAD_SHAPES]
    scratch = [pltpu.VMEM((X_SIZE, WEIGHT_SLAB, 128), F32)]
    scratch += [pltpu.VMEM((X_SIZE, TABLE_SLAB, 128), F32) for _ in range(2)]
    scratch += [pltpu.VMEM((TABLE_ROWS, 128), F32) for _ in range(2)] + type_scratch()
    return call(functools.partial(unpack_kernel, scale), here, ins, outs, scratch, aliases)


def type_scratch():
    return [pltpu.VMEM((TYPE_ROWS, 128), F32) for _ in range(3)]


def pack_scratch():
    return pltpu.VMEM((X_SIZE,) + SLAB_SHAPE.shape, BF16)


def stored_tokens(array):
    return array[0].transpose(1, 2, 0, 3).reshape(TOKENS, MODEL_WIDTH)


def on_device(
    inputs, grad_output, norm_gains, input_weight, output_weight, expand_weight, reduce_weight,
    bias_table,
):
    lat_index = lax.axis_index("lat")
    here = jnp.stack([lat_index, lax.axis_index("x")]).astype(jnp.int32)
    orders = [jnp.asarray(order) for order in quad_orders()]
    split, join_rolled, split_rolled, join, natural, early_split, stored = orders
    reduce_weight = reduce_weight.swapaxes(2, 3)
    bias_table = bias_table.swapaxes(3, 4)
    weights = [
        [(array, one_block(array, block)) for array in
         (norm_gains, input_weight, output_weight, expand_weight, reduce_weight)]
        for block in range(BLOCKS)
    ]
    tables = [[(bias_table, one_block(bias_table, block))] for block in range(BLOCKS)]
    front_scratch = [tall_scratch(), tall_scratch()] + type_scratch()
    front_scratch.append(pltpu.VMEM((8, BIAS_SLOTS), F32))
    outs = call(
        forward_kernel,
        here,
        plain(stored_tokens(inputs), stored_tokens(grad_output)) + weights[0] + tables[0]
        + plain(split, natural, early_split),
        plain(*((PAIR_SHAPE,) * 4 + (TOKEN_SHAPE,) * 3 + (WEIGHT_SHAPE,) + (TOKEN_SHAPE,) * 3)),
        front_scratch,
        limit=FULL_LIMIT,
    )
    saved = outs[4:10]
    tokens = outs[10]
    quads = exchange(outs[:4], -1)
    gate = outs[0]
    bias = call(
        bias_kernel,
        here,
        tables[1] + [(gate, pl.BlockSpec(memory_space=pl.ANY))],
        plain(BIAS_SHAPE, BIAS_SHAPE),
        front_scratch[2:],
    )
    outs = call(
        turn_kernel,
        here,
        plain(*quads) + weights[1] + plain(*bias, join_rolled, split_rolled),
        plain(*((QUAD_SHAPE,) * 4 + (HALF_PACK_SHAPE, WEIGHT_SHAPE, GAIN_SHAPE))),
        [token_scratch() for _ in range(3)]
        + [pltpu.VMEM(WEIGHT_SHAPE.shape, BF16), token_scratch(),
           pltpu.VMEM((3, TOKENS, MODEL_WIDTH), BF16)],
    )
    flow_quads = exchange(outs[:4], 1)
    late = call(
        late_kernel,
        here,
        plain(*outs[4:]),
        plain(*(SLAB_SHAPE,) * 4),
        [tall_scratch(), tall_scratch(), pltpu.VMEM((X_SIZE, TABLE_SLAB, 128), BF16)],
    )
    flow_quads, late = lax.optimization_barrier((flow_quads, late))
    late = pass_x(late)
    outs = call(
        backward_kernel,
        here,
        plain(tokens, *flow_quads) + weights[0] + plain(join, stored, *saved),
        plain(*((TOKEN_SHAPE,) + (SLAB_SHAPE,) * 4)),
        [tall_scratch(), tall_scratch(), pack_scratch(),
         pltpu.VMEM((3, TOKENS, MODEL_WIDTH), BF16)],
    )
    grad_flow = outs[0]
    late, early = lax.optimization_barrier((late, outs[1:]))
    early = pass_x(early)
    rest = ("z", "lat")
    count = lax.axis_size(rest)
    lat_total = LAT_DEV * lax.axis_size("lat")
    scale = float(LEVELS * lat_total * LON_DEV * lax.axis_size(("z", "x"))) ** (-0.5)

    def scatter(slabs):
        (parts,) = call(first_kernel, here, plain(*slabs), plain(parts_shape(count, SENT)), [])
        return swap_all(parts, rest)

    def gather(spread):
        (parts,) = call(sum_kernel, here, plain(spread), plain(parts_shape(count, PART)), [])
        return swap_all(parts, rest)

    late, early = lax.optimization_barrier((scatter(late), early))
    upstream = lax.ppermute(
        grad_flow, "section", [(i, i - 1) for i in range(1, lax.axis_size("section"))]
    )
    late, early, upstream = lax.optimization_barrier((gather(late), early, upstream))
    early, late = lax.optimization_barrier((scatter(early), pass_x((late,) * X_SIZE)))
    early = pass_x((gather(early),) * X_SIZE)
    upstream = upstream.reshape(LAT_DEV, LON_DEV, LEVELS, MODEL_WIDTH).transpose(2, 0, 1, 3)[None]
    grads = unpack(late, here, 1, scale, None)
    grads = list(unpack(early, here, 0, scale, grads))
    grads[3] = grads[3].swapaxes(2, 3)
    grads[5] = grads[5].swapaxes(3, 4)
    return (upstream,) + tuple(grads)


def solution(mesh):
    sizes = mesh.shape
    grid = mesh.devices.reshape(
        sizes["section"], sizes["lon"] // X_SIZE, X_SIZE, sizes["lat"]
    )
    mesh = Mesh(grid, ("section", "z", "x", "lat"))
    return jax.shard_map(
        on_device,
        mesh=mesh,
        in_specs=(
            P("section", None, "lat", ("z", "x"), None),
            P("section", None, "lat", ("z", "x"), None),
            P("section", None, None, None),
            P("section", None, None, None),
            P("section", None, None, None),
            P("section", None, None, None),
            P("section", None, None, None),
            P("section", None, None, None, None, None),
        ),
        out_specs=(
            P("section", None, "lat", ("z", "x"), None),
            P("section", None, None, None),
            P("section", None, None, None),
            P("section", None, None, None),
            P("section", None, None, None),
            P("section", None, None, None),
            P("section", None, None, None, None, None),
        ),
        check_vma=False,
    )
```

```python
import functools

import jax
import jax.numpy as jnp
import numpy as np
from jax import lax
from jax.experimental import pallas as pl
from jax.experimental.pallas import tpu as pltpu
from jax.sharding import Mesh
from jax.sharding import PartitionSpec as P

MODEL_WIDTH = 192
HEADS = 6
HEAD_SIZE = 32
LEVELS = 8
WIN_LEVELS = 2
WIN_LAT = 6
WIN_LON = 12
BLOCKS = 2
MLP_WIDTH = 768
LAT_DEV = 6
LON_DEV = 12
LEVEL_WINDOWS = 4
WIN_TOKENS = 144
BIAS_SLOTS = 3312

NORM_EPS = 1e-05
MASK_FILL = -10000.0
GELU_C = 0.7978845608028654
GELU_A = 0.044715

TOKENS = LEVELS * LAT_DEV * LON_DEV
QUAD = TOKENS // 4
STACK = HEADS * WIN_TOKENS
GROUPS = WIN_LEVELS * WIN_LAT
OFFSETS = 2 * WIN_LON - 1
PAIR_LANES = GROUPS * OFFSETS
PAIR_PAD = 384
TYPE_ROWS = LEVEL_WINDOWS * HEADS * GROUPS
X_SIZE = 4
WEIGHT_ROWS = 3456
TABLE_ROWS = 640
GAIN_ROW = 624
WEIGHT_SLAB = WEIGHT_ROWS // X_SIZE
TABLE_SLAB = TABLE_ROWS // X_SIZE
WEIGHT_PART = 54
TABLE_PART = 10
SENT = WEIGHT_PART + TABLE_PART
PART = 80

F32 = jnp.float32
BF16 = jnp.bfloat16


def quad_orders():
    level, row, col = np.meshgrid(
        np.arange(LEVELS), np.arange(LAT_DEV), np.arange(LON_DEV), indexing="ij"
    )
    half_rows, half_cols = WIN_LAT // 2, WIN_LON // 2
    quad = (1 - row // half_rows) * 2 + (1 - col // half_cols)
    place = (quad * LEVELS + level) * (half_rows * half_cols)
    place = place + (row % half_rows) * half_cols + col % half_cols
    split = place.reshape(-1)
    quad_r = (row // half_rows) * 2 + col // half_cols
    from_level = (level + WIN_LEVELS // 2) % LEVELS
    place_r = (quad_r * LEVELS + from_level) * (half_rows * half_cols)
    place_r = place_r + (row % half_rows) * half_cols + col % half_cols
    split_rolled = place_r.reshape(-1)
    join = np.argsort(split)
    join_rolled = np.argsort(split_rolled)
    natural = np.arange(TOKENS).reshape(LEVELS, LAT_DEV, LON_DEV).transpose(1, 2, 0).reshape(-1)
    stored = np.argsort(natural)
    orders = (split, join_rolled, split_rolled, join, natural, split[natural], stored)
    return [order.astype(np.int32)[None, :] for order in orders]


def dot_nn(a, b):
    return jnp.dot(a, b, preferred_element_type=F32)


def dot_nt(a, b):
    return lax.dot_general(a, b, (((1,), (1,)), ((), ())), preferred_element_type=F32)


def dot_tn(a, b):
    return lax.dot_general(a, b, (((0,), (0,)), ((), ())), preferred_element_type=F32)


def reorder(values, order_row):
    rows = lax.broadcasted_iota(jnp.int32, (TOKENS, TOKENS), 0)
    pick = jnp.where(rows == order_row, 1.0, 0.0).astype(BF16)
    return dot_nn(pick, values).astype(BF16)


def norm_stats(values):
    centred = values - jnp.mean(values, axis=-1, keepdims=True)
    spread = jnp.mean(centred * centred, axis=-1, keepdims=True)
    inv = lax.rsqrt(spread + NORM_EPS)
    return centred * inv, inv


def norm_grad(grad, unit, inv, gain_row):
    gain_grad = jnp.sum(grad * unit, axis=0, keepdims=True)
    grad_unit = grad * gain_row
    first = jnp.mean(grad_unit, axis=-1, keepdims=True)
    second = jnp.mean(grad_unit * unit, axis=-1, keepdims=True)
    return inv * (grad_unit - first - unit * second), gain_grad


def head_masks():
    lane = lax.broadcasted_iota(jnp.int32, (1, MODEL_WIDTH), 1)
    return [
        jnp.logical_and(lane >= h * HEAD_SIZE, lane < (h + 1) * HEAD_SIZE) for h in range(HEADS)
    ]


def stack_heads(values, masks):
    wide = values.astype(F32)
    return jnp.concatenate([jnp.where(m, wide, 0.0) for m in masks], axis=0).astype(BF16)


def fold_heads(stacked, masks):
    total = jnp.where(masks[0], stacked[:WIN_TOKENS], 0.0)
    for h in range(1, HEADS):
        total = jnp.where(masks[h], stacked[h * WIN_TOKENS : (h + 1) * WIN_TOKENS], total)
    return total


def pair_pick(query_col):
    key = lax.broadcasted_iota(jnp.int32, (256, PAIR_PAD), 0)
    lane = lax.broadcasted_iota(jnp.int32, (256, PAIR_PAD), 1)
    group = lax.shift_right_logical(key * 5462, 16)
    key_col = key - group * WIN_LON
    target = group * OFFSETS + (WIN_LON - 1 + query_col) - key_col
    hit = jnp.logical_and(lane == target, key < WIN_TOKENS)
    return jnp.where(hit, 1.0, 0.0).astype(BF16)


def segment_start(group, key_level):
    query_level, query_row = group // WIN_LAT, group % WIN_LAT
    return ((query_level * WIN_LEVELS + key_level) * WIN_LAT + query_row) * WIN_LAT * OFFSETS


def load_table(table_ref, side, parts, lines):
    width = WIN_LAT * OFFSETS
    for window in range(LEVEL_WINDOWS):
        for h in range(HEADS):
            lines[h : h + 1, :] = table_ref[0, 0, window, h, pl.ds(side, 1), :]
        rows = lines[:HEADS, :]
        for group in range(GROUPS):
            pieces = []
            for key_level in range(WIN_LEVELS):
                start = segment_start(group, key_level)
                pieces.append(rows[:, start : start + width])
            pieces.append(jnp.zeros((HEADS, PAIR_PAD - PAIR_LANES), F32))
            line = jnp.concatenate(pieces, axis=1)
            place = pl.ds(window * HEADS * GROUPS + group, HEADS, stride=GROUPS)
            for index, part in enumerate(parts):
                part[place, :] = line[:, index * 128 : (index + 1) * 128]
    return jnp.concatenate([part[...] for part in parts], axis=1)


def build_bias(table, bias_a, bias_b):
    high = table.astype(BF16)
    rest = table - high.astype(F32)
    middle = rest.astype(BF16)
    low = (rest - middle.astype(F32)).astype(BF16)
    for query_col in range(WIN_LON):
        pick = pair_pick(query_col)
        spread = dot_nt(high, pick) + dot_nt(middle, pick) + dot_nt(low, pick)
        bias_a[pl.ds(query_col, TYPE_ROWS, stride=WIN_LON), :] = spread[:, :128]
        bias_b[pl.ds(query_col, TYPE_ROWS, stride=WIN_LON), :] = spread[:, 128:]


def fold_table(score_a, score_b):
    total = jnp.zeros((TYPE_ROWS, PAIR_PAD), F32)
    for query_col in range(WIN_LON):
        pick = pair_pick(query_col)
        left = score_a[pl.ds(query_col, TYPE_ROWS, stride=WIN_LON), :]
        right = score_b[pl.ds(query_col, TYPE_ROWS, stride=WIN_LON), :]
        total = total + dot_nn(jnp.concatenate([left, right], axis=1).astype(BF16), pick)
    return total


def shift_mask(window, lat_row):
    shape = (WIN_TOKENS, WIN_TOKENS)
    half = WIN_TOKENS // 2
    parts = []
    for axis in (0, 1):
        token = lax.broadcasted_iota(jnp.int32, shape, axis)
        upper = token >= half
        inner = jnp.where(upper, token - half, token)
        parts.append((upper, inner >= half // 2))
    rows_differ = jnp.where(parts[0][1] != parts[1][1], 1.0, 0.0) * lat_row
    if window == LEVEL_WINDOWS - 1:
        levels_differ = jnp.where(parts[0][0] != parts[1][0], 1.0, 0.0)
        rows_differ = jnp.maximum(rows_differ, levels_differ)
    return rows_differ * MASK_FILL


def attention_front(unit, gain_row, input_weight, bias_a, bias_b, lat_row, q_ref, k_ref, v_ref, w_ref, mix_ref):
    normed = (unit * gain_row).astype(BF16)
    q_ref[...] = (dot_nn(normed, input_weight[:, :MODEL_WIDTH]) * HEAD_SIZE ** (-0.5)).astype(BF16)
    k_ref[...] = dot_nn(normed, input_weight[:, MODEL_WIDTH : 2 * MODEL_WIDTH]).astype(BF16)
    v_ref[...] = dot_nn(normed, input_weight[:, 2 * MODEL_WIDTH :]).astype(BF16)
    masks = head_masks()
    for window in range(LEVEL_WINDOWS):
        rows = pl.ds(window * WIN_TOKENS, WIN_TOKENS)
        stack_rows = pl.ds(window * STACK, STACK)
        queries = stack_heads(q_ref[rows, :], masks)
        scores = dot_nt(queries, k_ref[rows, :])
        bias = jnp.concatenate(
            [bias_a[stack_rows, :], bias_b[stack_rows, :][:, : WIN_TOKENS - 128]], axis=1
        )
        scores = scores + bias
        if lat_row is not None:
            mask = shift_mask(window, lat_row)
            scores = scores + jnp.concatenate([mask] * HEADS, axis=0)
        scores = jnp.exp(scores - jnp.max(scores, axis=-1, keepdims=True))
        weights = (scores / jnp.sum(scores, axis=-1, keepdims=True)).astype(BF16)
        w_ref[stack_rows, :] = weights
        mixed = dot_nn(weights, v_ref[rows, :])
        mix_ref[rows, :] = fold_heads(mixed, masks).astype(BF16)
    return normed


def gelu_parts(pre):
    square = pre * pre
    tanh = jnp.tanh(GELU_C * (pre + GELU_A * pre * square))
    half = 0.5 * (1.0 + tanh)
    slope = half + 0.5 * pre * (1.0 - tanh * tanh) * (GELU_C * (1.0 + 3.0 * GELU_A * square))
    return pre * half, slope


def pack_rows(out_ref, first, values, slab, base):
    done = 0
    while done < values.shape[0]:
        side, inner = (first + done) // slab, (first + done) % slab
        count = min(values.shape[0] - done, slab - inner)
        out_ref[side, pl.ds(base + inner, count), :] = values[done : done + count].astype(BF16)
        done += count


def pack_columns(out_ref, first, values, slab=WEIGHT_SLAB, base=0):
    rows, lanes = values.shape
    for block in range(lanes // 128):
        pack_rows(
            out_ref, first + block * rows, values[:, block * 128 : (block + 1) * 128], slab, base
        )


def backward(e, x_unit, x_inv, gains, middle, weights4, saved, keep_scores, pack_ref, gproj_ref):
    input_weight, output_weight, expand_weight, reduce_weight = weights4
    q_ref, k_ref, v_ref, w_ref, mix_ref = saved
    masks = head_masks()
    mid_unit, mid_inv = norm_stats(middle.astype(F32))
    gain_mid = gains[1:2, :]
    normed_mid = (mid_unit * gain_mid).astype(BF16)
    hidden, slope = gelu_parts(dot_nn(normed_mid, expand_weight))
    hidden = hidden.astype(BF16)
    grad_pre = (slope * dot_nn(e, reduce_weight)).astype(BF16)
    pack_columns(pack_ref, 2304, dot_tn(e, hidden))
    pack_columns(pack_ref, 1152, dot_tn(normed_mid, grad_pre))
    grad_norm, gain_mid_grad = norm_grad(dot_nt(grad_pre, expand_weight), mid_unit, mid_inv, gain_mid)
    grad_middle = e.astype(F32) + grad_norm
    grad_attended = grad_middle.astype(BF16)
    output_grad = dot_tn(mix_ref[...], grad_attended)
    grad_mixture = dot_nt(grad_attended, output_weight).astype(BF16)
    for window in range(LEVEL_WINDOWS):
        base = window * WIN_TOKENS
        rows = pl.ds(base, WIN_TOKENS)
        stack_rows = pl.ds(window * STACK, STACK)
        queries = stack_heads(q_ref[rows, :], masks)
        grads = stack_heads(grad_mixture[base : base + WIN_TOKENS], masks)
        weights = w_ref[stack_rows, :]
        keys = k_ref[rows, :]
        gproj_ref[2, rows, :] = dot_tn(weights, grads).astype(BF16)
        grad_weights = dot_nt(grads, v_ref[rows, :])
        attention = weights.astype(F32)
        moved = attention * grad_weights
        grad_scores = attention * (grad_weights - jnp.sum(moved, axis=-1, keepdims=True))
        score_part = grad_scores.astype(BF16)
        keep_scores(stack_rows, grad_scores, score_part)
        grad_queries = fold_heads(dot_nn(score_part, keys), masks) * HEAD_SIZE ** (-0.5)
        gproj_ref[0, rows, :] = grad_queries.astype(BF16)
        gproj_ref[1, rows, :] = dot_tn(score_part, queries).astype(BF16)
    normed = (x_unit * gains[0:1, :]).astype(BF16)
    parts = [gproj_ref[part] for part in range(3)]
    weight_grads = [dot_tn(normed, part) for part in parts] + [output_grad]
    pack_columns(pack_ref, 0, jnp.concatenate(weight_grads, axis=1))
    grad_normed = dot_nt(parts[0], input_weight[:, :MODEL_WIDTH])
    grad_normed = grad_normed + dot_nt(parts[1], input_weight[:, MODEL_WIDTH : 2 * MODEL_WIDTH])
    grad_normed = grad_normed + dot_nt(parts[2], input_weight[:, 2 * MODEL_WIDTH :])
    grad_normed = grad_normed.astype(BF16).astype(F32)
    grad_in, gain_in_grad = norm_grad(grad_normed, x_unit, x_inv, gains[0:1, :])
    gain_flat = jnp.concatenate([gain_in_grad, gain_mid_grad], axis=1)
    gain_rows = [gain_flat[:, i * 128 : (i + 1) * 128] for i in range(3)]
    gain_rows.append(jnp.zeros((TABLE_ROWS - GAIN_ROW - 3, 128), F32))
    result = (grad_middle + grad_in).astype(BF16)
    return result, jnp.concatenate(gain_rows, axis=0)


def keep_split(score_a, score_b):
    def keep(stack_rows, grad_scores, score_part):
        score_a[stack_rows, :] = grad_scores[:, :128]
        score_b[stack_rows, :] = jnp.concatenate(
            [grad_scores[:, 128:], jnp.zeros((STACK, 256 - WIN_TOKENS), F32)], axis=1
        )

    return keep


def pack_table(pack_ref, score_a, score_b, gain_rows, base):
    folded = fold_table(score_a, score_b)
    pack_columns(pack_ref, 0, folded[:, :256], TABLE_SLAB, base)
    tail = TYPE_ROWS // HEADS
    pieces = [folded[h * tail : (h + 1) * tail, 256:PAIR_LANES] for h in range(HEADS)]
    pieces.append(jnp.zeros((tail, 128 - HEADS * (PAIR_LANES - 256)), F32))
    rest = jnp.concatenate([jnp.concatenate(pieces, axis=1), gain_rows], axis=0)
    pack_rows(pack_ref, 2 * TYPE_ROWS, rest, TABLE_SLAB, base)


def forward_kernel(
    here_ref, x_ref, e_ref, gains_ref, wi_ref, wo_ref, we_ref, wr_ref, table_ref, order_ref,
    natural_ref, early_ref, quad0, quad1, quad2, quad3, q_ref, k_ref, v_ref, w_ref, mix_ref, mid_ref, tok_ref,
    bias_a, bias_b, part_a, part_b, part_c, lines,
):
    build_bias(load_table(table_ref, here_ref[0], (part_a, part_b, part_c), lines), bias_a, bias_b)
    gains = gains_ref[0, 0]
    order = order_ref[...]
    quads = (quad0, quad1, quad2, quad3)
    moved = reorder(e_ref[...], early_ref[...])
    for index, quad in enumerate(quads):
        quad[1] = moved[index * QUAD : (index + 1) * QUAD]
    tokens = reorder(x_ref[...], natural_ref[...])
    tok_ref[...] = tokens
    values = tokens.astype(F32)
    unit, _ = norm_stats(values)
    attention_front(
        unit, gains[0:1, :], wi_ref[0, 0], bias_a, bias_b, None, q_ref, k_ref, v_ref, w_ref, mix_ref
    )
    middle = (values + dot_nn(mix_ref[...], wo_ref[0, 0])).astype(BF16)
    mid_ref[...] = middle
    mid_f = middle.astype(F32)
    mid_unit, _ = norm_stats(mid_f)
    normed_mid = (mid_unit * gains[1:2, :]).astype(BF16)
    hidden, _ = gelu_parts(dot_nn(normed_mid, we_ref[0, 0]))
    output = (mid_f + dot_nt(hidden.astype(BF16), wr_ref[0, 0])).astype(BF16)
    moved = reorder(output, order)
    for index, quad in enumerate(quads):
        quad[0] = moved[index * QUAD : (index + 1) * QUAD]


def bias_kernel(here_ref, table_ref, gate_ref, bias_a, bias_b, part_a, part_b, part_c, lines):
    build_bias(load_table(table_ref, here_ref[0], (part_a, part_b, part_c), lines), bias_a, bias_b)


def turn_kernel(
    here_ref, x0, x1, x2, x3, gains_ref, wi_ref, wo_ref, we_ref, wr_ref, bias_a, bias_b,
    join_ref, split_ref, quad0, quad1, quad2, quad3, pack_ref, score_ref, gain_ref,
    q_ref, k_ref, v_ref, w_ref, mix_ref, gproj_ref,
):
    gains = gains_ref[0, 0]
    join = join_ref[...]
    pieces = (x0, x1, x2, x3)
    block_in = reorder(jnp.concatenate([piece[0] for piece in pieces], axis=0), join)
    e = reorder(jnp.concatenate([piece[1] for piece in pieces], axis=0), join)
    values = block_in.astype(F32)
    unit, inv = norm_stats(values)
    input_weight, output_weight = wi_ref[0, 0], wo_ref[0, 0]
    attention_front(
        unit, gains[0:1, :], input_weight, bias_a, bias_b, here_ref[0].astype(F32), q_ref, k_ref,
        v_ref, w_ref, mix_ref,
    )
    attended = dot_nn(mix_ref[...], output_weight).astype(BF16).astype(F32)
    middle = (values + attended).astype(BF16)

    def keep(stack_rows, grad_scores, score_part):
        score_ref[stack_rows, :] = score_part

    result, gain_ref[...] = backward(
        e, unit, inv, gains, middle, (input_weight, output_weight, we_ref[0, 0], wr_ref[0, 0]),
        (q_ref, k_ref, v_ref, w_ref, mix_ref), keep, pack_ref, gproj_ref,
    )
    moved = reorder(result, split_ref[...])
    for index, quad in enumerate((quad0, quad1, quad2, quad3)):
        quad[...] = moved[index * QUAD : (index + 1) * QUAD]


def late_kernel(
    here_ref, pack_ref, score_ref, gain_ref, send0, send1, send2, send3, score_a, score_b, table_ref
):
    keep = keep_split(score_a, score_b)
    for window in range(LEVEL_WINDOWS):
        stack_rows = pl.ds(window * STACK, STACK)
        keep(stack_rows, score_ref[stack_rows, :].astype(F32), None)
    pack_table(table_ref, score_a, score_b, gain_ref[...], 0)
    for step, send in enumerate((send0, send1, send2, send3)):
        owner = lax.rem(here_ref[1] + step, X_SIZE)
        send[pl.ds(0, WEIGHT_SLAB), :] = pack_ref[owner]
        send[pl.ds(WEIGHT_SLAB, TABLE_SLAB), :] = table_ref[owner]


def send_slabs(here_ref, pack_ref, sends):
    for step, send in enumerate(sends):
        send[...] = pack_ref[lax.rem(here_ref[1] + step, X_SIZE)]


def backward_kernel(
    here_ref, x_ref, e0, e1, e2, e3, gains_ref, wi_ref, wo_ref, we_ref, wr_ref, join_ref,
    stored_ref, q_ref, k_ref, v_ref, w_ref, mix_ref, mid_ref, out_ref, send0, send1, send2, send3,
    score_a, score_b, pack_ref, gproj_ref,
):
    e = reorder(jnp.concatenate([e0[...], e1[...], e2[...], e3[...]], axis=0), join_ref[...])
    unit, inv = norm_stats(x_ref[...].astype(F32))
    result, gain_rows = backward(
        e, unit, inv, gains_ref[0, 0], mid_ref[...],
        (wi_ref[0, 0], wo_ref[0, 0], we_ref[0, 0], wr_ref[0, 0]),
        (q_ref, k_ref, v_ref, w_ref, mix_ref), keep_split(score_a, score_b), pack_ref, gproj_ref,
    )
    pack_table(pack_ref, score_a, score_b, gain_rows, WEIGHT_SLAB)
    out_ref[...] = reorder(result, stored_ref[...])
    send_slabs(here_ref, pack_ref, (send0, send1, send2, send3))


def unpack_kernel(scale, here_ref, got0, got1, got2, got3, *refs):
    gi_ref, go_ref, ge_ref, gr_ref, gn_ref, gt_ref = refs[-14:-8]
    rows, slab0, slab1, t0, t1, part_a, part_b, part_c = refs[-8:]
    for step, got in enumerate((got0, got1, got2, got3)):
        origin = lax.rem(here_ref[1] + X_SIZE - step, X_SIZE)
        for index in range(got.shape[0]):
            part = got[index].astype(F32)
            rows[origin, pl.ds(index * WEIGHT_PART, WEIGHT_PART), :] = part[:WEIGHT_PART] * scale
            for side, table in enumerate((slab0, slab1)):
                first = WEIGHT_PART + side * TABLE_PART
                table[origin, pl.ds(index * TABLE_PART, TABLE_PART), :] = part[
                    first : first + TABLE_PART
                ]
    for slab, table in ((slab0, t0), (slab1, t1)):
        for origin in range(X_SIZE):
            table[pl.ds(origin * TABLE_SLAB, TABLE_SLAB), :] = slab[origin]

    def block(first, count):
        pieces = []
        while count:
            origin, inner = first // WEIGHT_SLAB, first % WEIGHT_SLAB
            here = min(count, WEIGHT_SLAB - inner)
            pieces.append(rows[origin, pl.ds(inner, here), :])
            first, count = first + here, count - here
        return pieces[0] if len(pieces) == 1 else jnp.concatenate(pieces, axis=0)

    for index in range(4):
        gi_ref[0, 0, :, pl.ds(index * 128, 128)] = block(index * 192, 192)
    mixed = block(4 * 192, 192)
    gi_ref[0, 0, :, pl.ds(512, 64)] = mixed[:, :64]
    go_ref[0, 0] = jnp.concatenate([mixed[:, 64:], block(5 * 192, 192)], axis=1)
    for index in range(6):
        ge_ref[0, 0, :, pl.ds(index * 128, 128)] = block(1152 + index * 192, 192)
    for index in range(6):
        gr_ref[0, 0, :, pl.ds(index * 128, 128)] = block(2304 + index * 192, 192)
    gain = (t0[pl.ds(GAIN_ROW, 8), :] + t1[pl.ds(GAIN_ROW, 8), :]) * scale
    gn_ref[0, 0, 0:1, :] = jnp.concatenate([gain[0:1], gain[1:2, :64]], axis=1)
    gn_ref[0, 0, 1:2, :] = jnp.concatenate([gain[1:2, 64:], gain[2:3]], axis=1)
    tail, width = TYPE_ROWS // HEADS, PAIR_LANES - 256
    for side, table in enumerate((t0, t1)):
        rest = table[pl.ds(2 * TYPE_ROWS, tail), :]
        for h in range(HEADS):
            part_c[pl.ds(h * tail, tail), pl.ds(0, width)] = rest[:, h * width : (h + 1) * width]
        for window in range(LEVEL_WINDOWS):
            lines = []
            for group in range(GROUPS):
                first = window * HEADS * GROUPS + group
                place = pl.ds(first, HEADS, stride=GROUPS)
                upper = pl.ds(TYPE_ROWS + first, HEADS, stride=GROUPS)
                lines.append(
                    jnp.concatenate([table[place, :], table[upper, :], part_c[place, :]], axis=1)
                )
            span = WIN_LAT * OFFSETS
            ordered = []
            for query_level in range(WIN_LEVELS):
                for key_level in range(WIN_LEVELS):
                    for row in range(WIN_LAT):
                        line = lines[query_level * WIN_LAT + row]
                        ordered.append(line[:, key_level * span : (key_level + 1) * span])
            result = jnp.concatenate(ordered, axis=1)
            for h in range(HEADS):
                gt_ref[0, 0, window, h, side : side + 1, :] = result[h : h + 1]


LIMIT = 32 * 1024 * 1024
FULL_LIMIT = 60 * 1024 * 1024
TOKEN_SHAPE = jax.ShapeDtypeStruct((TOKENS, MODEL_WIDTH), BF16)
QUAD_SHAPE = jax.ShapeDtypeStruct((QUAD, MODEL_WIDTH), BF16)
WEIGHT_SHAPE = jax.ShapeDtypeStruct((LEVEL_WINDOWS * STACK, WIN_TOKENS), BF16)
BIAS_SHAPE = jax.ShapeDtypeStruct((LEVEL_WINDOWS * STACK, 128), F32)
GAIN_SHAPE = jax.ShapeDtypeStruct((TABLE_ROWS - GAIN_ROW, 128), F32)
HALF_PACK_SHAPE = jax.ShapeDtypeStruct((X_SIZE, WEIGHT_SLAB, 128), BF16)
SLAB_SHAPE = jax.ShapeDtypeStruct((WEIGHT_SLAB + TABLE_SLAB, 128), BF16)
PAIR_SHAPE = jax.ShapeDtypeStruct((2, QUAD, MODEL_WIDTH), BF16)
GRAD_SHAPES = tuple(
    jax.ShapeDtypeStruct((1, BLOCKS) + shape, F32)
    for shape in (
        (MODEL_WIDTH, 3 * MODEL_WIDTH), (MODEL_WIDTH, MODEL_WIDTH), (MODEL_WIDTH, MLP_WIDTH),
        (MODEL_WIDTH, MLP_WIDTH), (2, MODEL_WIDTH), (LEVEL_WINDOWS, HEADS, 2, BIAS_SLOTS),
    )
)


def tall_scratch():
    return pltpu.VMEM((LEVEL_WINDOWS * STACK, 128), F32)


def token_scratch():
    return pltpu.VMEM((TOKENS, MODEL_WIDTH), BF16)


def whole(array):
    rank = len(array.shape)
    return pl.BlockSpec(array.shape, lambda i, lat: (0,) * rank)


def one_block(array, index):
    rank = len(array.shape)
    return pl.BlockSpec((1, 1) + array.shape[2:], lambda i, lat: (0, index) + (0,) * (rank - 2))


def call(kernel, lat, ins, outs, scratch, aliases=None, limit=LIMIT):
    arrays = [array for array, _ in ins]
    return pl.pallas_call(
        kernel,
        out_shape=tuple(shape for shape, _ in outs),
        grid_spec=pltpu.PrefetchScalarGridSpec(
            num_scalar_prefetch=1,
            grid=(1,),
            in_specs=[spec for _, spec in ins],
            out_specs=tuple(spec for _, spec in outs),
            scratch_shapes=scratch,
        ),
        input_output_aliases=aliases or {},
        compiler_params=pltpu.CompilerParams(vmem_limit_bytes=limit),
    )(lat, *arrays)


def plain(*arrays):
    return [(array, whole(array)) for array in arrays]


def exchange(quads, by):
    lon = ("z", "x")
    ring, sides = lax.axis_size(lon), lax.axis_size("lat")
    lon_pairs = [(i, (i + by) % ring) for i in range(ring)]
    swap = [(i, i ^ 1) for i in range(sides)]
    both = [
        (i * sides + j, ((i + by) % ring) * sides + (j ^ 1)) for i in range(ring) for j in range(sides)
    ]
    return (
        quads[0],
        lax.ppermute(quads[1], lon, lon_pairs),
        lax.ppermute(quads[2], "lat", swap),
        lax.ppermute(quads[3], lon + ("lat",), both),
    )


def swap_all(values, axes):
    return lax.all_to_all(values, axes, split_axis=0, concat_axis=0, tiled=True)


def pass_x(sends):
    size = lax.axis_size("x")
    return (sends[0],) + tuple(
        lax.ppermute(sends[step], "x", [(i, (i + step) % size) for i in range(size)])
        for step in range(1, size)
    )


def slab_sum(slabs):
    total = slabs[0][...].astype(F32)
    for slab in slabs[1:]:
        total = total + slab[...].astype(F32)
    return total


def write_parts(total, out_ref, first):
    for index in range(out_ref.shape[0]):
        weights = total[index * WEIGHT_PART : (index + 1) * WEIGHT_PART]
        start = WEIGHT_SLAB + index * TABLE_PART
        part = jnp.concatenate([weights, total[start : start + TABLE_PART]], axis=0)
        out_ref[index, pl.ds(first, SENT), :] = part.astype(BF16)


def part_sum(spread_ref, first):
    sides = []
    for side in range(2):
        total = spread_ref[side, pl.ds(first, SENT), :].astype(F32)
        for index in range(side + 2, spread_ref.shape[0], 2):
            total = total + spread_ref[index, pl.ds(first, SENT), :].astype(F32)
        sides.append(total)
    weights = sides[0][:WEIGHT_PART] + sides[1][:WEIGHT_PART]
    spare = jnp.zeros((PART - SENT - TABLE_PART, 128), F32)
    rows = [weights, sides[0][WEIGHT_PART:], sides[1][WEIGHT_PART:], spare]
    return jnp.concatenate(rows, axis=0).astype(BF16)


def first_kernel(here_ref, slab0, slab1, slab2, slab3, out_ref):
    write_parts(slab_sum((slab0, slab1, slab2, slab3)), out_ref, 0)


def second_kernel(here_ref, late_ref, slab0, slab1, slab2, slab3, out_ref):
    late = part_sum(late_ref, 0)
    for index in range(out_ref.shape[0]):
        out_ref[index, pl.ds(0, PART), :] = late
    write_parts(slab_sum((slab0, slab1, slab2, slab3)), out_ref, PART)


def third_kernel(here_ref, both_ref, late_ref, early_ref):
    early = part_sum(both_ref, PART)
    for index in range(late_ref.shape[0]):
        late_ref[index] = both_ref[index, pl.ds(0, PART), :]
        early_ref[index] = early


def parts_shape(count, width):
    return jax.ShapeDtypeStruct((count, width, 128), BF16)


def unpack(parts, here, index, scale, previous):
    ins = plain(*parts)
    aliases = {}
    if previous is not None:
        ins = ins + [(array, pl.BlockSpec(memory_space=pl.ANY)) for array in previous]
        aliases = {1 + len(parts) + place: place for place in range(6)}
    outs = [(shape, one_block(shape, index)) for shape in GRAD_SHAPES]
    scratch = [pltpu.VMEM((X_SIZE, WEIGHT_SLAB, 128), F32)]
    scratch += [pltpu.VMEM((X_SIZE, TABLE_SLAB, 128), F32) for _ in range(2)]
    scratch += [pltpu.VMEM((TABLE_ROWS, 128), F32) for _ in range(2)] + type_scratch()
    return call(functools.partial(unpack_kernel, scale), here, ins, outs, scratch, aliases)


def type_scratch():
    return [pltpu.VMEM((TYPE_ROWS, 128), F32) for _ in range(3)]


def pack_scratch():
    return pltpu.VMEM((X_SIZE,) + SLAB_SHAPE.shape, BF16)


def stored_tokens(array):
    return array[0].transpose(1, 2, 0, 3).reshape(TOKENS, MODEL_WIDTH)


def on_device(
    inputs, grad_output, norm_gains, input_weight, output_weight, expand_weight, reduce_weight,
    bias_table,
):
    lat_index = lax.axis_index("lat")
    here = jnp.stack([lat_index, lax.axis_index("x")]).astype(jnp.int32)
    orders = [jnp.asarray(order) for order in quad_orders()]
    split, join_rolled, split_rolled, join, natural, early_split, stored = orders
    reduce_weight = reduce_weight.swapaxes(2, 3)
    bias_table = bias_table.swapaxes(3, 4)
    weights = [
        [(array, one_block(array, block)) for array in
         (norm_gains, input_weight, output_weight, expand_weight, reduce_weight)]
        for block in range(BLOCKS)
    ]
    tables = [[(bias_table, one_block(bias_table, block))] for block in range(BLOCKS)]
    front_scratch = [tall_scratch(), tall_scratch()] + type_scratch()
    front_scratch.append(pltpu.VMEM((8, BIAS_SLOTS), F32))
    outs = call(
        forward_kernel,
        here,
        plain(stored_tokens(inputs), stored_tokens(grad_output)) + weights[0] + tables[0]
        + plain(split, natural, early_split),
        plain(*((PAIR_SHAPE,) * 4 + (TOKEN_SHAPE,) * 3 + (WEIGHT_SHAPE,) + (TOKEN_SHAPE,) * 3)),
        front_scratch,
        limit=FULL_LIMIT,
    )
    saved = outs[4:10]
    tokens = outs[10]
    quads = exchange(outs[:4], -1)
    gate = outs[0]
    bias = call(
        bias_kernel,
        here,
        tables[1] + [(gate, pl.BlockSpec(memory_space=pl.ANY))],
        plain(BIAS_SHAPE, BIAS_SHAPE),
        front_scratch[2:],
    )
    outs = call(
        turn_kernel,
        here,
        plain(*quads) + weights[1] + plain(*bias, join_rolled, split_rolled),
        plain(*((QUAD_SHAPE,) * 4 + (HALF_PACK_SHAPE, WEIGHT_SHAPE, GAIN_SHAPE))),
        [token_scratch() for _ in range(3)]
        + [pltpu.VMEM(WEIGHT_SHAPE.shape, BF16), token_scratch(),
           pltpu.VMEM((3, TOKENS, MODEL_WIDTH), BF16)],
    )
    flow_quads = exchange(outs[:4], 1)
    late = call(
        late_kernel,
        here,
        plain(*outs[4:]),
        plain(*(SLAB_SHAPE,) * 4),
        [tall_scratch(), tall_scratch(), pltpu.VMEM((X_SIZE, TABLE_SLAB, 128), BF16)],
    )
    flow_quads, late = lax.optimization_barrier((flow_quads, late))
    late = pass_x(late)
    outs = call(
        backward_kernel,
        here,
        plain(tokens, *flow_quads) + weights[0] + plain(join, stored, *saved),
        plain(*((TOKEN_SHAPE,) + (SLAB_SHAPE,) * 4)),
        [tall_scratch(), tall_scratch(), pack_scratch(),
         pltpu.VMEM((3, TOKENS, MODEL_WIDTH), BF16)],
    )
    grad_flow = outs[0]
    late, early = lax.optimization_barrier((late, outs[1:]))
    early = pass_x(early)
    rest = ("z", "lat")
    count = lax.axis_size(rest)
    lat_total = LAT_DEV * lax.axis_size("lat")
    scale = float(LEVELS * lat_total * LON_DEV * lax.axis_size(("z", "x"))) ** (-0.5)
    (late,) = call(first_kernel, here, plain(*late), plain(parts_shape(count, SENT)), [])
    late = swap_all(late, rest)
    (both,) = call(
        second_kernel, here, plain(late, *early), plain(parts_shape(count, PART + SENT)), []
    )
    upstream = lax.ppermute(
        grad_flow, "section", [(i, i - 1) for i in range(1, lax.axis_size("section"))]
    )
    both, upstream = lax.optimization_barrier((swap_all(both, rest), upstream))
    late, early = call(
        third_kernel, here, plain(both), plain(*(parts_shape(count, PART),) * 2), []
    )
    late = pass_x((late,) * X_SIZE)
    early = pass_x((swap_all(early, rest),) * X_SIZE)
    upstream = upstream.reshape(LAT_DEV, LON_DEV, LEVELS, MODEL_WIDTH).transpose(2, 0, 1, 3)[None]
    grads = unpack(late, here, 1, scale, None)
    grads = list(unpack(early, here, 0, scale, grads))
    grads[3] = grads[3].swapaxes(2, 3)
    grads[5] = grads[5].swapaxes(3, 4)
    return (upstream,) + tuple(grads)


def solution(mesh):
    sizes = mesh.shape
    grid = mesh.devices.reshape(
        sizes["section"], sizes["lon"] // X_SIZE, X_SIZE, sizes["lat"]
    )
    mesh = Mesh(grid, ("section", "z", "x", "lat"))
    return jax.shard_map(
        on_device,
        mesh=mesh,
        in_specs=(
            P("section", None, "lat", ("z", "x"), None),
            P("section", None, "lat", ("z", "x"), None),
            P("section", None, None, None),
            P("section", None, None, None),
            P("section", None, None, None),
            P("section", None, None, None),
            P("section", None, None, None),
            P("section", None, None, None, None, None),
        ),
        out_specs=(
            P("section", None, "lat", ("z", "x"), None),
            P("section", None, None, None),
            P("section", None, None, None),
            P("section", None, None, None),
            P("section", None, None, None),
            P("section", None, None, None),
            P("section", None, None, None, None, None),
        ),
        check_vma=False,
    )
```

```python
import functools

import jax
import jax.numpy as jnp
import numpy as np
from jax import lax
from jax.experimental import pallas as pl
from jax.experimental.pallas import tpu as pltpu
from jax.sharding import Mesh
from jax.sharding import PartitionSpec as P

MODEL_WIDTH = 192
HEADS = 6
HEAD_SIZE = 32
LEVELS = 8
WIN_LEVELS = 2
WIN_LAT = 6
WIN_LON = 12
BLOCKS = 2
MLP_WIDTH = 768
LAT_DEV = 6
LON_DEV = 12
LEVEL_WINDOWS = 4
WIN_TOKENS = 144
BIAS_SLOTS = 3312

NORM_EPS = 1e-05
MASK_FILL = -10000.0
GELU_C = 0.7978845608028654
GELU_A = 0.044715

TOKENS = LEVELS * LAT_DEV * LON_DEV
QUAD = TOKENS // 4
STACK = HEADS * WIN_TOKENS
GROUPS = WIN_LEVELS * WIN_LAT
OFFSETS = 2 * WIN_LON - 1
PAIR_LANES = GROUPS * OFFSETS
PAIR_PAD = 384
TYPE_ROWS = LEVEL_WINDOWS * HEADS * GROUPS
X_SIZE = 4
WEIGHT_ROWS = 3456
TABLE_ROWS = 640
GAIN_ROW = 624
WEIGHT_SLAB = WEIGHT_ROWS // X_SIZE
TABLE_SLAB = TABLE_ROWS // X_SIZE
WEIGHT_PART = 54
TABLE_PART = 10
SENT = WEIGHT_PART + TABLE_PART
PART = 80

F32 = jnp.float32
BF16 = jnp.bfloat16


def quad_orders():
    level, row, col = np.meshgrid(
        np.arange(LEVELS), np.arange(LAT_DEV), np.arange(LON_DEV), indexing="ij"
    )
    half_rows, half_cols = WIN_LAT // 2, WIN_LON // 2
    quad = (1 - row // half_rows) * 2 + (1 - col // half_cols)
    place = (quad * LEVELS + level) * (half_rows * half_cols)
    place = place + (row % half_rows) * half_cols + col % half_cols
    split = place.reshape(-1)
    quad_r = (row // half_rows) * 2 + col // half_cols
    from_level = (level + WIN_LEVELS // 2) % LEVELS
    place_r = (quad_r * LEVELS + from_level) * (half_rows * half_cols)
    place_r = place_r + (row % half_rows) * half_cols + col % half_cols
    split_rolled = place_r.reshape(-1)
    join = np.argsort(split)
    join_rolled = np.argsort(split_rolled)
    natural = np.arange(TOKENS).reshape(LEVELS, LAT_DEV, LON_DEV).transpose(1, 2, 0).reshape(-1)
    stored = np.argsort(natural)
    orders = (split, join_rolled, split_rolled, join, natural, split[natural], stored)
    return [order.astype(np.int32)[None, :] for order in orders]


def dot_nn(a, b):
    return jnp.dot(a, b, preferred_element_type=F32)


def dot_nt(a, b):
    return lax.dot_general(a, b, (((1,), (1,)), ((), ())), preferred_element_type=F32)


def dot_tn(a, b):
    return lax.dot_general(a, b, (((0,), (0,)), ((), ())), preferred_element_type=F32)


def reorder(values, order_row):
    rows = lax.broadcasted_iota(jnp.int32, (TOKENS, TOKENS), 0)
    pick = jnp.where(rows == order_row, 1.0, 0.0).astype(BF16)
    return dot_nn(pick, values).astype(BF16)


def norm_stats(values):
    centred = values - jnp.mean(values, axis=-1, keepdims=True)
    spread = jnp.mean(centred * centred, axis=-1, keepdims=True)
    inv = lax.rsqrt(spread + NORM_EPS)
    return centred * inv, inv


def norm_grad(grad, unit, inv, gain_row):
    gain_grad = jnp.sum(grad * unit, axis=0, keepdims=True)
    grad_unit = grad * gain_row
    first = jnp.mean(grad_unit, axis=-1, keepdims=True)
    second = jnp.mean(grad_unit * unit, axis=-1, keepdims=True)
    return inv * (grad_unit - first - unit * second), gain_grad


def head_masks():
    lane = lax.broadcasted_iota(jnp.int32, (1, MODEL_WIDTH), 1)
    return [
        jnp.logical_and(lane >= h * HEAD_SIZE, lane < (h + 1) * HEAD_SIZE) for h in range(HEADS)
    ]


def stack_heads(values, masks):
    wide = values.astype(F32)
    return jnp.concatenate([jnp.where(m, wide, 0.0) for m in masks], axis=0).astype(BF16)


def fold_heads(stacked, masks):
    total = jnp.where(masks[0], stacked[:WIN_TOKENS], 0.0)
    for h in range(1, HEADS):
        total = jnp.where(masks[h], stacked[h * WIN_TOKENS : (h + 1) * WIN_TOKENS], total)
    return total


def pair_pick(query_col):
    key = lax.broadcasted_iota(jnp.int32, (256, PAIR_PAD), 0)
    lane = lax.broadcasted_iota(jnp.int32, (256, PAIR_PAD), 1)
    group = lax.shift_right_logical(key * 5462, 16)
    key_col = key - group * WIN_LON
    target = group * OFFSETS + (WIN_LON - 1 + query_col) - key_col
    hit = jnp.logical_and(lane == target, key < WIN_TOKENS)
    return jnp.where(hit, 1.0, 0.0).astype(BF16)


def segment_start(group, key_level):
    query_level, query_row = group // WIN_LAT, group % WIN_LAT
    return ((query_level * WIN_LEVELS + key_level) * WIN_LAT + query_row) * WIN_LAT * OFFSETS


def load_table(table_ref, side, parts, lines):
    width = WIN_LAT * OFFSETS
    for window in range(LEVEL_WINDOWS):
        for h in range(HEADS):
            lines[h : h + 1, :] = table_ref[0, 0, window, h, pl.ds(side, 1), :]
        rows = lines[:HEADS, :]
        for group in range(GROUPS):
            pieces = []
            for key_level in range(WIN_LEVELS):
                start = segment_start(group, key_level)
                pieces.append(rows[:, start : start + width])
            pieces.append(jnp.zeros((HEADS, PAIR_PAD - PAIR_LANES), F32))
            line = jnp.concatenate(pieces, axis=1)
            place = pl.ds(window * HEADS * GROUPS + group, HEADS, stride=GROUPS)
            for index, part in enumerate(parts):
                part[place, :] = line[:, index * 128 : (index + 1) * 128]
    return jnp.concatenate([part[...] for part in parts], axis=1)


def pair_spread(query_col):
    lane = lax.broadcasted_iota(jnp.int32, (PAIR_PAD, 256), 0)
    key = lax.broadcasted_iota(jnp.int32, (PAIR_PAD, 256), 1)
    group = lax.shift_right_logical(key * 5462, 16)
    key_col = key - group * WIN_LON
    target = group * OFFSETS + (WIN_LON - 1 + query_col) - key_col
    hit = jnp.logical_and(lane == target, key < WIN_TOKENS)
    return jnp.where(hit, 1.0, 0.0).astype(BF16)


def build_bias(table, bias_a, bias_b):
    high = table.astype(BF16)
    rest = table - high.astype(F32)
    middle = rest.astype(BF16)
    low = (rest - middle.astype(F32)).astype(BF16)
    terms = jnp.concatenate([high, middle, low], axis=0)
    for query_col in range(WIN_LON):
        wide = dot_nn(terms, pair_spread(query_col))
        spread = wide[:TYPE_ROWS] + wide[TYPE_ROWS : 2 * TYPE_ROWS] + wide[2 * TYPE_ROWS :]
        bias_a[pl.ds(query_col, TYPE_ROWS, stride=WIN_LON), :] = spread[:, :128]
        bias_b[pl.ds(query_col, TYPE_ROWS, stride=WIN_LON), :] = spread[:, 128:]


def fold_table(score_a, score_b):
    total = jnp.zeros((TYPE_ROWS, PAIR_PAD), F32)
    for query_col in range(WIN_LON):
        pick = pair_pick(query_col)
        left = score_a[pl.ds(query_col, TYPE_ROWS, stride=WIN_LON), :]
        right = score_b[pl.ds(query_col, TYPE_ROWS, stride=WIN_LON), :]
        total = total + dot_nn(jnp.concatenate([left, right], axis=1).astype(BF16), pick)
    return total


def shift_mask(window, lat_row):
    shape = (WIN_TOKENS, WIN_TOKENS)
    half = WIN_TOKENS // 2
    parts = []
    for axis in (0, 1):
        token = lax.broadcasted_iota(jnp.int32, shape, axis)
        upper = token >= half
        inner = jnp.where(upper, token - half, token)
        parts.append((upper, inner >= half // 2))
    rows_differ = jnp.where(parts[0][1] != parts[1][1], 1.0, 0.0) * lat_row
    if window == LEVEL_WINDOWS - 1:
        levels_differ = jnp.where(parts[0][0] != parts[1][0], 1.0, 0.0)
        rows_differ = jnp.maximum(rows_differ, levels_differ)
    return rows_differ * MASK_FILL


def attention_front(unit, gain_row, input_weight, bias_a, bias_b, lat_row, q_ref, k_ref, v_ref, w_ref, mix_ref):
    normed = (unit * gain_row).astype(BF16)
    q_ref[...] = (dot_nn(normed, input_weight[:, :MODEL_WIDTH]) * HEAD_SIZE ** (-0.5)).astype(BF16)
    k_ref[...] = dot_nn(normed, input_weight[:, MODEL_WIDTH : 2 * MODEL_WIDTH]).astype(BF16)
    v_ref[...] = dot_nn(normed, input_weight[:, 2 * MODEL_WIDTH :]).astype(BF16)
    masks = head_masks()
    for window in range(LEVEL_WINDOWS):
        rows = pl.ds(window * WIN_TOKENS, WIN_TOKENS)
        stack_rows = pl.ds(window * STACK, STACK)
        queries = stack_heads(q_ref[rows, :], masks)
        scores = dot_nt(queries, k_ref[rows, :])
        bias = jnp.concatenate(
            [bias_a[stack_rows, :], bias_b[stack_rows, :][:, : WIN_TOKENS - 128]], axis=1
        )
        scores = scores + bias
        if lat_row is not None:
            mask = shift_mask(window, lat_row)
            scores = scores + jnp.concatenate([mask] * HEADS, axis=0)
        scores = jnp.exp(scores - jnp.max(scores, axis=-1, keepdims=True))
        weights = (scores / jnp.sum(scores, axis=-1, keepdims=True)).astype(BF16)
        w_ref[stack_rows, :] = weights
        mixed = dot_nn(weights, v_ref[rows, :])
        mix_ref[rows, :] = fold_heads(mixed, masks).astype(BF16)
    return normed


def gelu_parts(pre):
    square = pre * pre
    tanh = jnp.tanh(GELU_C * (pre + GELU_A * pre * square))
    half = 0.5 * (1.0 + tanh)
    slope = half + 0.5 * pre * (1.0 - tanh * tanh) * (GELU_C * (1.0 + 3.0 * GELU_A * square))
    return pre * half, slope


def pack_rows(out_ref, first, values, slab, base):
    done = 0
    while done < values.shape[0]:
        side, inner = (first + done) // slab, (first + done) % slab
        count = min(values.shape[0] - done, slab - inner)
        out_ref[side, pl.ds(base + inner, count), :] = values[done : done + count].astype(BF16)
        done += count


def pack_columns(out_ref, first, values, slab=WEIGHT_SLAB, base=0):
    rows, lanes = values.shape
    for block in range(lanes // 128):
        pack_rows(
            out_ref, first + block * rows, values[:, block * 128 : (block + 1) * 128], slab, base
        )


def backward(e, x_unit, x_inv, gains, middle, weights4, saved, keep_scores, pack_ref, gproj_ref):
    input_weight, output_weight, expand_weight, reduce_weight = weights4
    q_ref, k_ref, v_ref, w_ref, mix_ref = saved
    masks = head_masks()
    mid_unit, mid_inv = norm_stats(middle.astype(F32))
    gain_mid = gains[1:2, :]
    normed_mid = (mid_unit * gain_mid).astype(BF16)
    hidden, slope = gelu_parts(dot_nn(normed_mid, expand_weight))
    hidden = hidden.astype(BF16)
    grad_pre = (slope * dot_nn(e, reduce_weight)).astype(BF16)
    pack_columns(pack_ref, 2304, dot_tn(e, hidden))
    pack_columns(pack_ref, 1152, dot_tn(normed_mid, grad_pre))
    grad_norm, gain_mid_grad = norm_grad(dot_nt(grad_pre, expand_weight), mid_unit, mid_inv, gain_mid)
    grad_middle = e.astype(F32) + grad_norm
    grad_attended = grad_middle.astype(BF16)
    output_grad = dot_tn(mix_ref[...], grad_attended)
    grad_mixture = dot_nt(grad_attended, output_weight).astype(BF16)
    for window in range(LEVEL_WINDOWS):
        base = window * WIN_TOKENS
        rows = pl.ds(base, WIN_TOKENS)
        stack_rows = pl.ds(window * STACK, STACK)
        queries = stack_heads(q_ref[rows, :], masks)
        grads = stack_heads(grad_mixture[base : base + WIN_TOKENS], masks)
        weights = w_ref[stack_rows, :]
        keys = k_ref[rows, :]
        gproj_ref[2, rows, :] = dot_tn(weights, grads).astype(BF16)
        grad_weights = dot_nt(grads, v_ref[rows, :])
        attention = weights.astype(F32)
        moved = attention * grad_weights
        grad_scores = attention * (grad_weights - jnp.sum(moved, axis=-1, keepdims=True))
        score_part = grad_scores.astype(BF16)
        keep_scores(stack_rows, grad_scores, score_part)
        grad_queries = fold_heads(dot_nn(score_part, keys), masks) * HEAD_SIZE ** (-0.5)
        gproj_ref[0, rows, :] = grad_queries.astype(BF16)
        gproj_ref[1, rows, :] = dot_tn(score_part, queries).astype(BF16)
    normed = (x_unit * gains[0:1, :]).astype(BF16)
    parts = [gproj_ref[part] for part in range(3)]
    weight_grads = [dot_tn(normed, part) for part in parts] + [output_grad]
    pack_columns(pack_ref, 0, jnp.concatenate(weight_grads, axis=1))
    grad_normed = dot_nt(parts[0], input_weight[:, :MODEL_WIDTH])
    grad_normed = grad_normed + dot_nt(parts[1], input_weight[:, MODEL_WIDTH : 2 * MODEL_WIDTH])
    grad_normed = grad_normed + dot_nt(parts[2], input_weight[:, 2 * MODEL_WIDTH :])
    grad_normed = grad_normed.astype(BF16).astype(F32)
    grad_in, gain_in_grad = norm_grad(grad_normed, x_unit, x_inv, gains[0:1, :])
    gain_flat = jnp.concatenate([gain_in_grad, gain_mid_grad], axis=1)
    gain_rows = [gain_flat[:, i * 128 : (i + 1) * 128] for i in range(3)]
    gain_rows.append(jnp.zeros((TABLE_ROWS - GAIN_ROW - 3, 128), F32))
    result = (grad_middle + grad_in).astype(BF16)
    return result, jnp.concatenate(gain_rows, axis=0)


def keep_split(score_a, score_b):
    def keep(stack_rows, grad_scores, score_part):
        score_a[stack_rows, :] = grad_scores[:, :128]
        score_b[stack_rows, :] = jnp.concatenate(
            [grad_scores[:, 128:], jnp.zeros((STACK, 256 - WIN_TOKENS), F32)], axis=1
        )

    return keep


def pack_table(pack_ref, score_a, score_b, gain_rows, base):
    folded = fold_table(score_a, score_b)
    pack_columns(pack_ref, 0, folded[:, :256], TABLE_SLAB, base)
    tail = TYPE_ROWS // HEADS
    pieces = [folded[h * tail : (h + 1) * tail, 256:PAIR_LANES] for h in range(HEADS)]
    pieces.append(jnp.zeros((tail, 128 - HEADS * (PAIR_LANES - 256)), F32))
    rest = jnp.concatenate([jnp.concatenate(pieces, axis=1), gain_rows], axis=0)
    pack_rows(pack_ref, 2 * TYPE_ROWS, rest, TABLE_SLAB, base)


def forward_kernel(
    here_ref, x_ref, e_ref, gains_ref, wi_ref, wo_ref, we_ref, wr_ref, table_ref, order_ref,
    natural_ref, early_ref, quad0, quad1, quad2, quad3, q_ref, k_ref, v_ref, w_ref, mix_ref, mid_ref, tok_ref,
    bias_a, bias_b, part_a, part_b, part_c, lines,
):
    build_bias(load_table(table_ref, here_ref[0], (part_a, part_b, part_c), lines), bias_a, bias_b)
    gains = gains_ref[0, 0]
    order = order_ref[...]
    quads = (quad0, quad1, quad2, quad3)
    moved = reorder(e_ref[...], early_ref[...])
    for index, quad in enumerate(quads):
        quad[1] = moved[index * QUAD : (index + 1) * QUAD]
    tokens = reorder(x_ref[...], natural_ref[...])
    tok_ref[...] = tokens
    values = tokens.astype(F32)
    unit, _ = norm_stats(values)
    attention_front(
        unit, gains[0:1, :], wi_ref[0, 0], bias_a, bias_b, None, q_ref, k_ref, v_ref, w_ref, mix_ref
    )
    middle = (values + dot_nn(mix_ref[...], wo_ref[0, 0])).astype(BF16)
    mid_ref[...] = middle
    mid_f = middle.astype(F32)
    mid_unit, _ = norm_stats(mid_f)
    normed_mid = (mid_unit * gains[1:2, :]).astype(BF16)
    hidden, _ = gelu_parts(dot_nn(normed_mid, we_ref[0, 0]))
    output = (mid_f + dot_nt(hidden.astype(BF16), wr_ref[0, 0])).astype(BF16)
    moved = reorder(output, order)
    for index, quad in enumerate(quads):
        quad[0] = moved[index * QUAD : (index + 1) * QUAD]


def bias_kernel(here_ref, table_ref, gate_ref, bias_a, bias_b, part_a, part_b, part_c, lines):
    build_bias(load_table(table_ref, here_ref[0], (part_a, part_b, part_c), lines), bias_a, bias_b)


def turn_kernel(
    here_ref, x0, x1, x2, x3, gains_ref, wi_ref, wo_ref, we_ref, wr_ref, bias_a, bias_b,
    join_ref, split_ref, quad0, quad1, quad2, quad3, pack_ref, score_ref, gain_ref,
    q_ref, k_ref, v_ref, w_ref, mix_ref, gproj_ref,
):
    gains = gains_ref[0, 0]
    join = join_ref[...]
    pieces = (x0, x1, x2, x3)
    block_in = reorder(jnp.concatenate([piece[0] for piece in pieces], axis=0), join)
    e = reorder(jnp.concatenate([piece[1] for piece in pieces], axis=0), join)
    values = block_in.astype(F32)
    unit, inv = norm_stats(values)
    input_weight, output_weight = wi_ref[0, 0], wo_ref[0, 0]
    attention_front(
        unit, gains[0:1, :], input_weight, bias_a, bias_b, here_ref[0].astype(F32), q_ref, k_ref,
        v_ref, w_ref, mix_ref,
    )
    attended = dot_nn(mix_ref[...], output_weight).astype(BF16).astype(F32)
    middle = (values + attended).astype(BF16)

    def keep(stack_rows, grad_scores, score_part):
        score_ref[stack_rows, :] = score_part

    result, gain_ref[...] = backward(
        e, unit, inv, gains, middle, (input_weight, output_weight, we_ref[0, 0], wr_ref[0, 0]),
        (q_ref, k_ref, v_ref, w_ref, mix_ref), keep, pack_ref, gproj_ref,
    )
    moved = reorder(result, split_ref[...])
    for index, quad in enumerate((quad0, quad1, quad2, quad3)):
        quad[...] = moved[index * QUAD : (index + 1) * QUAD]


def late_kernel(
    here_ref, pack_ref, score_ref, gain_ref, send0, send1, send2, send3, score_a, score_b, table_ref
):
    keep = keep_split(score_a, score_b)
    for window in range(LEVEL_WINDOWS):
        stack_rows = pl.ds(window * STACK, STACK)
        keep(stack_rows, score_ref[stack_rows, :].astype(F32), None)
    pack_table(table_ref, score_a, score_b, gain_ref[...], 0)
    for step, send in enumerate((send0, send1, send2, send3)):
        owner = lax.rem(here_ref[1] + step, X_SIZE)
        send[pl.ds(0, WEIGHT_SLAB), :] = pack_ref[owner]
        send[pl.ds(WEIGHT_SLAB, TABLE_SLAB), :] = table_ref[owner]


def send_slabs(here_ref, pack_ref, sends):
    for step, send in enumerate(sends):
        send[...] = pack_ref[lax.rem(here_ref[1] + step, X_SIZE)]


def backward_kernel(
    here_ref, x_ref, e0, e1, e2, e3, gains_ref, wi_ref, wo_ref, we_ref, wr_ref, join_ref,
    stored_ref, q_ref, k_ref, v_ref, w_ref, mix_ref, mid_ref, out_ref, send0, send1, send2, send3,
    score_a, score_b, pack_ref, gproj_ref,
):
    e = reorder(jnp.concatenate([e0[...], e1[...], e2[...], e3[...]], axis=0), join_ref[...])
    unit, inv = norm_stats(x_ref[...].astype(F32))
    result, gain_rows = backward(
        e, unit, inv, gains_ref[0, 0], mid_ref[...],
        (wi_ref[0, 0], wo_ref[0, 0], we_ref[0, 0], wr_ref[0, 0]),
        (q_ref, k_ref, v_ref, w_ref, mix_ref), keep_split(score_a, score_b), pack_ref, gproj_ref,
    )
    pack_table(pack_ref, score_a, score_b, gain_rows, WEIGHT_SLAB)
    out_ref[...] = reorder(result, stored_ref[...])
    send_slabs(here_ref, pack_ref, (send0, send1, send2, send3))


def unpack_kernel(scale, here_ref, got0, got1, got2, got3, *refs):
    gi_ref, go_ref, ge_ref, gr_ref, gn_ref, gt_ref = refs[-14:-8]
    rows, slab0, slab1, t0, t1, part_a, part_b, part_c = refs[-8:]
    for step, got in enumerate((got0, got1, got2, got3)):
        origin = lax.rem(here_ref[1] + X_SIZE - step, X_SIZE)
        for index in range(got.shape[0]):
            part = got[index].astype(F32)
            rows[origin, pl.ds(index * WEIGHT_PART, WEIGHT_PART), :] = part[:WEIGHT_PART] * scale
            for side, table in enumerate((slab0, slab1)):
                first = WEIGHT_PART + side * TABLE_PART
                table[origin, pl.ds(index * TABLE_PART, TABLE_PART), :] = part[
                    first : first + TABLE_PART
                ]
    for slab, table in ((slab0, t0), (slab1, t1)):
        for origin in range(X_SIZE):
            table[pl.ds(origin * TABLE_SLAB, TABLE_SLAB), :] = slab[origin]

    def block(first, count):
        pieces = []
        while count:
            origin, inner = first // WEIGHT_SLAB, first % WEIGHT_SLAB
            here = min(count, WEIGHT_SLAB - inner)
            pieces.append(rows[origin, pl.ds(inner, here), :])
            first, count = first + here, count - here
        return pieces[0] if len(pieces) == 1 else jnp.concatenate(pieces, axis=0)

    for index in range(4):
        gi_ref[0, 0, :, pl.ds(index * 128, 128)] = block(index * 192, 192)
    mixed = block(4 * 192, 192)
    gi_ref[0, 0, :, pl.ds(512, 64)] = mixed[:, :64]
    go_ref[0, 0] = jnp.concatenate([mixed[:, 64:], block(5 * 192, 192)], axis=1)
    for index in range(6):
        ge_ref[0, 0, :, pl.ds(index * 128, 128)] = block(1152 + index * 192, 192)
    for index in range(6):
        gr_ref[0, 0, :, pl.ds(index * 128, 128)] = block(2304 + index * 192, 192)
    gain = (t0[pl.ds(GAIN_ROW, 8), :] + t1[pl.ds(GAIN_ROW, 8), :]) * scale
    gn_ref[0, 0, 0:1, :] = jnp.concatenate([gain[0:1], gain[1:2, :64]], axis=1)
    gn_ref[0, 0, 1:2, :] = jnp.concatenate([gain[1:2, 64:], gain[2:3]], axis=1)
    tail, width = TYPE_ROWS // HEADS, PAIR_LANES - 256
    for side, table in enumerate((t0, t1)):
        rest = table[pl.ds(2 * TYPE_ROWS, tail), :]
        for h in range(HEADS):
            part_c[pl.ds(h * tail, tail), pl.ds(0, width)] = rest[:, h * width : (h + 1) * width]
        for window in range(LEVEL_WINDOWS):
            lines = []
            for group in range(GROUPS):
                first = window * HEADS * GROUPS + group
                place = pl.ds(first, HEADS, stride=GROUPS)
                upper = pl.ds(TYPE_ROWS + first, HEADS, stride=GROUPS)
                lines.append(
                    jnp.concatenate([table[place, :], table[upper, :], part_c[place, :]], axis=1)
                )
            span = WIN_LAT * OFFSETS
            ordered = []
            for query_level in range(WIN_LEVELS):
                for key_level in range(WIN_LEVELS):
                    for row in range(WIN_LAT):
                        line = lines[query_level * WIN_LAT + row]
                        ordered.append(line[:, key_level * span : (key_level + 1) * span])
            result = jnp.concatenate(ordered, axis=1)
            for h in range(HEADS):
                gt_ref[0, 0, window, h, side : side + 1, :] = result[h : h + 1]


LIMIT = 32 * 1024 * 1024
FULL_LIMIT = 60 * 1024 * 1024
TOKEN_SHAPE = jax.ShapeDtypeStruct((TOKENS, MODEL_WIDTH), BF16)
QUAD_SHAPE = jax.ShapeDtypeStruct((QUAD, MODEL_WIDTH), BF16)
WEIGHT_SHAPE = jax.ShapeDtypeStruct((LEVEL_WINDOWS * STACK, WIN_TOKENS), BF16)
BIAS_SHAPE = jax.ShapeDtypeStruct((LEVEL_WINDOWS * STACK, 128), F32)
GAIN_SHAPE = jax.ShapeDtypeStruct((TABLE_ROWS - GAIN_ROW, 128), F32)
HALF_PACK_SHAPE = jax.ShapeDtypeStruct((X_SIZE, WEIGHT_SLAB, 128), BF16)
SLAB_SHAPE = jax.ShapeDtypeStruct((WEIGHT_SLAB + TABLE_SLAB, 128), BF16)
PAIR_SHAPE = jax.ShapeDtypeStruct((2, QUAD, MODEL_WIDTH), BF16)
GRAD_SHAPES = tuple(
    jax.ShapeDtypeStruct((1, BLOCKS) + shape, F32)
    for shape in (
        (MODEL_WIDTH, 3 * MODEL_WIDTH), (MODEL_WIDTH, MODEL_WIDTH), (MODEL_WIDTH, MLP_WIDTH),
        (MODEL_WIDTH, MLP_WIDTH), (2, MODEL_WIDTH), (LEVEL_WINDOWS, HEADS, 2, BIAS_SLOTS),
    )
)


def tall_scratch():
    return pltpu.VMEM((LEVEL_WINDOWS * STACK, 128), F32)


def token_scratch():
    return pltpu.VMEM((TOKENS, MODEL_WIDTH), BF16)


def whole(array):
    rank = len(array.shape)
    return pl.BlockSpec(array.shape, lambda i: (0,) * rank)


def one_block(array, index):
    rank = len(array.shape)
    return pl.BlockSpec((1, 1) + array.shape[2:], lambda i: (0, index) + (0,) * (rank - 2))


def call(kernel, here, ins, outs, scratch, aliases=None, limit=LIMIT):
    arrays = [array for array, _ in ins]
    return pl.pallas_call(
        functools.partial(kernel, here),
        out_shape=tuple(shape for shape, _ in outs),
        grid_spec=pltpu.PrefetchScalarGridSpec(
            num_scalar_prefetch=0,
            grid=(1,),
            in_specs=[spec for _, spec in ins],
            out_specs=tuple(spec for _, spec in outs),
            scratch_shapes=scratch,
        ),
        input_output_aliases=aliases or {},
        compiler_params=pltpu.CompilerParams(vmem_limit_bytes=limit),
    )(*arrays)


class Here:
    def __getitem__(self, index):
        return lax.axis_index(("lat", "x")[index])


def plain(*arrays):
    return [(array, whole(array)) for array in arrays]


def exchange(quads, by):
    lon = ("z", "x")
    ring, sides = lax.axis_size(lon), lax.axis_size("lat")
    lon_pairs = [(i, (i + by) % ring) for i in range(ring)]
    swap = [(i, i ^ 1) for i in range(sides)]
    both = [
        (i * sides + j, ((i + by) % ring) * sides + (j ^ 1)) for i in range(ring) for j in range(sides)
    ]
    return (
        quads[0],
        lax.ppermute(quads[1], lon, lon_pairs),
        lax.ppermute(quads[2], "lat", swap),
        lax.ppermute(quads[3], lon + ("lat",), both),
    )


def swap_all(values, axes):
    return lax.all_to_all(values, axes, split_axis=0, concat_axis=0, tiled=True)


def pass_x(sends):
    size = lax.axis_size("x")
    return (sends[0],) + tuple(
        lax.ppermute(sends[step], "x", [(i, (i + step) % size) for i in range(size)])
        for step in range(1, size)
    )


def slab_sum(slabs):
    total = slabs[0][...].astype(F32)
    for slab in slabs[1:]:
        total = total + slab[...].astype(F32)
    return total


def write_parts(total, out_ref, first):
    for index in range(out_ref.shape[0]):
        weights = total[index * WEIGHT_PART : (index + 1) * WEIGHT_PART]
        start = WEIGHT_SLAB + index * TABLE_PART
        part = jnp.concatenate([weights, total[start : start + TABLE_PART]], axis=0)
        out_ref[index, pl.ds(first, SENT), :] = part.astype(BF16)


def part_sum(spread_ref, first):
    sides = []
    for side in range(2):
        total = spread_ref[side, pl.ds(first, SENT), :].astype(F32)
        for index in range(side + 2, spread_ref.shape[0], 2):
            total = total + spread_ref[index, pl.ds(first, SENT), :].astype(F32)
        sides.append(total)
    weights = sides[0][:WEIGHT_PART] + sides[1][:WEIGHT_PART]
    spare = jnp.zeros((PART - SENT - TABLE_PART, 128), F32)
    rows = [weights, sides[0][WEIGHT_PART:], sides[1][WEIGHT_PART:], spare]
    return jnp.concatenate(rows, axis=0).astype(BF16)


def first_kernel(here_ref, slab0, slab1, slab2, slab3, out_ref):
    write_parts(slab_sum((slab0, slab1, slab2, slab3)), out_ref, 0)


def second_kernel(here_ref, late_ref, slab0, slab1, slab2, slab3, out_ref):
    late = part_sum(late_ref, 0)
    for index in range(out_ref.shape[0]):
        out_ref[index, pl.ds(0, PART), :] = late
    write_parts(slab_sum((slab0, slab1, slab2, slab3)), out_ref, PART)


def third_kernel(here_ref, both_ref, late_ref, early_ref):
    early = part_sum(both_ref, PART)
    for index in range(late_ref.shape[0]):
        late_ref[index] = both_ref[index, pl.ds(0, PART), :]
        early_ref[index] = early


def parts_shape(count, width):
    return jax.ShapeDtypeStruct((count, width, 128), BF16)


def unpack(parts, here, index, scale, previous):
    ins = plain(*parts)
    aliases = {}
    if previous is not None:
        ins = ins + [(array, pl.BlockSpec(memory_space=pl.ANY)) for array in previous]
        aliases = {len(parts) + place: place for place in range(6)}
    outs = [(shape, one_block(shape, index)) for shape in GRAD_SHAPES]
    scratch = [pltpu.VMEM((X_SIZE, WEIGHT_SLAB, 128), F32)]
    scratch += [pltpu.VMEM((X_SIZE, TABLE_SLAB, 128), F32) for _ in range(2)]
    scratch += [pltpu.VMEM((TABLE_ROWS, 128), F32) for _ in range(2)] + type_scratch()
    return call(functools.partial(unpack_kernel, scale), here, ins, outs, scratch, aliases)


def type_scratch():
    return [pltpu.VMEM((TYPE_ROWS, 128), F32) for _ in range(3)]


def pack_scratch():
    return pltpu.VMEM((X_SIZE,) + SLAB_SHAPE.shape, BF16)


def stored_tokens(array):
    return array[0].transpose(1, 2, 0, 3).reshape(TOKENS, MODEL_WIDTH)


def on_device(
    inputs, grad_output, norm_gains, input_weight, output_weight, expand_weight, reduce_weight,
    bias_table,
):
    here = Here()
    orders = [jnp.asarray(order) for order in quad_orders()]
    split, join_rolled, split_rolled, join, natural, early_split, stored = orders
    reduce_weight = reduce_weight.swapaxes(2, 3)
    bias_table = bias_table.swapaxes(3, 4)
    weights = [
        [(array, one_block(array, block)) for array in
         (norm_gains, input_weight, output_weight, expand_weight, reduce_weight)]
        for block in range(BLOCKS)
    ]
    tables = [[(bias_table, one_block(bias_table, block))] for block in range(BLOCKS)]
    front_scratch = [tall_scratch(), tall_scratch()] + type_scratch()
    front_scratch.append(pltpu.VMEM((8, BIAS_SLOTS), F32))
    outs = call(
        forward_kernel,
        here,
        plain(stored_tokens(inputs), stored_tokens(grad_output)) + weights[0] + tables[0]
        + plain(split, natural, early_split),
        plain(*((PAIR_SHAPE,) * 4 + (TOKEN_SHAPE,) * 3 + (WEIGHT_SHAPE,) + (TOKEN_SHAPE,) * 3)),
        front_scratch,
        limit=FULL_LIMIT,
    )
    saved = outs[4:10]
    tokens = outs[10]
    quads = exchange(outs[:4], -1)
    gate = outs[0]
    bias = call(
        bias_kernel,
        here,
        tables[1] + [(gate, pl.BlockSpec(memory_space=pl.ANY))],
        plain(BIAS_SHAPE, BIAS_SHAPE),
        front_scratch[2:],
    )
    outs = call(
        turn_kernel,
        here,
        plain(*quads) + weights[1] + plain(*bias, join_rolled, split_rolled),
        plain(*((QUAD_SHAPE,) * 4 + (HALF_PACK_SHAPE, WEIGHT_SHAPE, GAIN_SHAPE))),
        [token_scratch() for _ in range(3)]
        + [pltpu.VMEM(WEIGHT_SHAPE.shape, BF16), token_scratch(),
           pltpu.VMEM((3, TOKENS, MODEL_WIDTH), BF16)],
    )
    flow_quads = exchange(outs[:4], 1)
    late = call(
        late_kernel,
        here,
        plain(*outs[4:]),
        plain(*(SLAB_SHAPE,) * 4),
        [tall_scratch(), tall_scratch(), pltpu.VMEM((X_SIZE, TABLE_SLAB, 128), BF16)],
    )
    flow_quads, late = lax.optimization_barrier((flow_quads, late))
    late = pass_x(late)
    outs = call(
        backward_kernel,
        here,
        plain(tokens, *flow_quads) + weights[0] + plain(join, stored, *saved),
        plain(*((TOKEN_SHAPE,) + (SLAB_SHAPE,) * 4)),
        [tall_scratch(), tall_scratch(), pack_scratch(),
         pltpu.VMEM((3, TOKENS, MODEL_WIDTH), BF16)],
    )
    grad_flow = outs[0]
    late, early = lax.optimization_barrier((late, outs[1:]))
    early = pass_x(early)
    rest = ("z", "lat")
    count = lax.axis_size(rest)
    lat_total = LAT_DEV * lax.axis_size("lat")
    scale = float(LEVELS * lat_total * LON_DEV * lax.axis_size(("z", "x"))) ** (-0.5)
    (late,) = call(first_kernel, here, plain(*late), plain(parts_shape(count, SENT)), [])
    late = swap_all(late, rest)
    (both,) = call(
        second_kernel, here, plain(late, *early), plain(parts_shape(count, PART + SENT)), []
    )
    upstream = lax.ppermute(
        grad_flow, "section", [(i, i - 1) for i in range(1, lax.axis_size("section"))]
    )
    both, upstream = lax.optimization_barrier((swap_all(both, rest), upstream))
    late, early = call(
        third_kernel, here, plain(both), plain(*(parts_shape(count, PART),) * 2), []
    )
    late = pass_x((late,) * X_SIZE)
    early = pass_x((swap_all(early, rest),) * X_SIZE)
    upstream = upstream.reshape(LAT_DEV, LON_DEV, LEVELS, MODEL_WIDTH).transpose(2, 0, 1, 3)[None]
    grads = unpack(late, here, 1, scale, None)
    grads = list(unpack(early, here, 0, scale, grads))
    grads[3] = grads[3].swapaxes(2, 3)
    grads[5] = grads[5].swapaxes(3, 4)
    return (upstream,) + tuple(grads)


def solution(mesh):
    sizes = mesh.shape
    grid = mesh.devices.reshape(
        sizes["section"], sizes["lon"] // X_SIZE, X_SIZE, sizes["lat"]
    )
    mesh = Mesh(grid, ("section", "z", "x", "lat"))
    return jax.shard_map(
        on_device,
        mesh=mesh,
        in_specs=(
            P("section", None, "lat", ("z", "x"), None),
            P("section", None, "lat", ("z", "x"), None),
            P("section", None, None, None),
            P("section", None, None, None),
            P("section", None, None, None),
            P("section", None, None, None),
            P("section", None, None, None),
            P("section", None, None, None, None, None),
        ),
        out_specs=(
            P("section", None, "lat", ("z", "x"), None),
            P("section", None, None, None),
            P("section", None, None, None),
            P("section", None, None, None),
            P("section", None, None, None),
            P("section", None, None, None),
            P("section", None, None, None, None, None),
        ),
        check_vma=False,
    )
```

```python
import functools

import jax
import jax.numpy as jnp
import numpy as np
from jax import lax
from jax.experimental import pallas as pl
from jax.experimental.pallas import tpu as pltpu
from jax.sharding import Mesh
from jax.sharding import PartitionSpec as P

MODEL_WIDTH = 192
HEADS = 6
HEAD_SIZE = 32
LEVELS = 8
WIN_LEVELS = 2
WIN_LAT = 6
WIN_LON = 12
BLOCKS = 2
MLP_WIDTH = 768
LAT_DEV = 6
LON_DEV = 12
LEVEL_WINDOWS = 4
WIN_TOKENS = 144
BIAS_SLOTS = 3312

NORM_EPS = 1e-05
MASK_FILL = -10000.0
GELU_C = 0.7978845608028654
GELU_A = 0.044715

TOKENS = LEVELS * LAT_DEV * LON_DEV
QUAD = TOKENS // 4
STACK = HEADS * WIN_TOKENS
GROUPS = WIN_LEVELS * WIN_LAT
OFFSETS = 2 * WIN_LON - 1
PAIR_LANES = GROUPS * OFFSETS
PAIR_PAD = 384
TYPE_ROWS = LEVEL_WINDOWS * HEADS * GROUPS
X_SIZE = 4
WEIGHT_ROWS = 3456
TABLE_ROWS = 640
GAIN_ROW = 624
WEIGHT_SLAB = WEIGHT_ROWS // X_SIZE
TABLE_SLAB = TABLE_ROWS // X_SIZE
WEIGHT_PART = 54
TABLE_PART = 10
SENT = WEIGHT_PART + TABLE_PART
PART = 80

F32 = jnp.float32
BF16 = jnp.bfloat16


def quad_orders():
    level, row, col = np.meshgrid(
        np.arange(LEVELS), np.arange(LAT_DEV), np.arange(LON_DEV), indexing="ij"
    )
    half_rows, half_cols = WIN_LAT // 2, WIN_LON // 2
    quad = (1 - row // half_rows) * 2 + (1 - col // half_cols)
    place = (quad * LEVELS + level) * (half_rows * half_cols)
    place = place + (row % half_rows) * half_cols + col % half_cols
    split = place.reshape(-1)
    quad_r = (row // half_rows) * 2 + col // half_cols
    from_level = (level + WIN_LEVELS // 2) % LEVELS
    place_r = (quad_r * LEVELS + from_level) * (half_rows * half_cols)
    place_r = place_r + (row % half_rows) * half_cols + col % half_cols
    split_rolled = place_r.reshape(-1)
    join = np.argsort(split)
    join_rolled = np.argsort(split_rolled)
    natural = np.arange(TOKENS).reshape(LEVELS, LAT_DEV, LON_DEV).transpose(1, 2, 0).reshape(-1)
    stored = np.argsort(natural)
    orders = (split, join_rolled, split_rolled, join, natural, split[natural], stored)
    return [order.astype(np.int32)[None, :] for order in orders]


def dot_nn(a, b):
    return jnp.dot(a, b, preferred_element_type=F32)


def dot_nt(a, b):
    return lax.dot_general(a, b, (((1,), (1,)), ((), ())), preferred_element_type=F32)


def dot_tn(a, b):
    return lax.dot_general(a, b, (((0,), (0,)), ((), ())), preferred_element_type=F32)


def reorder(values, order_row):
    rows = lax.broadcasted_iota(jnp.int32, (TOKENS, TOKENS), 0)
    pick = jnp.where(rows == order_row, 1.0, 0.0).astype(BF16)
    return dot_nn(pick, values).astype(BF16)


def norm_stats(values):
    centred = values - jnp.mean(values, axis=-1, keepdims=True)
    spread = jnp.mean(centred * centred, axis=-1, keepdims=True)
    inv = lax.rsqrt(spread + NORM_EPS)
    return centred * inv, inv


def norm_grad(grad, unit, inv, gain_row):
    gain_grad = jnp.sum(grad * unit, axis=0, keepdims=True)
    grad_unit = grad * gain_row
    first = jnp.mean(grad_unit, axis=-1, keepdims=True)
    second = jnp.mean(grad_unit * unit, axis=-1, keepdims=True)
    return inv * (grad_unit - first - unit * second), gain_grad


def head_masks():
    lane = lax.broadcasted_iota(jnp.int32, (1, MODEL_WIDTH), 1)
    return [
        jnp.logical_and(lane >= h * HEAD_SIZE, lane < (h + 1) * HEAD_SIZE) for h in range(HEADS)
    ]


def stack_heads(values, masks):
    wide = values.astype(F32)
    return jnp.concatenate([jnp.where(m, wide, 0.0) for m in masks], axis=0).astype(BF16)


def fold_heads(stacked, masks):
    total = jnp.where(masks[0], stacked[:WIN_TOKENS], 0.0)
    for h in range(1, HEADS):
        total = jnp.where(masks[h], stacked[h * WIN_TOKENS : (h + 1) * WIN_TOKENS], total)
    return total


def pair_pick(query_col):
    key = lax.broadcasted_iota(jnp.int32, (256, PAIR_PAD), 0)
    lane = lax.broadcasted_iota(jnp.int32, (256, PAIR_PAD), 1)
    group = lax.shift_right_logical(key * 5462, 16)
    key_col = key - group * WIN_LON
    target = group * OFFSETS + (WIN_LON - 1 + query_col) - key_col
    hit = jnp.logical_and(lane == target, key < WIN_TOKENS)
    return jnp.where(hit, 1.0, 0.0).astype(BF16)


def segment_start(group, key_level):
    query_level, query_row = group // WIN_LAT, group % WIN_LAT
    return ((query_level * WIN_LEVELS + key_level) * WIN_LAT + query_row) * WIN_LAT * OFFSETS


def load_table(table_ref, side, parts, lines):
    width = WIN_LAT * OFFSETS
    for window in range(LEVEL_WINDOWS):
        for h in range(HEADS):
            lines[h : h + 1, :] = table_ref[0, 0, window, h, pl.ds(side, 1), :]
        rows = lines[:HEADS, :]
        for group in range(GROUPS):
            pieces = []
            for key_level in range(WIN_LEVELS):
                start = segment_start(group, key_level)
                pieces.append(rows[:, start : start + width])
            pieces.append(jnp.zeros((HEADS, PAIR_PAD - PAIR_LANES), F32))
            line = jnp.concatenate(pieces, axis=1)
            place = pl.ds(window * HEADS * GROUPS + group, HEADS, stride=GROUPS)
            for index, part in enumerate(parts):
                part[place, :] = line[:, index * 128 : (index + 1) * 128]
    return jnp.concatenate([part[...] for part in parts], axis=1)


def pair_spread(query_col):
    lane = lax.broadcasted_iota(jnp.int32, (PAIR_PAD, 256), 0)
    key = lax.broadcasted_iota(jnp.int32, (PAIR_PAD, 256), 1)
    group = lax.shift_right_logical(key * 5462, 16)
    key_col = key - group * WIN_LON
    target = group * OFFSETS + (WIN_LON - 1 + query_col) - key_col
    hit = jnp.logical_and(lane == target, key < WIN_TOKENS)
    return jnp.where(hit, 1.0, 0.0).astype(BF16)


def build_bias(table, bias_a, bias_b):
    high = table.astype(BF16)
    rest = table - high.astype(F32)
    middle = rest.astype(BF16)
    low = (rest - middle.astype(F32)).astype(BF16)
    terms = jnp.concatenate([high, middle, low], axis=0)
    for query_col in range(WIN_LON):
        wide = dot_nn(terms, pair_spread(query_col))
        spread = wide[:TYPE_ROWS] + wide[TYPE_ROWS : 2 * TYPE_ROWS] + wide[2 * TYPE_ROWS :]
        bias_a[pl.ds(query_col, TYPE_ROWS, stride=WIN_LON), :] = spread[:, :128]
        bias_b[pl.ds(query_col, TYPE_ROWS, stride=WIN_LON), :] = spread[:, 128:]


def fold_table(score_a, score_b):
    total = jnp.zeros((TYPE_ROWS, PAIR_PAD), F32)
    for query_col in range(WIN_LON):
        pick = pair_pick(query_col)
        left = score_a[pl.ds(query_col, TYPE_ROWS, stride=WIN_LON), :]
        right = score_b[pl.ds(query_col, TYPE_ROWS, stride=WIN_LON), :]
        total = total + dot_nn(jnp.concatenate([left, right], axis=1).astype(BF16), pick)
    return total


def shift_mask(window, lat_row):
    shape = (WIN_TOKENS, WIN_TOKENS)
    half = WIN_TOKENS // 2
    parts = []
    for axis in (0, 1):
        token = lax.broadcasted_iota(jnp.int32, shape, axis)
        upper = token >= half
        inner = jnp.where(upper, token - half, token)
        parts.append((upper, inner >= half // 2))
    rows_differ = jnp.where(parts[0][1] != parts[1][1], 1.0, 0.0) * lat_row
    if window == LEVEL_WINDOWS - 1:
        levels_differ = jnp.where(parts[0][0] != parts[1][0], 1.0, 0.0)
        rows_differ = jnp.maximum(rows_differ, levels_differ)
    return rows_differ * MASK_FILL


def attention_front(unit, gain_row, input_weight, bias_a, bias_b, q_ref, k_ref, v_ref, w_ref, mix_ref):
    normed = (unit * gain_row).astype(BF16)
    q_ref[...] = (dot_nn(normed, input_weight[:, :MODEL_WIDTH]) * HEAD_SIZE ** (-0.5)).astype(BF16)
    k_ref[...] = dot_nn(normed, input_weight[:, MODEL_WIDTH : 2 * MODEL_WIDTH]).astype(BF16)
    v_ref[...] = dot_nn(normed, input_weight[:, 2 * MODEL_WIDTH :]).astype(BF16)
    masks = head_masks()
    for window in range(LEVEL_WINDOWS):
        rows = pl.ds(window * WIN_TOKENS, WIN_TOKENS)
        stack_rows = pl.ds(window * STACK, STACK)
        queries = stack_heads(q_ref[rows, :], masks)
        scores = dot_nt(queries, k_ref[rows, :])
        bias = jnp.concatenate(
            [bias_a[stack_rows, :], bias_b[stack_rows, :][:, : WIN_TOKENS - 128]], axis=1
        )
        scores = scores + bias
        scores = jnp.exp(scores - jnp.max(scores, axis=-1, keepdims=True))
        weights = (scores / jnp.sum(scores, axis=-1, keepdims=True)).astype(BF16)
        w_ref[stack_rows, :] = weights
        mixed = dot_nn(weights, v_ref[rows, :])
        mix_ref[rows, :] = fold_heads(mixed, masks).astype(BF16)
    return normed


def gelu_parts(pre):
    square = pre * pre
    tanh = jnp.tanh(GELU_C * (pre + GELU_A * pre * square))
    half = 0.5 * (1.0 + tanh)
    slope = half + 0.5 * pre * (1.0 - tanh * tanh) * (GELU_C * (1.0 + 3.0 * GELU_A * square))
    return pre * half, slope


def pack_rows(out_ref, first, values, slab, base):
    done = 0
    while done < values.shape[0]:
        side, inner = (first + done) // slab, (first + done) % slab
        count = min(values.shape[0] - done, slab - inner)
        out_ref[side, pl.ds(base + inner, count), :] = values[done : done + count].astype(BF16)
        done += count


def pack_columns(out_ref, first, values, slab=WEIGHT_SLAB, base=0):
    rows, lanes = values.shape
    for block in range(lanes // 128):
        pack_rows(
            out_ref, first + block * rows, values[:, block * 128 : (block + 1) * 128], slab, base
        )


def backward(e, x_unit, x_inv, gains, middle, weights4, saved, keep_scores, pack_ref, gproj_ref):
    input_weight, output_weight, expand_weight, reduce_weight = weights4
    q_ref, k_ref, v_ref, w_ref, mix_ref = saved
    masks = head_masks()
    mid_unit, mid_inv = norm_stats(middle.astype(F32))
    gain_mid = gains[1:2, :]
    normed_mid = (mid_unit * gain_mid).astype(BF16)
    hidden, slope = gelu_parts(dot_nn(normed_mid, expand_weight))
    hidden = hidden.astype(BF16)
    grad_pre = (slope * dot_nn(e, reduce_weight)).astype(BF16)
    pack_columns(pack_ref, 2304, dot_tn(e, hidden))
    pack_columns(pack_ref, 1152, dot_tn(normed_mid, grad_pre))
    grad_norm, gain_mid_grad = norm_grad(dot_nt(grad_pre, expand_weight), mid_unit, mid_inv, gain_mid)
    grad_middle = e.astype(F32) + grad_norm
    grad_attended = grad_middle.astype(BF16)
    output_grad = dot_tn(mix_ref[...], grad_attended)
    grad_mixture = dot_nt(grad_attended, output_weight).astype(BF16)
    for window in range(LEVEL_WINDOWS):
        base = window * WIN_TOKENS
        rows = pl.ds(base, WIN_TOKENS)
        stack_rows = pl.ds(window * STACK, STACK)
        queries = stack_heads(q_ref[rows, :], masks)
        grads = stack_heads(grad_mixture[base : base + WIN_TOKENS], masks)
        weights = w_ref[stack_rows, :]
        keys = k_ref[rows, :]
        gproj_ref[2, rows, :] = dot_tn(weights, grads).astype(BF16)
        grad_weights = dot_nt(grads, v_ref[rows, :])
        attention = weights.astype(F32)
        moved = attention * grad_weights
        grad_scores = attention * (grad_weights - jnp.sum(moved, axis=-1, keepdims=True))
        score_part = grad_scores.astype(BF16)
        keep_scores(stack_rows, grad_scores, score_part)
        grad_queries = fold_heads(dot_nn(score_part, keys), masks) * HEAD_SIZE ** (-0.5)
        gproj_ref[0, rows, :] = grad_queries.astype(BF16)
        gproj_ref[1, rows, :] = dot_tn(score_part, queries).astype(BF16)
    normed = (x_unit * gains[0:1, :]).astype(BF16)
    parts = [gproj_ref[part] for part in range(3)]
    weight_grads = [dot_tn(normed, part) for part in parts] + [output_grad]
    pack_columns(pack_ref, 0, jnp.concatenate(weight_grads, axis=1))
    grad_normed = dot_nt(parts[0], input_weight[:, :MODEL_WIDTH])
    grad_normed = grad_normed + dot_nt(parts[1], input_weight[:, MODEL_WIDTH : 2 * MODEL_WIDTH])
    grad_normed = grad_normed + dot_nt(parts[2], input_weight[:, 2 * MODEL_WIDTH :])
    grad_normed = grad_normed.astype(BF16).astype(F32)
    grad_in, gain_in_grad = norm_grad(grad_normed, x_unit, x_inv, gains[0:1, :])
    gain_flat = jnp.concatenate([gain_in_grad, gain_mid_grad], axis=1)
    gain_rows = [gain_flat[:, i * 128 : (i + 1) * 128] for i in range(3)]
    gain_rows.append(jnp.zeros((TABLE_ROWS - GAIN_ROW - 3, 128), F32))
    result = (grad_middle + grad_in).astype(BF16)
    return result, jnp.concatenate(gain_rows, axis=0)


def keep_split(score_a, score_b):
    def keep(stack_rows, grad_scores, score_part):
        score_a[stack_rows, :] = grad_scores[:, :128]
        score_b[stack_rows, :] = jnp.concatenate(
            [grad_scores[:, 128:], jnp.zeros((STACK, 256 - WIN_TOKENS), F32)], axis=1
        )

    return keep


def pack_table(pack_ref, score_a, score_b, gain_rows, base):
    folded = fold_table(score_a, score_b)
    pack_columns(pack_ref, 0, folded[:, :256], TABLE_SLAB, base)
    tail = TYPE_ROWS // HEADS
    pieces = [folded[h * tail : (h + 1) * tail, 256:PAIR_LANES] for h in range(HEADS)]
    pieces.append(jnp.zeros((tail, 128 - HEADS * (PAIR_LANES - 256)), F32))
    rest = jnp.concatenate([jnp.concatenate(pieces, axis=1), gain_rows], axis=0)
    pack_rows(pack_ref, 2 * TYPE_ROWS, rest, TABLE_SLAB, base)


def forward_kernel(
    here_ref, x_ref, e_ref, gains_ref, wi_ref, wo_ref, we_ref, wr_ref, table_ref, order_ref,
    natural_ref, early_ref, quad0, quad1, quad2, quad3, q_ref, k_ref, v_ref, w_ref, mix_ref, mid_ref, tok_ref,
    bias_a, bias_b, part_a, part_b, part_c, lines,
):
    build_bias(load_table(table_ref, here_ref[0], (part_a, part_b, part_c), lines), bias_a, bias_b)
    gains = gains_ref[0, 0]
    order = order_ref[...]
    quads = (quad0, quad1, quad2, quad3)
    moved = reorder(e_ref[...], early_ref[...])
    for index, quad in enumerate(quads):
        quad[1] = moved[index * QUAD : (index + 1) * QUAD]
    tokens = reorder(x_ref[...], natural_ref[...])
    tok_ref[...] = tokens
    values = tokens.astype(F32)
    unit, _ = norm_stats(values)
    attention_front(
        unit, gains[0:1, :], wi_ref[0, 0], bias_a, bias_b, q_ref, k_ref, v_ref, w_ref, mix_ref
    )
    middle = (values + dot_nn(mix_ref[...], wo_ref[0, 0])).astype(BF16)
    mid_ref[...] = middle
    mid_f = middle.astype(F32)
    mid_unit, _ = norm_stats(mid_f)
    normed_mid = (mid_unit * gains[1:2, :]).astype(BF16)
    hidden, _ = gelu_parts(dot_nn(normed_mid, we_ref[0, 0]))
    output = (mid_f + dot_nt(hidden.astype(BF16), wr_ref[0, 0])).astype(BF16)
    moved = reorder(output, order)
    for index, quad in enumerate(quads):
        quad[0] = moved[index * QUAD : (index + 1) * QUAD]


def bias_kernel(here_ref, table_ref, gate_ref, bias_a, bias_b, part_a, part_b, part_c, lines):
    build_bias(load_table(table_ref, here_ref[0], (part_a, part_b, part_c), lines), bias_a, bias_b)
    for window in range(LEVEL_WINDOWS):
        mask = shift_mask(window, here_ref[0].astype(F32))
        right = jnp.concatenate(
            [mask[:, 128:], jnp.zeros((WIN_TOKENS, 256 - WIN_TOKENS), F32)], axis=1
        )
        for h in range(HEADS):
            rows = pl.ds(window * STACK + h * WIN_TOKENS, WIN_TOKENS)
            bias_a[rows, :] = bias_a[rows, :] + mask[:, :128]
            bias_b[rows, :] = bias_b[rows, :] + right


def turn_kernel(
    here_ref, x0, x1, x2, x3, gains_ref, wi_ref, wo_ref, we_ref, wr_ref, bias_a, bias_b,
    join_ref, split_ref, quad0, quad1, quad2, quad3, pack_ref, score_ref, gain_ref,
    q_ref, k_ref, v_ref, w_ref, mix_ref, gproj_ref,
):
    gains = gains_ref[0, 0]
    join = join_ref[...]
    pieces = (x0, x1, x2, x3)
    block_in = reorder(jnp.concatenate([piece[0] for piece in pieces], axis=0), join)
    e = reorder(jnp.concatenate([piece[1] for piece in pieces], axis=0), join)
    values = block_in.astype(F32)
    unit, inv = norm_stats(values)
    input_weight, output_weight = wi_ref[0, 0], wo_ref[0, 0]
    attention_front(
        unit, gains[0:1, :], input_weight, bias_a, bias_b, q_ref, k_ref,
        v_ref, w_ref, mix_ref,
    )
    attended = dot_nn(mix_ref[...], output_weight).astype(BF16).astype(F32)
    middle = (values + attended).astype(BF16)

    def keep(stack_rows, grad_scores, score_part):
        score_ref[stack_rows, :] = score_part

    result, gain_ref[...] = backward(
        e, unit, inv, gains, middle, (input_weight, output_weight, we_ref[0, 0], wr_ref[0, 0]),
        (q_ref, k_ref, v_ref, w_ref, mix_ref), keep, pack_ref, gproj_ref,
    )
    moved = reorder(result, split_ref[...])
    for index, quad in enumerate((quad0, quad1, quad2, quad3)):
        quad[...] = moved[index * QUAD : (index + 1) * QUAD]


def late_kernel(
    here_ref, pack_ref, score_ref, gain_ref, send0, send1, send2, send3, score_a, score_b, table_ref
):
    keep = keep_split(score_a, score_b)
    for window in range(LEVEL_WINDOWS):
        stack_rows = pl.ds(window * STACK, STACK)
        keep(stack_rows, score_ref[stack_rows, :].astype(F32), None)
    pack_table(table_ref, score_a, score_b, gain_ref[...], 0)
    for step, send in enumerate((send0, send1, send2, send3)):
        owner = lax.rem(here_ref[1] + step, X_SIZE)
        send[pl.ds(0, WEIGHT_SLAB), :] = pack_ref[owner]
        send[pl.ds(WEIGHT_SLAB, TABLE_SLAB), :] = table_ref[owner]


def send_slabs(here_ref, pack_ref, sends):
    for step, send in enumerate(sends):
        send[...] = pack_ref[lax.rem(here_ref[1] + step, X_SIZE)]


def backward_kernel(
    here_ref, x_ref, e0, e1, e2, e3, gains_ref, wi_ref, wo_ref, we_ref, wr_ref, join_ref,
    stored_ref, q_ref, k_ref, v_ref, w_ref, mix_ref, mid_ref, out_ref, send0, send1, send2, send3,
    score_a, score_b, pack_ref, gproj_ref,
):
    e = reorder(jnp.concatenate([e0[...], e1[...], e2[...], e3[...]], axis=0), join_ref[...])
    unit, inv = norm_stats(x_ref[...].astype(F32))
    result, gain_rows = backward(
        e, unit, inv, gains_ref[0, 0], mid_ref[...],
        (wi_ref[0, 0], wo_ref[0, 0], we_ref[0, 0], wr_ref[0, 0]),
        (q_ref, k_ref, v_ref, w_ref, mix_ref), keep_split(score_a, score_b), pack_ref, gproj_ref,
    )
    pack_table(pack_ref, score_a, score_b, gain_rows, WEIGHT_SLAB)
    out_ref[...] = reorder(result, stored_ref[...])
    send_slabs(here_ref, pack_ref, (send0, send1, send2, send3))


def unpack_kernel(scale, here_ref, got0, got1, got2, got3, *refs):
    gi_ref, go_ref, ge_ref, gr_ref, gn_ref, gt_ref = refs[-14:-8]
    rows, slab0, slab1, t0, t1, part_a, part_b, part_c = refs[-8:]
    for step, got in enumerate((got0, got1, got2, got3)):
        origin = lax.rem(here_ref[1] + X_SIZE - step, X_SIZE)
        for index in range(got.shape[0]):
            part = got[index].astype(F32)
            rows[origin, pl.ds(index * WEIGHT_PART, WEIGHT_PART), :] = part[:WEIGHT_PART] * scale
            for side, table in enumerate((slab0, slab1)):
                first = WEIGHT_PART + side * TABLE_PART
                table[origin, pl.ds(index * TABLE_PART, TABLE_PART), :] = part[
                    first : first + TABLE_PART
                ]
    for slab, table in ((slab0, t0), (slab1, t1)):
        for origin in range(X_SIZE):
            table[pl.ds(origin * TABLE_SLAB, TABLE_SLAB), :] = slab[origin]

    def block(first, count):
        pieces = []
        while count:
            origin, inner = first // WEIGHT_SLAB, first % WEIGHT_SLAB
            here = min(count, WEIGHT_SLAB - inner)
            pieces.append(rows[origin, pl.ds(inner, here), :])
            first, count = first + here, count - here
        return pieces[0] if len(pieces) == 1 else jnp.concatenate(pieces, axis=0)

    for index in range(4):
        gi_ref[0, 0, :, pl.ds(index * 128, 128)] = block(index * 192, 192)
    mixed = block(4 * 192, 192)
    gi_ref[0, 0, :, pl.ds(512, 64)] = mixed[:, :64]
    go_ref[0, 0] = jnp.concatenate([mixed[:, 64:], block(5 * 192, 192)], axis=1)
    for index in range(6):
        ge_ref[0, 0, :, pl.ds(index * 128, 128)] = block(1152 + index * 192, 192)
    for index in range(6):
        gr_ref[0, 0, :, pl.ds(index * 128, 128)] = block(2304 + index * 192, 192)
    gain = (t0[pl.ds(GAIN_ROW, 8), :] + t1[pl.ds(GAIN_ROW, 8), :]) * scale
    gn_ref[0, 0, 0:1, :] = jnp.concatenate([gain[0:1], gain[1:2, :64]], axis=1)
    gn_ref[0, 0, 1:2, :] = jnp.concatenate([gain[1:2, 64:], gain[2:3]], axis=1)
    tail, width = TYPE_ROWS // HEADS, PAIR_LANES - 256
    for side, table in enumerate((t0, t1)):
        rest = table[pl.ds(2 * TYPE_ROWS, tail), :]
        for h in range(HEADS):
            part_c[pl.ds(h * tail, tail), pl.ds(0, width)] = rest[:, h * width : (h + 1) * width]
        for window in range(LEVEL_WINDOWS):
            lines = []
            for group in range(GROUPS):
                first = window * HEADS * GROUPS + group
                place = pl.ds(first, HEADS, stride=GROUPS)
                upper = pl.ds(TYPE_ROWS + first, HEADS, stride=GROUPS)
                lines.append(
                    jnp.concatenate([table[place, :], table[upper, :], part_c[place, :]], axis=1)
                )
            span = WIN_LAT * OFFSETS
            ordered = []
            for query_level in range(WIN_LEVELS):
                for key_level in range(WIN_LEVELS):
                    for row in range(WIN_LAT):
                        line = lines[query_level * WIN_LAT + row]
                        ordered.append(line[:, key_level * span : (key_level + 1) * span])
            result = jnp.concatenate(ordered, axis=1)
            for h in range(HEADS):
                gt_ref[0, 0, window, h, side : side + 1, :] = result[h : h + 1]


LIMIT = 32 * 1024 * 1024
TOKEN_SHAPE = jax.ShapeDtypeStruct((TOKENS, MODEL_WIDTH), BF16)
QUAD_SHAPE = jax.ShapeDtypeStruct((QUAD, MODEL_WIDTH), BF16)
WEIGHT_SHAPE = jax.ShapeDtypeStruct((LEVEL_WINDOWS * STACK, WIN_TOKENS), BF16)
BIAS_SHAPE = jax.ShapeDtypeStruct((LEVEL_WINDOWS * STACK, 128), F32)
GAIN_SHAPE = jax.ShapeDtypeStruct((TABLE_ROWS - GAIN_ROW, 128), F32)
HALF_PACK_SHAPE = jax.ShapeDtypeStruct((X_SIZE, WEIGHT_SLAB, 128), BF16)
SLAB_SHAPE = jax.ShapeDtypeStruct((WEIGHT_SLAB + TABLE_SLAB, 128), BF16)
PAIR_SHAPE = jax.ShapeDtypeStruct((2, QUAD, MODEL_WIDTH), BF16)
GRAD_SHAPES = tuple(
    jax.ShapeDtypeStruct((1, BLOCKS) + shape, F32)
    for shape in (
        (MODEL_WIDTH, 3 * MODEL_WIDTH), (MODEL_WIDTH, MODEL_WIDTH), (MODEL_WIDTH, MLP_WIDTH),
        (MODEL_WIDTH, MLP_WIDTH), (2, MODEL_WIDTH), (LEVEL_WINDOWS, HEADS, 2, BIAS_SLOTS),
    )
)


def tall_scratch():
    return pltpu.VMEM((LEVEL_WINDOWS * STACK, 128), F32)


def token_scratch():
    return pltpu.VMEM((TOKENS, MODEL_WIDTH), BF16)


def whole(array):
    rank = len(array.shape)
    return pl.BlockSpec(array.shape, lambda i: (0,) * rank)


def one_block(array, index):
    rank = len(array.shape)
    return pl.BlockSpec((1, 1) + array.shape[2:], lambda i: (0, index) + (0,) * (rank - 2))


def call(kernel, here, ins, outs, scratch, aliases=None, pinned=False):
    arrays = [array for array, _ in ins]
    if pinned:
        arrays = [pltpu.with_memory_space_constraint(array, pltpu.HBM) for array in arrays]
    return pl.pallas_call(
        functools.partial(kernel, here),
        out_shape=tuple(shape for shape, _ in outs),
        grid_spec=pltpu.PrefetchScalarGridSpec(
            num_scalar_prefetch=0,
            grid=(1,),
            in_specs=[spec for _, spec in ins],
            out_specs=tuple(spec for _, spec in outs),
            scratch_shapes=scratch,
        ),
        input_output_aliases=aliases or {},
        compiler_params=pltpu.CompilerParams(vmem_limit_bytes=LIMIT),
    )(*arrays)


class Here:
    def __getitem__(self, index):
        return lax.axis_index(("lat", "x")[index])


def plain(*arrays):
    return [(array, whole(array)) for array in arrays]


def exchange(quads, by):
    lon = ("z", "x")
    ring, sides = lax.axis_size(lon), lax.axis_size("lat")
    lon_pairs = [(i, (i + by) % ring) for i in range(ring)]
    swap = [(i, i ^ 1) for i in range(sides)]
    both = [
        (i * sides + j, ((i + by) % ring) * sides + (j ^ 1)) for i in range(ring) for j in range(sides)
    ]
    return (
        quads[0],
        lax.ppermute(quads[1], lon, lon_pairs),
        lax.ppermute(quads[2], "lat", swap),
        lax.ppermute(quads[3], lon + ("lat",), both),
    )


def swap_all(values, axes):
    return lax.all_to_all(values, axes, split_axis=0, concat_axis=0, tiled=True)


def pass_x(sends):
    size = lax.axis_size("x")
    return (sends[0],) + tuple(
        lax.ppermute(sends[step], "x", [(i, (i + step) % size) for i in range(size)])
        for step in range(1, size)
    )


def slab_sum(slabs):
    total = slabs[0][...].astype(F32)
    for slab in slabs[1:]:
        total = total + slab[...].astype(F32)
    return total


def write_parts(total, out_ref, first):
    for index in range(out_ref.shape[0]):
        weights = total[index * WEIGHT_PART : (index + 1) * WEIGHT_PART]
        start = WEIGHT_SLAB + index * TABLE_PART
        part = jnp.concatenate([weights, total[start : start + TABLE_PART]], axis=0)
        out_ref[index, pl.ds(first, SENT), :] = part.astype(BF16)


def part_sum(spread_ref, first):
    sides = []
    for side in range(2):
        total = spread_ref[side, pl.ds(first, SENT), :].astype(F32)
        for index in range(side + 2, spread_ref.shape[0], 2):
            total = total + spread_ref[index, pl.ds(first, SENT), :].astype(F32)
        sides.append(total)
    weights = sides[0][:WEIGHT_PART] + sides[1][:WEIGHT_PART]
    spare = jnp.zeros((PART - SENT - TABLE_PART, 128), F32)
    rows = [weights, sides[0][WEIGHT_PART:], sides[1][WEIGHT_PART:], spare]
    return jnp.concatenate(rows, axis=0).astype(BF16)


def first_kernel(here_ref, slab0, slab1, slab2, slab3, out_ref):
    write_parts(slab_sum((slab0, slab1, slab2, slab3)), out_ref, 0)


def second_kernel(here_ref, late_ref, slab0, slab1, slab2, slab3, out_ref):
    late = part_sum(late_ref, 0)
    for index in range(out_ref.shape[0]):
        out_ref[index, pl.ds(0, PART), :] = late
    write_parts(slab_sum((slab0, slab1, slab2, slab3)), out_ref, PART)


def third_kernel(here_ref, both_ref, late_ref, early_ref):
    early = part_sum(both_ref, PART)
    for index in range(late_ref.shape[0]):
        late_ref[index] = both_ref[index, pl.ds(0, PART), :]
        early_ref[index] = early


def parts_shape(count, width):
    return jax.ShapeDtypeStruct((count, width, 128), BF16)


def unpack(parts, here, index, scale, previous):
    ins = plain(*parts)
    aliases = {}
    if previous is not None:
        ins = ins + [(array, pl.BlockSpec(memory_space=pl.ANY)) for array in previous]
        aliases = {len(parts) + place: place for place in range(6)}
    outs = [(shape, one_block(shape, index)) for shape in GRAD_SHAPES]
    scratch = [pltpu.VMEM((X_SIZE, WEIGHT_SLAB, 128), F32)]
    scratch += [pltpu.VMEM((X_SIZE, TABLE_SLAB, 128), F32) for _ in range(2)]
    scratch += [pltpu.VMEM((TABLE_ROWS, 128), F32) for _ in range(2)] + type_scratch()
    return call(functools.partial(unpack_kernel, scale), here, ins, outs, scratch, aliases)


def type_scratch():
    return [pltpu.VMEM((TYPE_ROWS, 128), F32) for _ in range(3)]


def pack_scratch():
    return pltpu.VMEM((X_SIZE,) + SLAB_SHAPE.shape, BF16)


def stored_tokens(array):
    return array[0].transpose(1, 2, 0, 3).reshape(TOKENS, MODEL_WIDTH)


def on_device(
    inputs, grad_output, norm_gains, input_weight, output_weight, expand_weight, reduce_weight,
    bias_table,
):
    here = Here()
    orders = [jnp.asarray(order) for order in quad_orders()]
    split, join_rolled, split_rolled, join, natural, early_split, stored = orders
    reduce_weight = reduce_weight.swapaxes(2, 3)
    bias_table = bias_table.swapaxes(3, 4)
    weights = [
        [(array, one_block(array, block)) for array in
         (norm_gains, input_weight, output_weight, expand_weight, reduce_weight)]
        for block in range(BLOCKS)
    ]
    tables = [[(bias_table, one_block(bias_table, block))] for block in range(BLOCKS)]
    front_scratch = [tall_scratch(), tall_scratch()] + type_scratch()
    front_scratch.append(pltpu.VMEM((8, BIAS_SLOTS), F32))
    outs = call(
        forward_kernel,
        here,
        plain(stored_tokens(inputs), stored_tokens(grad_output)) + weights[0] + tables[0]
        + plain(split, natural, early_split),
        plain(*((PAIR_SHAPE,) * 4 + (TOKEN_SHAPE,) * 3 + (WEIGHT_SHAPE,) + (TOKEN_SHAPE,) * 3)),
        front_scratch,
        pinned=True,
    )
    saved = outs[4:10]
    tokens = outs[10]
    quads = exchange(outs[:4], -1)
    gate = outs[0]
    bias = call(
        bias_kernel,
        here,
        tables[1] + [(gate, pl.BlockSpec(memory_space=pl.ANY))],
        plain(BIAS_SHAPE, BIAS_SHAPE),
        front_scratch[2:],
    )
    outs = call(
        turn_kernel,
        here,
        plain(*quads) + weights[1] + plain(*bias, join_rolled, split_rolled),
        plain(*((QUAD_SHAPE,) * 4 + (HALF_PACK_SHAPE, WEIGHT_SHAPE, GAIN_SHAPE))),
        [token_scratch() for _ in range(3)]
        + [pltpu.VMEM(WEIGHT_SHAPE.shape, BF16), token_scratch(),
           pltpu.VMEM((3, TOKENS, MODEL_WIDTH), BF16)],
    )
    flow_quads = exchange(outs[:4], 1)
    late = call(
        late_kernel,
        here,
        plain(*outs[4:]),
        plain(*(SLAB_SHAPE,) * 4),
        [tall_scratch(), tall_scratch(), pltpu.VMEM((X_SIZE, TABLE_SLAB, 128), BF16)],
    )
    flow_quads, late = lax.optimization_barrier((flow_quads, late))
    late = pass_x(late)
    outs = call(
        backward_kernel,
        here,
        plain(tokens, *flow_quads) + weights[0] + plain(join, stored, *saved),
        plain(*((TOKEN_SHAPE,) + (SLAB_SHAPE,) * 4)),
        [tall_scratch(), tall_scratch(), pack_scratch(),
         pltpu.VMEM((3, TOKENS, MODEL_WIDTH), BF16)],
    )
    grad_flow = outs[0]
    late, early = lax.optimization_barrier((late, outs[1:]))
    early = pass_x(early)
    rest = ("z", "lat")
    count = lax.axis_size(rest)
    lat_total = LAT_DEV * lax.axis_size("lat")
    scale = float(LEVELS * lat_total * LON_DEV * lax.axis_size(("z", "x"))) ** (-0.5)
    (late,) = call(first_kernel, here, plain(*late), plain(parts_shape(count, SENT)), [])
    late = swap_all(late, rest)
    (both,) = call(
        second_kernel, here, plain(late, *early), plain(parts_shape(count, PART + SENT)), []
    )
    upstream = lax.ppermute(
        grad_flow, "section", [(i, i - 1) for i in range(1, lax.axis_size("section"))]
    )
    both, upstream = lax.optimization_barrier((swap_all(both, rest), upstream))
    late, early = call(
        third_kernel, here, plain(both), plain(*(parts_shape(count, PART),) * 2), []
    )
    late = pass_x((late,) * X_SIZE)
    early = pass_x((swap_all(early, rest),) * X_SIZE)
    upstream = upstream.reshape(LAT_DEV, LON_DEV, LEVELS, MODEL_WIDTH).transpose(2, 0, 1, 3)[None]
    grads = unpack(late, here, 1, scale, None)
    grads = list(unpack(early, here, 0, scale, grads))
    grads[3] = grads[3].swapaxes(2, 3)
    grads[5] = grads[5].swapaxes(3, 4)
    return (upstream,) + tuple(grads)


def solution(mesh):
    sizes = mesh.shape
    grid = mesh.devices.reshape(
        sizes["section"], sizes["lon"] // X_SIZE, X_SIZE, sizes["lat"]
    )
    mesh = Mesh(grid, ("section", "z", "x", "lat"))
    return jax.shard_map(
        on_device,
        mesh=mesh,
        in_specs=(
            P("section", None, "lat", ("z", "x"), None),
            P("section", None, "lat", ("z", "x"), None),
            P("section", None, None, None),
            P("section", None, None, None),
            P("section", None, None, None),
            P("section", None, None, None),
            P("section", None, None, None),
            P("section", None, None, None, None, None),
        ),
        out_specs=(
            P("section", None, "lat", ("z", "x"), None),
            P("section", None, None, None),
            P("section", None, None, None),
            P("section", None, None, None),
            P("section", None, None, None),
            P("section", None, None, None),
            P("section", None, None, None, None, None),
        ),
        check_vma=False,
    )
```
